32 devices in a mesh: dp: 8 (over y, x, core), seq: 4 (over z).
Axes of the slice: x: 2, y: 2, z: 4, core: 2. Of those that a mesh axis runs over, the one named last changes fastest.
Arguments:
- tokens: bfloat16 [8, 512, 1024], P('dp', 'seq'), may hold values from -6 to 6
- cotangent: bfloat16 [8, 512, 1024], P('dp', 'seq'), may hold values from -6 to 6
- stamps: int32 [8, 512], P('dp'), may hold values from 0 to 1080832, as said below
- lengths: int32 [8], P('dp'), may hold values from 64 to 512, as said below
- w_qkvu: bfloat16 [1024, 4096], P('dp'), may hold values from -0.1875 to 0.1875
- w_out: bfloat16 [1024, 1024], P('dp'), may hold values from -0.1875 to 0.1875
- gain_in: float32 [1024], replicated, may hold values from 0.25 to 1.75
- gain_out: float32 [1024], replicated, may hold values from 0.25 to 1.75
- bias_table: float32 [8, 16], replicated, may hold values from -4 to 4
Outputs:
- mixed: bfloat16 [8, 512, 1024], P('dp', 'seq')
- input_grad: bfloat16 [8, 512, 1024], P('dp', 'seq')
- out_weight_grad: float32 [1024, 1024], P('dp')
The draws below stay inside these ranges and needn't reach their ends.
Inputs may be any that keep to these rules, and one draw needn't show every extreme that they name: `lengths`: each stream has 64 valid actions or more; some stream is full. `stamps`: timestamps never fall along a stream, and consecutive ones differ by less than 64.
All inputs are finite; a program needn't handle non-finite values.
Results may differ from the reference program's by a relative error of at most 0.019.
Values may be sent and summed in bfloat16 or wider, within the bound.
A program may use at most 128 MiB of HBM per device.

```python
import jax
import jax.numpy as jnp
from jax import lax

D = 1024
H = 8
DH = 128
NB = 16
TOK_DEV = 128
SEQLEN = 512
STREAMS = 8
N_SEQ = 4


def draw_lengths(key, part):
    spread = jax.random.randint(key, (STREAMS,), SEQLEN // 8, SEQLEN + 1)
    chosen = jax.random.randint(jax.random.fold_in(key, 7), (), 0, STREAMS)
    return jnp.where(jnp.arange(STREAMS) == chosen, SEQLEN, spread).astype(jnp.int32)


def draw_stamps(key, part):
    anchor = jax.random.randint(key, (STREAMS, 1), 0, 2 ** 20)
    increments = jax.random.randint(jax.random.fold_in(key, 3), (STREAMS, SEQLEN), 0, 64)
    return (anchor + jnp.cumsum(increments, axis=1) - increments[:, :1]).astype(jnp.int32)


def shard_levels(rng, dims, pieces, low, high):
    def one(position, shards_of):
        steps = jax.random.uniform(jax.random.fold_in(jax.random.fold_in(rng, 6), position), (shards_of,), jnp.float32, low / len(pieces), high / len(pieces))
        return jnp.repeat(jnp.exp(steps), dims[position] // shards_of).reshape((-1,) + (1,) * (len(dims) - position - 1))

    loudness = one(*pieces[0])
    for cut in pieces[1:]:
        loudness = loudness * one(*cut)
    return loudness


def normal_values(own_key, shape, deviation, limit, pieces=(), held_as=jnp.bfloat16):
    level = shard_levels(own_key, shape, pieces, -0.22, 0.18) if pieces else 1.0
    entries = jax.random.normal(own_key, shape, jnp.float32) * deviation * level
    return jnp.minimum(jnp.maximum(entries, -limit), limit).astype(held_as)


def setup_inputs(seed: int = 0) -> dict:
    streams_of = jax.random.split(jax.random.key(seed), 10)
    tokens = normal_values(streams_of[0], (STREAMS, SEQLEN, D), 1.0, 6.0, ((0, 8), (1, 4)))
    cotangent = normal_values(streams_of[1], (STREAMS, SEQLEN, D), 1.0, 6.0, ((0, 8), (1, 4)))
    stamps = draw_stamps(jax.random.fold_in(streams_of[9], 71), 0)
    lengths = draw_lengths(jax.random.fold_in(streams_of[9], 71), 0)
    w_qkvu = normal_values(streams_of[4], (D, 4 * D), D ** -0.5, 0.1875, ((0, 8),))
    w_out = normal_values(streams_of[5], (D, D), D ** -0.5, 0.1875, ((0, 8),))
    gain_in = jnp.clip(1.0 + 0.15 * jax.random.normal(streams_of[6], (D,), jnp.float32), 0.25, 1.75)
    gain_out = jnp.clip(1.0 + 0.15 * jax.random.normal(streams_of[7], (D,), jnp.float32), 0.25, 1.75)
    bias_table = normal_values(streams_of[8], (H, NB), 1.0, 4.0, (), jnp.float32)
    return {"tokens": tokens, "cotangent": cotangent, "stamps": stamps, "lengths": lengths, "w_qkvu": w_qkvu, "w_out": w_out, "gain_in": gain_in, "gain_out": gain_out, "bias_table": bias_table}


EPS = 1e-05

def layer_norm(values, gain):
    average = lax.optimization_barrier(jnp.mean(values, axis=-1, keepdims=True))
    centred = values - average
    variance = lax.optimization_barrier(jnp.mean(centred * centred, axis=-1, keepdims=True))
    return centred * lax.rsqrt(variance + EPS) * gain

def silu_slope(values):
    sigmoid_v = jax.nn.sigmoid(values)
    return sigmoid_v * (1.0 + values * (1.0 - sigmoid_v))

def rounded(values):
    return lax.optimization_barrier(values.astype(jnp.bfloat16)).astype(jnp.float32)

def time_bias(bias_table, stamps_q, stamps_k):
    elapsed = stamps_q[:, None] - stamps_k[None, :]
    bucket = jnp.zeros(elapsed.shape, jnp.int32)
    for degree in range(1, bias_table.shape[1]):
        bucket = bucket + (elapsed >= 2 ** degree - 1).astype(jnp.int32)
    biases = jnp.zeros((bias_table.shape[0],) + elapsed.shape, jnp.float32)
    for degree in range(bias_table.shape[1]):
        biases = biases + jnp.where(bucket[None] == degree, bias_table[:, degree][:, None, None], 0.0)
    return biases

def one_stream(x_rows, cot_rows, stamp_row, length, w_qkvu, w_out, gain_in, gain_out, bias_table):
    scale = DH ** (-0.5)
    wide_rows = x_rows.astype(jnp.float32)
    normed = layer_norm(wide_rows, gain_in).astype(jnp.bfloat16)
    projected = jnp.dot(normed, w_qkvu, preferred_element_type=jnp.float32)
    activated = jax.nn.silu(projected)
    gate_u = activated[:, :D]
    v_heads = rounded(activated[:, D:2 * D]).reshape(SEQLEN, H, DH)
    q_heads = rounded(activated[:, 2 * D:3 * D]).reshape(SEQLEN, H, DH)
    k_heads = rounded(activated[:, 3 * D:]).reshape(SEQLEN, H, DH)
    positions = jnp.arange(SEQLEN, dtype=jnp.int32)
    live = positions < length
    allowed = (positions[None, :] <= positions[:, None]) & live[None, :] & live[:, None]
    scores = jnp.einsum('qhd,khd->hqk', q_heads, k_heads) * scale + time_bias(bias_table, stamp_row, stamp_row)
    weight = rounded(jnp.where(allowed[None], jax.nn.silu(scores), 0.0))
    attended = jnp.einsum('hqk,khd->qhd', weight, v_heads).reshape(SEQLEN, D)
    normed_att, norm_back = jax.vjp(lambda values: layer_norm(values, gain_out), attended)
    mixed_rows = (normed_att * gate_u).astype(jnp.bfloat16)
    mixed = (wide_rows + jnp.dot(mixed_rows, w_out, preferred_element_type=jnp.float32)).astype(jnp.bfloat16)
    w_grad = jnp.dot(mixed_rows.T, cot_rows, preferred_element_type=jnp.float32)
    d_mix = jnp.dot(cot_rows, w_out.T, preferred_element_type=jnp.float32)
    d_gate = d_mix * normed_att
    d_heads = rounded(norm_back(d_mix * gate_u)[0]).reshape(SEQLEN, H, DH)
    d_weight = jnp.einsum('qhd,khd->hqk', d_heads, v_heads)
    d_scores = rounded(jnp.where(allowed[None], d_weight * silu_slope(scores), 0.0))
    q_grad = jnp.einsum('hqk,khd->qhd', d_scores, k_heads) * scale
    scores_sh = d_scores.reshape(H, N_SEQ, TOK_DEV, SEQLEN)
    weight_sh = weight.reshape(H, N_SEQ, TOK_DEV, SEQLEN)
    q_sh = q_heads.reshape(N_SEQ, TOK_DEV, H, DH)
    d_sh = d_heads.reshape(N_SEQ, TOK_DEV, H, DH)
    k_parts = rounded(jnp.einsum('hsqk,sqhd->skhd', scores_sh, q_sh) * scale)
    v_parts = rounded(jnp.einsum('hsqk,sqhd->skhd', weight_sh, d_sh))
    k_grad = lax.optimization_barrier(jnp.sum(k_parts, axis=0)).reshape(SEQLEN, D)
    v_grad = lax.optimization_barrier(jnp.sum(v_parts, axis=0)).reshape(SEQLEN, D)
    d_act = jnp.concatenate([d_gate, v_grad, q_grad.reshape(SEQLEN, D), k_grad], axis=1)
    d_proj = (d_act * silu_slope(projected)).astype(jnp.bfloat16)
    d_normed = jnp.dot(d_proj, w_qkvu.T, preferred_element_type=jnp.float32)
    unused_rows, in_back = jax.vjp(lambda values: layer_norm(values, gain_in), wide_rows)
    input_grad = (cot_rows.astype(jnp.float32) + in_back(d_normed)[0]).astype(jnp.bfloat16)
    return (mixed, input_grad, w_grad)

def reference(tokens, cotangent, stamps, lengths, w_qkvu, w_out, gain_in, gain_out, bias_table):

    def visit(total, inputs):
        x_rows, cot_rows, stamp_row, length = inputs
        mixed, input_grad, w_grad = one_stream(x_rows, cot_rows, stamp_row, length, w_qkvu, w_out, gain_in, gain_out, bias_table)
        return (total + w_grad, (mixed, input_grad))
    w_total, outputs = lax.scan(visit, jnp.zeros((D, D), jnp.float32), (tokens, cotangent, stamps, lengths))
    return (outputs[0], outputs[1], w_total)
```

```python
import jax
import jax.numpy as jnp
from jax import lax
from jax.experimental import pallas as pl
from jax.experimental.pallas import tpu as pltpu
from jax.sharding import PartitionSpec as P

H = 8
DH = 128


EPS = 1e-05


def layer_norm(values, gain):
    average = jnp.mean(values, axis=-1, keepdims=True)
    centred = values - average
    variance = jnp.mean(centred * centred, axis=-1, keepdims=True)
    return centred * lax.rsqrt(variance + EPS) * gain


def silu_slope(values):
    sigmoid_v = jax.nn.sigmoid(values)
    return sigmoid_v * (1.0 + values * (1.0 - sigmoid_v))


def time_bias(bias_table, stamps_q, stamps_k):
    elapsed = stamps_q[:, None] - stamps_k[None, :]
    bucket = jnp.zeros(elapsed.shape, jnp.int32)
    for degree in range(1, bias_table.shape[1]):
        bucket = bucket + (elapsed >= 2**degree - 1).astype(jnp.int32)
    levels = jnp.arange(bias_table.shape[1], dtype=jnp.int32)
    one_hot = (bucket[:, :, None] == levels[None, None, :]).astype(jnp.float32)
    return jnp.einsum(
        "qkb,hb->hqk",
        one_hot,
        bias_table,
        precision=lax.Precision.HIGHEST,
        preferred_element_type=jnp.float32,
    )


def pair_terms(
    q_heads, d_heads, stamps_q, pos_q, k_heads, v_heads, stamps_k, pos_k, length, bias_table, scale
):
    scores = (
        jnp.einsum("qhd,khd->hqk", q_heads, k_heads, preferred_element_type=jnp.float32) * scale
    )
    scores = scores + time_bias(bias_table, stamps_q, stamps_k)
    allowed = (
        (pos_k[None, :] <= pos_q[:, None]) & (pos_k[None, :] < length) & (pos_q[:, None] < length)
    )
    weight = jnp.where(allowed[None], jax.nn.silu(scores), 0.0).astype(jnp.bfloat16)
    if d_heads is None:
        return (weight, None)
    d_weight = jnp.einsum("qhd,khd->hqk", d_heads, v_heads, preferred_element_type=jnp.float32)
    d_scores = jnp.where(allowed[None], d_weight * silu_slope(scores), 0.0).astype(jnp.bfloat16)
    return (weight, d_scores)


def per_device(tokens, cotangent, stamps, lengths, w_qkvu, w_out, gain_in, gain_out, bias_table):
    rows = tokens[0]
    cot_rows = cotangent[0]
    tok_count = rows.shape[0]
    feature_width = rows.shape[1]
    seq_count = lax.axis_size("seq")
    total_rows = tok_count * seq_count
    first_row = lax.axis_index("seq") * tok_count
    length = lengths[0]
    stamp_all = stamps[0]
    pos_own = first_row + jnp.arange(tok_count, dtype=jnp.int32)
    stamp_own = lax.dynamic_slice_in_dim(stamp_all, first_row, tok_count)
    scale = DH ** (-0.5)
    block_rows = min(512, total_rows)
    block_count = total_rows // block_rows
    w_full, w_out_full = (
        lax.all_gather(w_qkvu, "dp", axis=0, tiled=True),
        lax.all_gather(w_out, "dp", axis=0, tiled=True),
    )
    wide_rows = rows.astype(jnp.float32)
    normed = layer_norm(wide_rows, gain_in).astype(jnp.bfloat16)
    projected = jnp.dot(normed, w_full, preferred_element_type=jnp.float32)
    activated = jax.nn.silu(projected)
    gate_u = activated[:, :feature_width]
    values_own = activated[:, feature_width : 2 * feature_width].astype(jnp.bfloat16)
    queries_own = activated[:, 2 * feature_width : 3 * feature_width].astype(jnp.bfloat16)
    keys_own = activated[:, 3 * feature_width :].astype(jnp.bfloat16)
    keys_all, values_all = (
        lax.all_gather(keys_own, "seq", axis=0, tiled=True),
        lax.all_gather(values_own, "seq", axis=0, tiled=True),
    )
    q_heads = queries_own.reshape(tok_count, H, DH)

    def key_block(start):
        k_heads = lax.dynamic_slice_in_dim(keys_all, start, block_rows).reshape(block_rows, H, DH)
        v_heads = lax.dynamic_slice_in_dim(values_all, start, block_rows).reshape(block_rows, H, DH)
        stamps_k = lax.dynamic_slice_in_dim(stamp_all, start, block_rows)
        pos_k = start + jnp.arange(block_rows, dtype=jnp.int32)
        return (k_heads, v_heads, stamps_k, pos_k)

    def guarded(active, action, state):
        return lax.cond(active, action, lambda same: same, state)

    def reaches(start):
        return (start <= first_row + tok_count - 1) & (start < length) & (first_row < length)

    def forward_step(block_idx, totals):
        start = block_idx * block_rows

        def forward_compute(totals):
            k_heads, v_heads, stamps_k, pos_k = key_block(start)
            weight, unused = pair_terms(
                q_heads,
                None,
                stamp_own,
                pos_own,
                k_heads,
                v_heads,
                stamps_k,
                pos_k,
                length,
                bias_table,
                scale,
            )
            return totals + jnp.einsum(
                "hqk,khd->qhd", weight, v_heads, preferred_element_type=jnp.float32
            )

        return guarded(reaches(start), forward_compute, totals)

    attended = lax.fori_loop(
        0, block_count, forward_step, jnp.zeros((tok_count, H, DH), jnp.float32)
    )
    attended = attended.reshape(tok_count, feature_width)
    normed_att, norm_back = jax.vjp(lambda values: layer_norm(values, gain_out), attended)
    mixed_rows = (normed_att * gate_u).astype(jnp.bfloat16)
    mixed = (
        wide_rows + jnp.dot(mixed_rows, w_out_full, preferred_element_type=jnp.float32)
    ).astype(jnp.bfloat16)
    grad_part = lax.psum_scatter(
        jnp.einsum("tr,tc->rc", mixed_rows, cot_rows, preferred_element_type=jnp.float32).astype(
            jnp.bfloat16
        ),
        "dp",
        scatter_dimension=0,
        tiled=True,
    )
    w_grad = lax.psum(grad_part, "seq").astype(jnp.float32)
    d_mix = jnp.einsum("tc,rc->tr", cot_rows, w_out_full, preferred_element_type=jnp.float32)
    d_gate = d_mix * normed_att
    d_att = norm_back(d_mix * gate_u)[0].astype(jnp.bfloat16)
    d_heads = d_att.reshape(tok_count, H, DH)

    def backward_step():

        def step(block_idx, state_pair):
            start = block_idx * block_rows

            def step_compute(state_pair):
                q_grad, key_terms = state_pair
                k_heads, v_heads, stamps_k, pos_k = key_block(start)
                weight, d_scores = pair_terms(
                    q_heads,
                    d_heads,
                    stamp_own,
                    pos_own,
                    k_heads,
                    v_heads,
                    stamps_k,
                    pos_k,
                    length,
                    bias_table,
                    scale,
                )
                q_grad = (
                    q_grad
                    + jnp.einsum(
                        "hqk,khd->qhd", d_scores, k_heads, preferred_element_type=jnp.float32
                    )
                    * scale
                )
                k_grad = (
                    jnp.einsum(
                        "hqk,qhd->khd", d_scores, q_heads, preferred_element_type=jnp.float32
                    )
                    * scale
                )
                v_grad = jnp.einsum(
                    "hqk,qhd->khd", weight, d_heads, preferred_element_type=jnp.float32
                )
                joined = jnp.concatenate(
                    [
                        k_grad.reshape(block_rows, feature_width),
                        v_grad.reshape(block_rows, feature_width),
                    ],
                    axis=1,
                )
                key_terms = lax.dynamic_update_slice_in_dim(key_terms, joined, start, 0)
                return (q_grad, key_terms)

            return guarded(reaches(start), step_compute, state_pair)

        return step

    q_start = jnp.zeros((tok_count, H, DH), jnp.float32)
    term_start = jnp.zeros((total_rows, 2 * feature_width), jnp.float32)
    q_grad, key_terms = lax.fori_loop(0, block_count, backward_step(), (q_start, term_start))
    key_grads = lax.psum_scatter(
        key_terms.astype(jnp.bfloat16), "seq", scatter_dimension=0, tiled=True
    ).astype(jnp.float32)
    d_act = jnp.concatenate(
        [
            d_gate,
            key_grads[:, feature_width:],
            q_grad.reshape(tok_count, feature_width),
            key_grads[:, :feature_width],
        ],
        axis=1,
    )
    d_proj = (d_act * silu_slope(projected)).astype(jnp.bfloat16)
    d_normed = jnp.einsum("tf,df->td", d_proj, w_full, preferred_element_type=jnp.float32)
    unused_rows, in_back = jax.vjp(lambda values: layer_norm(values, gain_in), wide_rows)
    input_grad = (cot_rows.astype(jnp.float32) + in_back(d_normed)[0]).astype(jnp.bfloat16)
    return (mixed[None], input_grad[None], w_grad)


MESH = pl.DeviceIdType.MESH
VM = pl.BlockSpec(memory_space=pltpu.VMEM)
F32 = jnp.float32
BF16 = jnp.bfloat16
MASKED = -1e30


def mm(a, b, dims):
    return lax.dot_general(a, b, (dims, ((), ())), preferred_element_type=F32)


def remote(src, dst, send_sem, recv_sem, target):
    return pltpu.make_async_remote_copy(
        src_ref=src,
        dst_ref=dst,
        send_sem=send_sem,
        recv_sem=recv_sem,
        device_id=target,
        device_id_type=MESH,
    )


def arrived(dst, sem):
    pltpu.make_async_copy(dst, dst, sem).wait()


def column_kernel(
    n_dp, n_seq, w_ref, x_ref, c_ref, wo_ref, meta_ref, gin_ref, gout_ref, bias_ref,
    mixed_ref, grad_ref, wg_ref,
    W, X, C, WO, mbuf, NB, BI, PJ, GT, ACT, ATT, WT, SL, DM, DG, DA, DP, MR, KA, VA, ST,
    MW, WG, PS, PR, TS, TR, PB, SB, CS, FB, FIN, RO,
    wsend, wrelay, wrecv, zsend, ssend, farsend, xrecv, wosend, worecv, msem,
    stsend, strecv, gsend, grecv, hsem, tsend, trecv, psend, precv, csend, crecv, osend, orecv,
):
    me = lax.axis_index("dp")
    z = lax.axis_index("seq")
    tok, width = x_ref.shape
    rows = tok * n_seq
    half = tok // 2
    n_heads = n_dp
    scale = DH ** (-0.5)
    chip, k = me // 2, me % 2
    cy, cx = chip // 2, chip % 2
    xn, yn = 2 * cy + (1 - cx), 2 * (1 - cy) + cx
    dn = 2 * (1 - cy) + (1 - cx)
    sib = 2 * chip + (1 - k)
    p, ks = z % 2, z // 2
    near, far = 1 + ks, (n_seq - 1) * ks
    zp = near + far - z
    is_near, is_far = z == near, z == far
    is_main = k == ks
    is_aux = jnp.logical_not(is_main)
    main_dp = 2 * chip + ks

    def head_of(core, j):
        return 4 * core + 2 * j + p

    def rows_of(ref_rows, index):
        return pl.ds(pl.multiple_of(index * ref_rows, ref_rows), ref_rows)

    def lanes_of(index):
        return pl.ds(pl.multiple_of(index * DH, DH), DH)

    def w_copies(core, j, make):
        return [
            make(
                w_ref.at[:, lanes_of(g * n_heads + head_of(core, j))],
                W.at[j, rows_of(tok, me), slice(g * DH, (g + 1) * DH)],
            )
            for g in range(4)
        ]

    w_targets = ((xn, 0, 1), (yn, 1, 4), (chip, 1 - k, 0), (xn, 1, 2), (yn, 0, 3))

    def w_start(j):
        for where, core, index in w_targets:
            for copy in w_copies(
                core, j,
                lambda s, d: remote(s, d, wsend.at[index, j], wrecv.at[me, j], (2 * where + core, z)),
            ):
                copy.start()

    def w_piece(src, j):
        return W.at[j, rows_of(tok, src)]

    via, to = (1 - k) * xn + k * yn, (1 - k) * yn + k * xn

    def w_relay(i, j):
        src = 2 * via + i
        block = w_piece(src, j)
        return remote(block, block, wrelay.at[i, j], wrecv.at[src, j], (2 * to + k, z))

    def w_wait(src, j):
        arrived(w_piece(src, j), wrecv.at[src, j])

    ins, outs = (x_ref, c_ref), (X, C)
    z_to = jnp.where(is_main, zp, 1 + k)

    def z_send(a):
        return remote(ins[a], outs[a].at[z], zsend.at[a], xrecv.at[a, z], (me, z_to))

    def own_copy(a):
        return pltpu.make_async_copy(ins[a], outs[a].at[z], xrecv.at[a, z])

    def share(a, b):
        block = ins[a] if b is None else outs[a].at[b]
        at = z if b is None else b
        return remote(block, outs[a].at[at], ssend.at[a, at], xrecv.at[a, at], (sib, z))

    foreign = (2 * (1 - ks), 2 * (1 - ks) + 1)

    def to_far(a, i):
        block = outs[a].at[foreign[i]]
        return remote(block, block, farsend.at[a, i], xrecv.at[a, foreign[i]], (me, far))

    def x_wait(a, b):
        arrived(outs[a].at[b], xrecv.at[a, b])

    def meta_send():
        return remote(meta_ref, mbuf, msem.at[0], msem.at[1], (sib, z))

    wo_core, wo_slot = chip // 2, chip % 2
    wo_here = wo_core == k
    wo_sends = [
        remote(wo_ref, WO.at[wo_slot], wosend.at[i], worecv.at[wo_slot], (2 * where + wo_core, z))
        for i, where in enumerate((xn, yn, dn, chip))
    ]

    @pl.when(is_main)
    def _():
        pltpu.make_async_copy(meta_ref, mbuf, msem.at[1]).start()
        meta_send().start()

    w_start(0)
    z_send(0).start()

    @pl.when(is_main)
    def _():
        own_copy(0).start()
        share(0, None).start()

    z_send(1).start()

    @pl.when(is_main)
    def _():
        own_copy(1).start()
        share(1, None).start()

    for j in range(2):
        for copy in w_copies(k, j, lambda s, d: pltpu.make_async_copy(s, d, wrecv.at[me, j])):
            copy.start()

    def relay_weights(j):
        for i in range(2):
            w_wait(2 * via + i, j)
            w_relay(i, j).start()

    def near_relay(a):
        @pl.when(is_main)
        def _():
            x_wait(a, zp)
            share(a, zp).start()

        @pl.when(is_main & is_near)
        def _():
            for i in range(2):
                x_wait(a, foreign[i])
                to_far(a, i).start()
                share(a, foreign[i]).start()

    def far_relay(a):
        @pl.when(is_main & is_far)
        def _():
            for i in range(2):
                x_wait(a, foreign[i])
                share(a, foreign[i]).start()

    relay_weights(0)
    w_start(1)
    near_relay(0)

    arrived(mbuf, msem.at[1])
    lane_row = lax.broadcasted_iota(jnp.int32, (DH, DH), 0)
    lane_col = lax.broadcasted_iota(jnp.int32, (DH, DH), 1)
    length = mbuf[n_seq : n_seq + 1, :]
    for i in range(n_seq):
        col = jnp.broadcast_to(mbuf[i : i + 1, :].astype(F32), (DH, DH)).T
        valid = lane_row + i * DH < length
        for b in range(i + 1):
            elapsed = col - mbuf[b : b + 1, :].astype(F32)
            allowed = valid & (lane_col <= lane_row) if b == i else valid
            heads = [head_of(k, j) for j in range(2)]
            terms = [jnp.full(elapsed.shape, bias_ref[h, 0], F32) for h in heads]
            for degree in range(1, bias_ref.shape[1]):
                reached = elapsed >= float(2**degree - 1)
                terms = [
                    jnp.where(reached, bias_ref[h, degree], t) for h, t in zip(heads, terms)
                ]
            for j in range(2):
                BI[j, i * DH : (i + 1) * DH, b * DH : (b + 1) * DH] = jnp.where(
                    allowed, terms[j], MASKED
                )

    relay_weights(1)

    @pl.when(k == p)
    def _():
        for i in range(3):
            wo_sends[i].start()

        @pl.when(wo_here)
        def _():
            pltpu.make_async_copy(wo_ref, WO.at[wo_slot], worecv.at[wo_slot]).start()

        @pl.when(jnp.logical_not(wo_here))
        def _():
            wo_sends[3].start()

    far_relay(0)
    near_relay(1)

    @pl.when(is_main)
    def _():
        x_wait(0, z)

    @pl.when(is_aux)
    def _():
        for b in range(n_seq):
            x_wait(0, b)

    for b in range(n_seq):
        NB[b * tok : (b + 1) * tok, :] = layer_norm(X[b].astype(F32), gin_ref[...]).astype(BF16)

    def forward(j):
        w_wait(me, j)
        w_wait(sib, j)
        for i in range(2):
            w_wait(2 * to + i, j)
            w_wait(2 * dn + i, j)
        PJ[j] = mm(NB[...], W[j], ((1,), (0,)))
        cols = slice(j * DH, (j + 1) * DH)
        GT[:, cols] = jax.nn.silu(PJ[j, :, :DH])
        for g in range(3):
            ACT[j, g] = jax.nn.silu(PJ[j, :, (1 + g) * DH : (2 + g) * DH]).astype(BF16)
        for i in range(n_seq):
            at, end = slice(i * tok, (i + 1) * tok), (i + 1) * tok
            scores = mm(ACT[j, 1, at], ACT[j, 2, :end], ((1,), (1,))) * scale + BI[j, at, :end]
            sig = jax.nn.sigmoid(scores)
            weight = (scores * sig).astype(BF16)
            WT[j, at, :end] = weight
            SL[j, at, :end] = sig * (1.0 + scores * (1.0 - sig))
            ATT[at, cols] = mm(weight, ACT[j, 0, :end], ((1,), (0,)))

    forward(0)
    far_relay(1)
    forward(1)

    @pl.when(is_main)
    def _():
        x_wait(1, z)

    @pl.when(is_aux)
    def _():
        for b in range(n_seq):
            x_wait(1, b)

    for j in range(2):
        arrived(WO.at[j], worecv.at[j])
    wo_heads = WO[...].reshape(2 * DH, width)
    c_rows = C[...].reshape(rows, width)
    DM[...] = mm(c_rows, wo_heads, ((1,), (1,)))

    gain = jnp.concatenate([gout_ref[:, lanes_of(head_of(k, j))] for j in range(2)], axis=1)
    pid = 2 * p + k
    own_width = 2 * DH
    for b in range(n_seq):
        at = slice(b * tok, (b + 1) * tok)
        att = ATT[at, :]
        g = DM[at, :] * GT[at, :] * gain
        mean_own = jnp.mean(att, axis=1, keepdims=True)
        off = att - mean_own
        packed = jnp.where(
            lane_col == 0,
            mean_own,
            jnp.where(
                lane_col == 1,
                jnp.sum(off * off, axis=1, keepdims=True),
                jnp.where(
                    lane_col == 2,
                    jnp.sum(g, axis=1, keepdims=True),
                    jnp.sum(g * off, axis=1, keepdims=True),
                ),
            ),
        )
        ST[pid, :, at] = packed.T[:8]
    st_peers = ((sib, z), (me, zp), (sib, zp))
    st_slots = (2 * p + 1 - k, 2 * (1 - p) + k, 2 * (1 - p) + 1 - k)
    st_sends = [
        remote(ST.at[pid], ST.at[pid], stsend.at[i], strecv.at[pid], peer)
        for i, peer in enumerate(st_peers)
    ]
    for copy in st_sends:
        copy.start()
    for slot in st_slots:
        arrived(ST.at[slot], strecv.at[slot])
    means = [ST[q, 0:1, :] for q in range(4)]
    mean = sum(means[1:], means[0]) / 4.0
    shifts = [m - mean for m in means]
    squares = sum(ST[q, 1:2, :] + own_width * shifts[q] * shifts[q] for q in range(4))
    rstd = lax.rsqrt(squares / width + EPS)
    g_mean = sum(ST[q, 2:3, :] for q in range(4)) / width
    g_dot = rstd * sum(ST[q, 3:4, :] + shifts[q] * ST[q, 2:3, :] for q in range(4)) / width
    table = jnp.concatenate([mean, rstd, g_mean, g_dot, mean, rstd, g_mean, g_dot], axis=0)
    for b in range(n_seq):
        at = slice(b * tok, (b + 1) * tok)
        turned = jnp.concatenate([table[:, at]] * (DH // 8), axis=0).T
        mean_c, rstd_c, g_mean_c, g_dot_c = [turned[:, q : q + 1] for q in range(4)]
        d_mix, gate = DM[at, :], GT[at, :]
        hat = (ATT[at, :] - mean_c) * rstd_c
        normed_att = hat * gain
        MR[at, :] = (normed_att * gate).astype(BF16)
        DG[at, :] = d_mix * normed_att
        DA[at, :] = (rstd_c * (d_mix * gate * gain - g_mean_c - hat * g_dot_c)).astype(BF16)

    def block_at(i):
        return (1 - ks) * (n_seq - 1 - i) + ks * i

    def pair_send(o, i):
        return remote(PB.at[o, i, 1 - k], SB.at[o, i], psend.at[o, i], precv.at[o, i], (sib, z))

    def cross_send(o, i):
        return remote(CS.at[o, i], FB.at[o, i], csend.at[o, i], crecv.at[o, i], (me, zp))

    def home_is_self(i):
        return is_main & (block_at(i) == z)

    def home_send(o, i):
        return remote(
            FIN.at[o, i], RO.at[o, k], osend.at[o, i], orecv.at[o, k], (main_dp, block_at(i))
        )

    last = n_seq - 1

    def sends_cross(i):
        return is_near if i == last else is_far

    def put_partial(o, i, part):
        PB[o, i, 0] = part[:half].astype(BF16)
        PB[o, i, 1] = part[half:].astype(BF16)

    def pair_sum(o, i):
        return PB[o, i, k].astype(F32) + SB[o, i].astype(F32)

    def cross(o):
        for i in range(n_seq):
            arrived(SB.at[o, i], precv.at[o, i])

            @pl.when(sends_cross(i))
            def _():
                CS[o, i] = pair_sum(o, i).astype(BF16)
                cross_send(o, i).start()

    def finish(o):
        for i in range(n_seq):

            @pl.when(jnp.logical_not(sends_cross(i)))
            def _():
                arrived(FB.at[o, i], crecv.at[o, i])
                FIN[o, i] = (pair_sum(o, i) + FB[o, i].astype(F32)).astype(BF16)
                if i < 2:
                    home_send(o, i).start()
                else:

                    @pl.when(home_is_self(i))
                    def _():
                        pltpu.make_async_copy(FIN.at[o, i], RO.at[o, k], orecv.at[o, k]).start()

                    @pl.when(jnp.logical_not(home_is_self(i)))
                    def _():
                        home_send(o, i).start()

    for i in range(n_seq):
        put_partial(0, i, mm(MR[rows_of(tok, block_at(i)), :], wo_heads, ((1,), (0,))))
        if i > 0:
            pair_send(0, i - 1).start()
    pair_send(0, last).start()

    def g_send(j):
        return remote(MW.at[j], WG.at[chip], gsend.at[j], grecv.at[chip], (2 * (2 * k + j) + p, z))

    def g_self(j):
        return (2 * k + j == chip) & (k == p)

    for j in range(2):
        MW[j] = mm(MR[:, j * DH : (j + 1) * DH], c_rows, ((0,), (0,))).astype(BF16)
    cross(0)
    for j in range(2):

        @pl.when(g_self(j))
        def _():
            pltpu.make_async_copy(MW.at[j], WG.at[chip], grecv.at[chip]).start()

        @pl.when(jnp.logical_not(g_self(j)))
        def _():
            g_send(j).start()

    is_root = k == p
    centre = 2 - k
    is_centre = z == centre

    def h_send():
        return remote(PS, PR, hsem.at[0], hsem.at[1], (me, lax.rem(z + 2, n_seq)))

    def t_send(i):
        return remote(TS, TR, tsend.at[i], trecv, (me, z - 1 + 2 * i))

    def plane_sum():
        @pl.when(is_root)
        def _():
            for c in range(n_dp // 2):
                arrived(WG.at[c], grecv.at[c])
            total = WG[0].astype(F32)
            for c in range(1, n_dp // 2):
                total = total + WG[c].astype(F32)
            PS[...] = total.astype(BF16)
            h_send().start()

    def plane_total():
        @pl.when(is_root)
        def _():
            arrived(PR, hsem.at[1])
            TS[...] = (PS[...].astype(F32) + PR[...].astype(F32)).astype(BF16)
            wg_ref[...] = TS[...].astype(F32)

            @pl.when(is_centre)
            def _():
                for i in range(2):
                    t_send(i).start()

    def backward(j):
        values, queries, keys = [ACT[j, g] for g in range(3)]
        cols = slice(j * DH, (j + 1) * DH)

        def put(group, start, end, grad):
            at = slice(group * DH, (group + 1) * DH)
            DP[j, start:end, at] = (grad * silu_slope(PJ[j, start:end, at])).astype(BF16)

        for i in reversed(range(n_seq)):
            start, end = i * tok, (i + 1) * tok
            d_att = DA[start:end, cols]
            d_weight = mm(d_att, values[:end], ((1,), (1,)))
            d_scores = (d_weight * SL[j, start:end, :end]).astype(BF16)
            put(2, start, end, mm(d_scores, keys[:end], ((1,), (0,))) * scale)
            k_part = mm(d_scores, queries[start:end], ((0,), (0,)))
            v_part = mm(WT[j, start:end, :end], d_att, ((0,), (0,)))
            if end == rows:
                KA[...] = k_part
                VA[...] = v_part
            else:
                KA[:end] += k_part
                VA[:end] += v_part
        put(0, 0, rows, DG[:, cols])
        put(1, 0, rows, VA[...])
        put(3, 0, rows, KA[...] * scale)

    backward(0)
    finish(0)
    plane_sum()
    backward(1)
    for i in range(n_seq):
        at = rows_of(tok, block_at(i))
        put_partial(
            1, i, mm(DP[0, at, :], W[0], ((1,), (1,))) + mm(DP[1, at, :], W[1], ((1,), (1,)))
        )
        if i > 0:
            pair_send(1, i - 1).start()
    pair_send(1, last).start()
    cross(1)
    plane_total()
    finish(1)

    for h in range(2):
        arrived(RO.at[0, h], orecv.at[0, h])
    wide = x_ref[...].astype(F32)
    mixed_ref[...] = (wide + RO[0].reshape(tok, width).astype(F32)).astype(BF16)

    @pl.when(jnp.logical_not(is_root))
    def _():
        arrived(TR, trecv)
        wg_ref[...] = TR[...].astype(F32)

    average = jnp.mean(wide, axis=-1, keepdims=True)
    centred = wide - average
    inv = lax.rsqrt(jnp.mean(centred * centred, axis=-1, keepdims=True) + EPS)
    hat = centred * inv
    for h in range(2):
        arrived(RO.at[1, h], orecv.at[1, h])
    grad = RO[1].reshape(tok, width).astype(F32) * gin_ref[...]
    back = inv * (
        grad
        - jnp.mean(grad, axis=-1, keepdims=True)
        - hat * jnp.mean(grad * hat, axis=-1, keepdims=True)
    )
    grad_ref[...] = (c_ref[...].astype(F32) + back).astype(BF16)

    for j in range(2):
        for index in range(5):
            block = w_piece(me, j)
            remote(block, block, wsend.at[index, j], wrecv.at[me, j], (sib, z)).wait_send()
        for i in range(2):
            w_relay(i, j).wait_send()

        @pl.when(jnp.logical_not(g_self(j)))
        def _():
            g_send(j).wait_send()

    for a in range(2):
        z_send(a).wait_send()

        @pl.when(is_main)
        def _():
            share(a, None).wait_send()
            share(a, zp).wait_send()
            for i in range(2):
                share(a, foreign[i]).wait_send()

        @pl.when(is_main & is_near)
        def _():
            for i in range(2):
                to_far(a, i).wait_send()

    @pl.when(is_main)
    def _():
        meta_send().wait_send()

    @pl.when(k == p)
    def _():
        for i in range(3):
            wo_sends[i].wait_send()

        @pl.when(jnp.logical_not(wo_here))
        def _():
            wo_sends[3].wait_send()

    for copy in st_sends:
        copy.wait_send()

    @pl.when(is_root)
    def _():
        h_send().wait_send()

        @pl.when(is_centre)
        def _():
            for i in range(2):
                t_send(i).wait_send()

    for o in range(2):
        for i in range(n_seq):
            pair_send(o, i).wait_send()

            @pl.when(sends_cross(i))
            def _():
                cross_send(o, i).wait_send()

            @pl.when(jnp.logical_not(sends_cross(i)) & jnp.logical_not(home_is_self(i)))
            def _():
                home_send(o, i).wait_send()


def column_parallel(
    n_dp, n_seq, tokens, cotangent, stamps, lengths, w_qkvu, w_out, gain_in, gain_out, bias_table
):
    tok, width = tokens.shape[1:]
    rows = tok * n_seq
    meta = jnp.concatenate([stamps.reshape(-1, DH), jnp.broadcast_to(lengths[:, None], (4, DH))])
    dma = pltpu.SemaphoreType.DMA
    sds = jax.ShapeDtypeStruct
    smem = pl.BlockSpec(memory_space=pltpu.SMEM)

    def vb(*shape):
        return pltpu.VMEM(shape, BF16)

    def vf(*shape):
        return pltpu.VMEM(shape, F32)

    half = tok // 2
    mixed, grad, w_grad = pl.pallas_call(
        lambda *refs: column_kernel(n_dp, n_seq, *refs),
        out_shape=(sds((tok, width), BF16), sds((tok, width), BF16), sds(w_out.shape, F32)),
        in_specs=[VM] * 7 + [smem],
        out_specs=[VM] * 3,
        scratch_shapes=[
            vb(2, width, 4 * DH),
            vb(n_seq, tok, width),
            vb(n_seq, tok, width),
            vb(2, DH, width),
            pltpu.VMEM(meta.shape, jnp.int32),
            vb(rows, width),
            vf(2, rows, rows),
            vf(2, rows, 4 * DH),
            vf(rows, 2 * DH),
            vb(2, 3, rows, DH),
            vf(rows, 2 * DH),
            vb(2, rows, rows),
            vf(2, rows, rows),
            vf(rows, 2 * DH),
            vf(rows, 2 * DH),
            vb(rows, 2 * DH),
            vb(2, rows, 4 * DH),
            vb(rows, 2 * DH),
            vf(rows, DH),
            vf(rows, DH),
            vf(4, 8, rows),
            vb(2, DH, width),
            vb(n_dp // 2, DH, width),
            vb(DH, width),
            vb(DH, width),
            vb(DH, width),
            vb(DH, width),
            vb(2, n_seq, 2, half, width),
            vb(2, n_seq, half, width),
            vb(2, n_seq, half, width),
            vb(2, n_seq, half, width),
            vb(2, n_seq, half, width),
            vb(2, 2, half, width),
            dma((5, 2)),
            dma((2, 2)),
            dma((n_dp, 2)),
            dma((2,)),
            dma((2, n_seq)),
            dma((2, 2)),
            dma((2, n_seq)),
            dma((4,)),
            dma((2,)),
            dma((2,)),
            dma((3,)),
            dma((4,)),
            dma((2,)),
            dma((n_dp // 2,)),
            dma((2,)),
            dma((2,)),
            dma,
            dma((2, n_seq)),
            dma((2, n_seq)),
            dma((2, n_seq)),
            dma((2, n_seq)),
            dma((2, n_seq)),
            dma((2, 2)),
        ],
        compiler_params=pltpu.CompilerParams(has_side_effects=True),
        name="column",
    )(
        w_qkvu, tokens[0], cotangent[0], w_out, meta, gain_in[None], gain_out[None], bias_table
    )
    return (mixed[None], grad[None], w_grad)


def solution(mesh):
    n_dp, n_seq = mesh.shape["dp"], mesh.shape["seq"]

    def body(*args):
        tokens, stamps, w_out = args[0], args[2], args[5]
        mesh_fits = n_seq == 4 and n_dp == 2 * n_seq and n_dp == H
        sizes_fit = w_out.shape[0] == DH and tokens.shape[1] == DH
        if mesh_fits and sizes_fit and stamps.shape == (1, n_seq * DH):
            return column_parallel(n_dp, n_seq, *args)
        return per_device(*args)

    return jax.shard_map(
        body,
        mesh=mesh,
        in_specs=(
            P("dp", "seq", None),
            P("dp", "seq", None),
            P("dp", None),
            P("dp"),
            P("dp", None),
            P("dp", None),
            P(),
            P(),
            P(),
        ),
        out_specs=(P("dp", "seq", None), P("dp", "seq", None), P("dp", None)),
        check_vma=False,
    )
```

```python
import jax
import jax.numpy as jnp
from jax import lax
from jax.experimental import pallas as pl
from jax.experimental.pallas import tpu as pltpu
from jax.sharding import PartitionSpec as P

H = 8
DH = 128


EPS = 1e-05


def layer_norm(values, gain):
    average = jnp.mean(values, axis=-1, keepdims=True)
    centred = values - average
    variance = jnp.mean(centred * centred, axis=-1, keepdims=True)
    return centred * lax.rsqrt(variance + EPS) * gain


def silu_slope(values):
    sigmoid_v = jax.nn.sigmoid(values)
    return sigmoid_v * (1.0 + values * (1.0 - sigmoid_v))


def time_bias(bias_table, stamps_q, stamps_k):
    elapsed = stamps_q[:, None] - stamps_k[None, :]
    bucket = jnp.zeros(elapsed.shape, jnp.int32)
    for degree in range(1, bias_table.shape[1]):
        bucket = bucket + (elapsed >= 2**degree - 1).astype(jnp.int32)
    levels = jnp.arange(bias_table.shape[1], dtype=jnp.int32)
    one_hot = (bucket[:, :, None] == levels[None, None, :]).astype(jnp.float32)
    return jnp.einsum(
        "qkb,hb->hqk",
        one_hot,
        bias_table,
        precision=lax.Precision.HIGHEST,
        preferred_element_type=jnp.float32,
    )


def pair_terms(
    q_heads, d_heads, stamps_q, pos_q, k_heads, v_heads, stamps_k, pos_k, length, bias_table, scale
):
    scores = (
        jnp.einsum("qhd,khd->hqk", q_heads, k_heads, preferred_element_type=jnp.float32) * scale
    )
    scores = scores + time_bias(bias_table, stamps_q, stamps_k)
    allowed = (
        (pos_k[None, :] <= pos_q[:, None]) & (pos_k[None, :] < length) & (pos_q[:, None] < length)
    )
    weight = jnp.where(allowed[None], jax.nn.silu(scores), 0.0).astype(jnp.bfloat16)
    if d_heads is None:
        return (weight, None)
    d_weight = jnp.einsum("qhd,khd->hqk", d_heads, v_heads, preferred_element_type=jnp.float32)
    d_scores = jnp.where(allowed[None], d_weight * silu_slope(scores), 0.0).astype(jnp.bfloat16)
    return (weight, d_scores)


def per_device(tokens, cotangent, stamps, lengths, w_qkvu, w_out, gain_in, gain_out, bias_table):
    rows = tokens[0]
    cot_rows = cotangent[0]
    tok_count = rows.shape[0]
    feature_width = rows.shape[1]
    seq_count = lax.axis_size("seq")
    total_rows = tok_count * seq_count
    first_row = lax.axis_index("seq") * tok_count
    length = lengths[0]
    stamp_all = stamps[0]
    pos_own = first_row + jnp.arange(tok_count, dtype=jnp.int32)
    stamp_own = lax.dynamic_slice_in_dim(stamp_all, first_row, tok_count)
    scale = DH ** (-0.5)
    block_rows = min(512, total_rows)
    block_count = total_rows // block_rows
    w_full, w_out_full = (
        lax.all_gather(w_qkvu, "dp", axis=0, tiled=True),
        lax.all_gather(w_out, "dp", axis=0, tiled=True),
    )
    wide_rows = rows.astype(jnp.float32)
    normed = layer_norm(wide_rows, gain_in).astype(jnp.bfloat16)
    projected = jnp.dot(normed, w_full, preferred_element_type=jnp.float32)
    activated = jax.nn.silu(projected)
    gate_u = activated[:, :feature_width]
    values_own = activated[:, feature_width : 2 * feature_width].astype(jnp.bfloat16)
    queries_own = activated[:, 2 * feature_width : 3 * feature_width].astype(jnp.bfloat16)
    keys_own = activated[:, 3 * feature_width :].astype(jnp.bfloat16)
    keys_all, values_all = (
        lax.all_gather(keys_own, "seq", axis=0, tiled=True),
        lax.all_gather(values_own, "seq", axis=0, tiled=True),
    )
    q_heads = queries_own.reshape(tok_count, H, DH)

    def key_block(start):
        k_heads = lax.dynamic_slice_in_dim(keys_all, start, block_rows).reshape(block_rows, H, DH)
        v_heads = lax.dynamic_slice_in_dim(values_all, start, block_rows).reshape(block_rows, H, DH)
        stamps_k = lax.dynamic_slice_in_dim(stamp_all, start, block_rows)
        pos_k = start + jnp.arange(block_rows, dtype=jnp.int32)
        return (k_heads, v_heads, stamps_k, pos_k)

    def guarded(active, action, state):
        return lax.cond(active, action, lambda same: same, state)

    def reaches(start):
        return (start <= first_row + tok_count - 1) & (start < length) & (first_row < length)

    def forward_step(block_idx, totals):
        start = block_idx * block_rows

        def forward_compute(totals):
            k_heads, v_heads, stamps_k, pos_k = key_block(start)
            weight, unused = pair_terms(
                q_heads,
                None,
                stamp_own,
                pos_own,
                k_heads,
                v_heads,
                stamps_k,
                pos_k,
                length,
                bias_table,
                scale,
            )
            return totals + jnp.einsum(
                "hqk,khd->qhd", weight, v_heads, preferred_element_type=jnp.float32
            )

        return guarded(reaches(start), forward_compute, totals)

    attended = lax.fori_loop(
        0, block_count, forward_step, jnp.zeros((tok_count, H, DH), jnp.float32)
    )
    attended = attended.reshape(tok_count, feature_width)
    normed_att, norm_back = jax.vjp(lambda values: layer_norm(values, gain_out), attended)
    mixed_rows = (normed_att * gate_u).astype(jnp.bfloat16)
    mixed = (
        wide_rows + jnp.dot(mixed_rows, w_out_full, preferred_element_type=jnp.float32)
    ).astype(jnp.bfloat16)
    grad_part = lax.psum_scatter(
        jnp.einsum("tr,tc->rc", mixed_rows, cot_rows, preferred_element_type=jnp.float32).astype(
            jnp.bfloat16
        ),
        "dp",
        scatter_dimension=0,
        tiled=True,
    )
    w_grad = lax.psum(grad_part, "seq").astype(jnp.float32)
    d_mix = jnp.einsum("tc,rc->tr", cot_rows, w_out_full, preferred_element_type=jnp.float32)
    d_gate = d_mix * normed_att
    d_att = norm_back(d_mix * gate_u)[0].astype(jnp.bfloat16)
    d_heads = d_att.reshape(tok_count, H, DH)

    def backward_step():

        def step(block_idx, state_pair):
            start = block_idx * block_rows

            def step_compute(state_pair):
                q_grad, key_terms = state_pair
                k_heads, v_heads, stamps_k, pos_k = key_block(start)
                weight, d_scores = pair_terms(
                    q_heads,
                    d_heads,
                    stamp_own,
                    pos_own,
                    k_heads,
                    v_heads,
                    stamps_k,
                    pos_k,
                    length,
                    bias_table,
                    scale,
                )
                q_grad = (
                    q_grad
                    + jnp.einsum(
                        "hqk,khd->qhd", d_scores, k_heads, preferred_element_type=jnp.float32
                    )
                    * scale
                )
                k_grad = (
                    jnp.einsum(
                        "hqk,qhd->khd", d_scores, q_heads, preferred_element_type=jnp.float32
                    )
                    * scale
                )
                v_grad = jnp.einsum(
                    "hqk,qhd->khd", weight, d_heads, preferred_element_type=jnp.float32
                )
                joined = jnp.concatenate(
                    [
                        k_grad.reshape(block_rows, feature_width),
                        v_grad.reshape(block_rows, feature_width),
                    ],
                    axis=1,
                )
                key_terms = lax.dynamic_update_slice_in_dim(key_terms, joined, start, 0)
                return (q_grad, key_terms)

            return guarded(reaches(start), step_compute, state_pair)

        return step

    q_start = jnp.zeros((tok_count, H, DH), jnp.float32)
    term_start = jnp.zeros((total_rows, 2 * feature_width), jnp.float32)
    q_grad, key_terms = lax.fori_loop(0, block_count, backward_step(), (q_start, term_start))
    key_grads = lax.psum_scatter(
        key_terms.astype(jnp.bfloat16), "seq", scatter_dimension=0, tiled=True
    ).astype(jnp.float32)
    d_act = jnp.concatenate(
        [
            d_gate,
            key_grads[:, feature_width:],
            q_grad.reshape(tok_count, feature_width),
            key_grads[:, :feature_width],
        ],
        axis=1,
    )
    d_proj = (d_act * silu_slope(projected)).astype(jnp.bfloat16)
    d_normed = jnp.einsum("tf,df->td", d_proj, w_full, preferred_element_type=jnp.float32)
    unused_rows, in_back = jax.vjp(lambda values: layer_norm(values, gain_in), wide_rows)
    input_grad = (cot_rows.astype(jnp.float32) + in_back(d_normed)[0]).astype(jnp.bfloat16)
    return (mixed[None], input_grad[None], w_grad)


MESH = pl.DeviceIdType.MESH
VM = pl.BlockSpec(memory_space=pltpu.VMEM)
F32 = jnp.float32
BF16 = jnp.bfloat16
MASKED = -1e30


def mm(a, b, dims):
    return lax.dot_general(a, b, (dims, ((), ())), preferred_element_type=F32)


def remote(src, dst, send_sem, recv_sem, target):
    return pltpu.make_async_remote_copy(
        src_ref=src,
        dst_ref=dst,
        send_sem=send_sem,
        recv_sem=recv_sem,
        device_id=target,
        device_id_type=MESH,
    )


def arrived(dst, sem):
    pltpu.make_async_copy(dst, dst, sem).wait()


def column_kernel(
    n_dp, n_seq, w_hbm, x_hbm, c_hbm, wo_hbm, stamps_hbm, length_ref, gin_hbm, gout_hbm, bias_hbm,
    mixed_ref, grad_ref, wg_ref,
    w_ref, x_ref, c_ref, wo_ref, stamps_ref, gin_ref, gout_ref, bias_ref, meta_ref,
    W, X, C, WO, mbuf, NB, BI, PJ, GT, ACT, ATT, WT, SL, DM, DG, DA, DP, MR, KA, VA, SA, SG, TB,
    MW, WG, PS, PR, TS, TR, MA, MB, PB, SB, CS, FB, FIN, RO,
    lsem, wsend, wrelay, wrecv, zsend, ssend, farsend, xrecv, wosend, worecv, msem,
    sasend, sarecv, sgsend, sgrecv, gsend, grecv, hsem, tsend, trecv, psend, precv, csend, crecv, osend, orecv,
):
    me = lax.axis_index("dp")
    z = lax.axis_index("seq")
    tok, width = x_ref.shape
    rows = tok * n_seq
    half = tok // 2
    n_heads = n_dp
    scale = DH ** (-0.5)
    chip, k = me // 2, me % 2
    cy, cx = chip // 2, chip % 2
    xn, yn = 2 * cy + (1 - cx), 2 * (1 - cy) + cx
    dn = 2 * (1 - cy) + (1 - cx)
    sib = 2 * chip + (1 - k)
    p, ks = z % 2, z // 2
    near, far = 1 + ks, (n_seq - 1) * ks
    zp = near + far - z
    is_near, is_far = z == near, z == far
    is_main = k == ks
    is_aux = jnp.logical_not(is_main)
    main_dp = 2 * chip + ks

    def head_of(core, j):
        return 4 * core + 2 * j + p

    def rows_of(ref_rows, index):
        return pl.ds(pl.multiple_of(index * ref_rows, ref_rows), ref_rows)

    def lanes_of(index):
        return pl.ds(pl.multiple_of(index * DH, DH), DH)

    def w_copies(core, j, make):
        return [
            make(
                w_ref.at[:, lanes_of(g * n_heads + head_of(core, j))],
                W.at[j, rows_of(tok, me), slice(g * DH, (g + 1) * DH)],
            )
            for g in range(4)
        ]

    w_targets = ((xn, 0, 1), (yn, 1, 4), (chip, 1 - k, 0), (xn, 1, 2), (yn, 0, 3))

    def w_start(j):
        for where, core, index in w_targets:
            for copy in w_copies(
                core, j,
                lambda s, d: remote(s, d, wsend.at[index, j], wrecv.at[me, j], (2 * where + core, z)),
            ):
                copy.start()

    def w_piece(src, j):
        return W.at[j, rows_of(tok, src)]

    via, to = (1 - k) * xn + k * yn, (1 - k) * yn + k * xn

    def w_relay(i, j):
        src = 2 * via + i
        block = w_piece(src, j)
        return remote(block, block, wrelay.at[i, j], wrecv.at[src, j], (2 * to + k, z))

    def w_wait(src, j):
        arrived(w_piece(src, j), wrecv.at[src, j])

    ins, outs = (x_ref, c_ref), (X, C)
    z_to = jnp.where(is_main, zp, 1 + k)

    def z_send(a):
        return remote(ins[a], outs[a].at[z], zsend.at[a], xrecv.at[a, z], (me, z_to))

    def own_copy(a):
        return pltpu.make_async_copy(ins[a], outs[a].at[z], xrecv.at[a, z])

    def share(a, b):
        block = ins[a] if b is None else outs[a].at[b]
        at = z if b is None else b
        return remote(block, outs[a].at[at], ssend.at[a, at], xrecv.at[a, at], (sib, z))

    foreign = (2 * (1 - ks), 2 * (1 - ks) + 1)

    def to_far(a, i):
        block = outs[a].at[foreign[i]]
        return remote(block, block, farsend.at[a, i], xrecv.at[a, foreign[i]], (me, far))

    def x_wait(a, b):
        arrived(outs[a].at[b], xrecv.at[a, b])

    def meta_send():
        return remote(meta_ref, mbuf, msem.at[0], msem.at[1], (sib, z))

    wo_core, wo_slot = chip // 2, chip % 2
    wo_here = wo_core == k
    wo_sends = [
        remote(wo_ref, WO.at[wo_slot], wosend.at[i], worecv.at[wo_slot], (2 * where + wo_core, z))
        for i, where in enumerate((xn, yn, dn, chip))
    ]

    loads = [
        pltpu.make_async_copy(src, dst, lsem.at[i])
        for i, (src, dst) in enumerate(
            (
                (stamps_hbm, stamps_ref), (w_hbm, w_ref), (x_hbm, x_ref), (c_hbm, c_ref),
                (wo_hbm, wo_ref), (gin_hbm, gin_ref), (gout_hbm, gout_ref), (bias_hbm, bias_ref),
            )
        )
    ]
    barrier = pltpu.get_barrier_semaphore()
    peers = [(lax.rem(me + step, n_dp), z) for step in range(1, n_dp)]
    for step in range(1, n_seq):
        peers += [(me, lax.rem(z + step, n_seq)), (sib, lax.rem(z + step, n_seq))]
    for peer in peers:
        pl.semaphore_signal(barrier, inc=1, device_id=peer, device_id_type=MESH)
    for load in loads:
        load.start()
    loads[0].wait()
    meta_ref[0:1, :] = stamps_ref[...]
    meta_ref[1:2, :] = jnp.full(stamps_ref.shape, length_ref[0], jnp.int32)
    for load in loads[1:]:
        load.wait()
    pl.semaphore_wait(barrier, len(peers))
    @pl.when(is_main)
    def _():
        pltpu.make_async_copy(meta_ref, mbuf, msem.at[1]).start()
        meta_send().start()

    w_start(0)
    z_send(0).start()

    @pl.when(is_main)
    def _():
        own_copy(0).start()
        share(0, None).start()

    z_send(1).start()

    @pl.when(is_main)
    def _():
        own_copy(1).start()
        share(1, None).start()

    for j in range(2):
        for copy in w_copies(k, j, lambda s, d: pltpu.make_async_copy(s, d, wrecv.at[me, j])):
            copy.start()

    def relay_weights(j):
        for i in range(2):
            w_wait(2 * via + i, j)
            w_relay(i, j).start()

    def near_relay(a):
        @pl.when(is_main)
        def _():
            x_wait(a, zp)
            share(a, zp).start()

        @pl.when(is_main & is_near)
        def _():
            for i in range(2):
                x_wait(a, foreign[i])
                to_far(a, i).start()
                share(a, foreign[i]).start()

    def far_relay(a):
        @pl.when(is_main & is_far)
        def _():
            for i in range(2):
                x_wait(a, foreign[i])
                share(a, foreign[i]).start()

    relay_weights(0)
    w_start(1)
    near_relay(0)

    arrived(mbuf, msem.at[1])
    lane_row = lax.broadcasted_iota(jnp.int32, (DH, DH), 0)
    lane_col = lax.broadcasted_iota(jnp.int32, (DH, DH), 1)
    length = mbuf[1:2, :DH]
    for i in range(n_seq):
        col = jnp.broadcast_to(mbuf[0:1, i * DH : (i + 1) * DH].astype(F32), (DH, DH)).T
        valid = lane_row + i * DH < length
        for b in range(i + 1):
            elapsed = col - mbuf[0:1, b * DH : (b + 1) * DH].astype(F32)
            allowed = valid & (lane_col <= lane_row) if b == i else valid
            heads = [head_of(k, j) for j in range(2)]
            terms = [jnp.full(elapsed.shape, bias_ref[h, 0], F32) for h in heads]
            for degree in range(1, bias_ref.shape[1]):
                reached = elapsed >= float(2**degree - 1)
                terms = [
                    jnp.where(reached, bias_ref[h, degree], t) for h, t in zip(heads, terms)
                ]
            for j in range(2):
                BI[j, i * DH : (i + 1) * DH, b * DH : (b + 1) * DH] = jnp.where(
                    allowed, terms[j], MASKED
                )

    near_relay(1)
    relay_weights(1)

    @pl.when(k == p)
    def _():
        for i in range(3):
            wo_sends[i].start()

        @pl.when(wo_here)
        def _():
            pltpu.make_async_copy(wo_ref, WO.at[wo_slot], worecv.at[wo_slot]).start()

        @pl.when(jnp.logical_not(wo_here))
        def _():
            wo_sends[3].start()

    far_relay(0)

    @pl.when(is_main)
    def _():
        x_wait(0, z)

    @pl.when(is_aux)
    def _():
        for b in range(n_seq):
            x_wait(0, b)

    for b in range(n_seq):
        NB[b * tok : (b + 1) * tok, :] = layer_norm(X[b].astype(F32), gin_ref[...]).astype(BF16)

    def forward(j):
        w_wait(me, j)
        w_wait(sib, j)
        for i in range(2):
            w_wait(2 * to + i, j)
            w_wait(2 * dn + i, j)
        PJ[j] = mm(NB[...], W[j], ((1,), (0,)))
        cols = slice(j * DH, (j + 1) * DH)
        GT[:, cols] = jax.nn.silu(PJ[j, :, :DH])
        for g in range(3):
            ACT[j, g] = jax.nn.silu(PJ[j, :, (1 + g) * DH : (2 + g) * DH]).astype(BF16)
        for i in range(n_seq):
            at, end = slice(i * tok, (i + 1) * tok), (i + 1) * tok
            scores = mm(ACT[j, 1, at], ACT[j, 2, :end], ((1,), (1,))) * scale + BI[j, at, :end]
            sig = jax.nn.sigmoid(scores)
            weight = (scores * sig).astype(BF16)
            WT[j, at, :end] = weight
            SL[j, at, :end] = sig * (1.0 + scores * (1.0 - sig))
            ATT[at, cols] = mm(weight, ACT[j, 0, :end], ((1,), (0,)))

    forward(0)
    forward(1)

    gain = jnp.concatenate([gout_ref[:, lanes_of(head_of(k, j))] for j in range(2)], axis=1)
    pid = 2 * p + k
    own_width = 2 * DH
    st_peers = ((sib, z), (me, zp), (sib, zp))
    st_slots = (2 * p + 1 - k, 2 * (1 - p) + k, 2 * (1 - p) + 1 - k)

    def stat_sends(ref, send_sem, recv_sem):
        return [
            remote(ref.at[pid], ref.at[pid], send_sem.at[i], recv_sem.at[pid], peer)
            for i, peer in enumerate(st_peers)
        ]

    def put_stats(ref, at, first, second):
        ref[pid, :, at] = jnp.where(lane_col == 0, first, second).T[:8]

    for b in range(n_seq):
        at = slice(b * tok, (b + 1) * tok)
        att = ATT[at, :]
        mean_own = jnp.mean(att, axis=1, keepdims=True)
        off = att - mean_own
        put_stats(SA, at, mean_own, jnp.sum(off * off, axis=1, keepdims=True))
    for copy in stat_sends(SA, sasend, sarecv):
        copy.start()
    far_relay(1)
    for j in range(2):
        arrived(WO.at[j], worecv.at[j])
    wo_heads = WO[...].reshape(2 * DH, width)
    @pl.when(is_main)
    def _():
        x_wait(1, z)

    @pl.when(is_aux)
    def _():
        for b in range(n_seq):
            x_wait(1, b)

    c_rows = C[...].reshape(rows, width)
    DM[...] = mm(c_rows, wo_heads, ((1,), (1,)))
    for b in range(n_seq):
        at = slice(b * tok, (b + 1) * tok)
        att = ATT[at, :]
        g = DM[at, :] * GT[at, :] * gain
        off = att - jnp.mean(att, axis=1, keepdims=True)
        put_stats(
            SG, at, jnp.sum(g, axis=1, keepdims=True), jnp.sum(g * off, axis=1, keepdims=True)
        )
    for copy in stat_sends(SG, sgsend, sgrecv):
        copy.start()
    for slot in st_slots:
        arrived(SA.at[slot], sarecv.at[slot])
    means = [SA[q, 0:1, :] for q in range(4)]
    mean = sum(means[1:], means[0]) / 4.0
    shifts = [m - mean for m in means]
    squares = sum(SA[q, 1:2, :] + own_width * shifts[q] * shifts[q] for q in range(4))
    rstd = lax.rsqrt(squares / width + EPS)
    TB[...] = jnp.concatenate([mean, rstd] * 4, axis=0)

    def turned(at):
        return jnp.concatenate([TB[:, at]] * (DH // 8), axis=0).T

    def block_at(i):
        return (1 - ks) * (n_seq - 1 - i) + ks * i

    def pair_send(o, i):
        return remote(PB.at[o, i, 1 - k], SB.at[o, i], psend.at[o, i], precv.at[o, i], (sib, z))

    def cross_send(o, i):
        return remote(CS.at[o, i], FB.at[o, i], csend.at[o, i], crecv.at[o, i], (me, zp))

    def home_is_self(i):
        return is_main & (block_at(i) == z)

    def home_send(o, i):
        return remote(
            FIN.at[o, i], RO.at[o, k], osend.at[o, i], orecv.at[o, k], (main_dp, block_at(i))
        )

    last = n_seq - 1

    def sends_cross(i):
        return is_near if i == last else is_far

    def put_partial(o, i, part):
        PB[o, i, 0] = part[:half].astype(BF16)
        PB[o, i, 1] = part[half:].astype(BF16)

    def pair_sum(o, i):
        return PB[o, i, k].astype(F32) + SB[o, i].astype(F32)

    def cross(o):
        for i in range(n_seq):
            arrived(SB.at[o, i], precv.at[o, i])

            @pl.when(sends_cross(i))
            def _():
                CS[o, i] = pair_sum(o, i).astype(BF16)
                cross_send(o, i).start()

    def finish(o, which):
        for i in which:

            @pl.when(jnp.logical_not(sends_cross(i)))
            def _():
                arrived(FB.at[o, i], crecv.at[o, i])
                FIN[o, i] = (pair_sum(o, i) + FB[o, i].astype(F32)).astype(BF16)
                if i < 2:
                    home_send(o, i).start()
                else:

                    @pl.when(home_is_self(i))
                    def _():
                        pltpu.make_async_copy(FIN.at[o, i], RO.at[o, k], orecv.at[o, k]).start()

                    @pl.when(jnp.logical_not(home_is_self(i)))
                    def _():
                        home_send(o, i).start()

    for i in range(n_seq):
        at = rows_of(tok, block_at(i))
        columns = turned(at)
        hat = (ATT[at, :] - columns[:, 0:1]) * columns[:, 1:2]
        ATT[at, :] = hat
        mixed_rows = (hat * gain * GT[at, :]).astype(BF16)
        MR[at, :] = mixed_rows
        put_partial(0, i, mm(mixed_rows, wo_heads, ((1,), (0,))))
        if i > 0:
            pair_send(0, i - 1).start()
    pair_send(0, last).start()
    cross(0)

    def g_send(j):
        return remote(MW.at[j], WG.at[chip], gsend.at[j], grecv.at[chip], (2 * (2 * k + j) + p, z))

    def g_self(j):
        return (2 * k + j == chip) & (k == p)

    for j in range(2):
        MW[j] = mm(MR[:, j * DH : (j + 1) * DH], c_rows, ((0,), (0,))).astype(BF16)
    for j in range(2):

        @pl.when(g_self(j))
        def _():
            pltpu.make_async_copy(MW.at[j], WG.at[chip], grecv.at[chip]).start()

        @pl.when(jnp.logical_not(g_self(j)))
        def _():
            g_send(j).start()

    is_root = k == p
    far_root, near_root, middle, edge = (n_seq - 1) * k, 2 - k, 1 + k, (n_seq - 1) * (1 - k)

    def h_send(dst, recv):
        return remote(PS, dst, hsem.at[0], hsem.at[recv], (me, middle))

    def h_relay(src, i, to):
        return remote(src, PR, tsend.at[i], hsem.at[3], (me, to))

    def t_send():
        return remote(TS, TR, tsend.at[2], trecv, (me, edge))

    def plane_sum():
        @pl.when(is_root)
        def _():
            for c in range(n_dp // 2):
                arrived(WG.at[c], grecv.at[c])
            total = WG[0].astype(F32)
            for c in range(1, n_dp // 2):
                total = total + WG[c].astype(F32)
            PS[...] = total.astype(BF16)

            @pl.when(z == far_root)
            def _():
                h_send(MA, 1).start()

            @pl.when(z == near_root)
            def _():
                h_send(MB, 2).start()

    def pass_sums():
        @pl.when(z == middle)
        def _():
            arrived(MB, hsem.at[2])
            h_relay(MB, 0, far_root).start()
            arrived(MA, hsem.at[1])
            h_relay(MA, 1, near_root).start()
            wg_ref[...] = (MA[...].astype(F32) + MB[...].astype(F32)).astype(BF16)

    def root_total():
        arrived(PR, hsem.at[3])
        TS[...] = (PS[...].astype(F32) + PR[...].astype(F32)).astype(BF16)
        wg_ref[...] = TS[...]

    def near_total():
        @pl.when(z == near_root)
        def _():
            root_total()
            t_send().start()

    def outer_total():
        @pl.when(z == far_root)
        def _():
            root_total()

        @pl.when(z == edge)
        def _():
            arrived(TR, trecv)
            wg_ref[...] = TR[...]

    def backward(j):
        values, queries, keys = [ACT[j, g] for g in range(3)]
        cols = slice(j * DH, (j + 1) * DH)

        def put(group, start, end, grad):
            at = slice(group * DH, (group + 1) * DH)
            DP[j, start:end, at] = (grad * silu_slope(PJ[j, start:end, at])).astype(BF16)

        for i in reversed(range(n_seq)):
            start, end = i * tok, (i + 1) * tok
            d_att = DA[start:end, cols]
            d_weight = mm(d_att, values[:end], ((1,), (1,)))
            d_scores = (d_weight * SL[j, start:end, :end]).astype(BF16)
            put(2, start, end, mm(d_scores, keys[:end], ((1,), (0,))) * scale)
            k_part = mm(d_scores, queries[start:end], ((0,), (0,)))
            v_part = mm(WT[j, start:end, :end], d_att, ((0,), (0,)))
            if end == rows:
                KA[...] = k_part
                VA[...] = v_part
            else:
                KA[:end] += k_part
                VA[:end] += v_part
        put(0, 0, rows, DG[:, cols])
        put(1, 0, rows, VA[...])
        put(3, 0, rows, KA[...] * scale)

    for slot in st_slots:
        arrived(SG.at[slot], sgrecv.at[slot])
    g_mean = sum(SG[q, 0:1, :] for q in range(4)) / width
    g_dot = rstd * sum(SG[q, 1:2, :] + shifts[q] * SG[q, 0:1, :] for q in range(4)) / width
    TB[...] = jnp.concatenate([rstd, g_mean, g_dot, rstd] * 2, axis=0)
    for b in range(n_seq):
        at = slice(b * tok, (b + 1) * tok)
        columns = turned(at)
        d_mix, hat = DM[at, :], ATT[at, :]
        DG[at, :] = d_mix * (hat * gain)
        g = d_mix * GT[at, :] * gain
        DA[at, :] = (
            columns[:, 0:1] * (g - columns[:, 1:2] - hat * columns[:, 2:3])
        ).astype(BF16)

    backward(0)
    backward(1)
    for i in range(n_seq):
        at = rows_of(tok, block_at(i))
        put_partial(
            1, i, mm(DP[0, at, :], W[0], ((1,), (1,))) + mm(DP[1, at, :], W[1], ((1,), (1,)))
        )
        if i > 0:
            pair_send(1, i - 1).start()
            finish(0, (i - 1,))
    pair_send(1, last).start()
    plane_sum()
    cross(1)
    finish(0, (last,))
    pass_sums()
    finish(1, (0,))
    near_total()
    finish(1, (1, 2, 3))

    for h in range(2):
        arrived(RO.at[0, h], orecv.at[0, h])
    wide = x_ref[...].astype(F32)
    mixed_ref[...] = (wide + RO[0].reshape(tok, width).astype(F32)).astype(BF16)

    average = jnp.mean(wide, axis=-1, keepdims=True)
    centred = wide - average
    inv = lax.rsqrt(jnp.mean(centred * centred, axis=-1, keepdims=True) + EPS)
    hat = centred * inv
    outer_total()
    for h in range(2):
        arrived(RO.at[1, h], orecv.at[1, h])
    grad = RO[1].reshape(tok, width).astype(F32) * gin_ref[...]
    back = inv * (
        grad
        - jnp.mean(grad, axis=-1, keepdims=True)
        - hat * jnp.mean(grad * hat, axis=-1, keepdims=True)
    )
    grad_ref[...] = (c_ref[...].astype(F32) + back).astype(BF16)

    for j in range(2):
        for index in range(5):
            block = w_piece(me, j)
            remote(block, block, wsend.at[index, j], wrecv.at[me, j], (sib, z)).wait_send()
        for i in range(2):
            w_relay(i, j).wait_send()

        @pl.when(jnp.logical_not(g_self(j)))
        def _():
            g_send(j).wait_send()

    for a in range(2):
        z_send(a).wait_send()

        @pl.when(is_main)
        def _():
            share(a, None).wait_send()
            share(a, zp).wait_send()
            for i in range(2):
                share(a, foreign[i]).wait_send()

        @pl.when(is_main & is_near)
        def _():
            for i in range(2):
                to_far(a, i).wait_send()

    @pl.when(is_main)
    def _():
        meta_send().wait_send()

    @pl.when(k == p)
    def _():
        for i in range(3):
            wo_sends[i].wait_send()

        @pl.when(jnp.logical_not(wo_here))
        def _():
            wo_sends[3].wait_send()

    for copy in stat_sends(SA, sasend, sarecv) + stat_sends(SG, sgsend, sgrecv):
        copy.wait_send()

    @pl.when(is_root)
    def _():
        h_send(MA, 1).wait_send()

    @pl.when(z == near_root)
    def _():
        t_send().wait_send()

    @pl.when(z == middle)
    def _():
        h_relay(MB, 0, far_root).wait_send()
        h_relay(MA, 1, near_root).wait_send()

    for o in range(2):
        for i in range(n_seq):
            pair_send(o, i).wait_send()

            @pl.when(sends_cross(i))
            def _():
                cross_send(o, i).wait_send()

            @pl.when(jnp.logical_not(sends_cross(i)) & jnp.logical_not(home_is_self(i)))
            def _():
                home_send(o, i).wait_send()


def tail_kernel(mixed_ref, grad_ref, wg_ref, mixed_out, grad_out, wg_out, wide, sems):
    copies = [
        pltpu.make_async_copy(src, dst, sems.at[i])
        for i, (src, dst) in enumerate(
            ((mixed_ref, mixed_out), (grad_ref, grad_out), (wide, wg_out))
        )
    ]
    copies[0].start()
    copies[1].start()
    wide[...] = wg_ref[...].astype(F32)
    copies[2].start()
    for copy in copies:
        copy.wait()


def column_parallel(
    n_dp, n_seq, tokens, cotangent, stamps, lengths, w_qkvu, w_out, gain_in, gain_out, bias_table
):
    tok, width = tokens.shape[1:]
    rows = tok * n_seq
    dma = pltpu.SemaphoreType.DMA
    sds = jax.ShapeDtypeStruct
    hbm = pl.BlockSpec(memory_space=pltpu.HBM)

    def vb(*shape):
        return pltpu.VMEM(shape, BF16)

    def vf(*shape):
        return pltpu.VMEM(shape, F32)

    def in_hbm(value):
        return pltpu.with_memory_space_constraint(value, pltpu.HBM)

    half = tok // 2
    mixed, grad, w_grad = pl.pallas_call(
        lambda *refs: column_kernel(n_dp, n_seq, *refs),
        out_shape=(sds((tok, width), BF16), sds((tok, width), BF16), sds(w_out.shape, BF16)),
        in_specs=[hbm] * 5 + [pl.BlockSpec(memory_space=pltpu.SMEM)] + [hbm] * 3,
        out_specs=[VM] * 3,
        scratch_shapes=[
            pltpu.VMEM(w_qkvu.shape, BF16),
            vb(tok, width),
            vb(tok, width),
            vb(DH, width),
            pltpu.VMEM(stamps.shape, jnp.int32),
            vf(1, width),
            vf(1, width),
            pltpu.SMEM(bias_table.shape, F32),
            pltpu.VMEM((8, rows), jnp.int32),
            vb(2, width, 4 * DH),
            vb(n_seq, tok, width),
            vb(n_seq, tok, width),
            vb(2, DH, width),
            pltpu.VMEM((8, rows), jnp.int32),
            vb(rows, width),
            vf(2, rows, rows),
            vf(2, rows, 4 * DH),
            vf(rows, 2 * DH),
            vb(2, 3, rows, DH),
            vf(rows, 2 * DH),
            vb(2, rows, rows),
            vf(2, rows, rows),
            vf(rows, 2 * DH),
            vf(rows, 2 * DH),
            vb(rows, 2 * DH),
            vb(2, rows, 4 * DH),
            vb(rows, 2 * DH),
            vf(rows, DH),
            vf(rows, DH),
            vf(4, 8, rows),
            vf(4, 8, rows),
            vf(8, rows),
            vb(2, DH, width),
            vb(n_dp // 2, DH, width),
            vb(DH, width),
            vb(DH, width),
            vb(DH, width),
            vb(DH, width),
            vb(DH, width),
            vb(DH, width),
            vb(2, n_seq, 2, half, width),
            vb(2, n_seq, half, width),
            vb(2, n_seq, half, width),
            vb(2, n_seq, half, width),
            vb(2, n_seq, half, width),
            vb(2, 2, half, width),
            dma((8,)),
            dma((5, 2)),
            dma((2, 2)),
            dma((n_dp, 2)),
            dma((2,)),
            dma((2, n_seq)),
            dma((2, 2)),
            dma((2, n_seq)),
            dma((4,)),
            dma((2,)),
            dma((2,)),
            dma((3,)),
            dma((4,)),
            dma((3,)),
            dma((4,)),
            dma((2,)),
            dma((n_dp // 2,)),
            dma((4,)),
            dma((3,)),
            dma,
            dma((2, n_seq)),
            dma((2, n_seq)),
            dma((2, n_seq)),
            dma((2, n_seq)),
            dma((2, n_seq)),
            dma((2, 2)),
        ],
        compiler_params=pltpu.CompilerParams(
            has_side_effects=True, collective_id=0, vmem_limit_bytes=44 * 2**20
        ),
        name="column",
    )(
        *[in_hbm(v) for v in (w_qkvu, tokens[0], cotangent[0], w_out, stamps)],
        lengths,
        *[in_hbm(v) for v in (gain_in[None], gain_out[None], bias_table)],
    )
    mixed, grad, w_grad = pl.pallas_call(
        tail_kernel,
        out_shape=(sds(mixed.shape, BF16), sds(grad.shape, BF16), sds(w_grad.shape, F32)),
        in_specs=[VM] * 3,
        out_specs=[hbm] * 3,
        scratch_shapes=[vf(*w_grad.shape), dma((3,))],
        compiler_params=pltpu.CompilerParams(vmem_limit_bytes=8 * 2**20),
        name="tail",
    )(mixed, grad, w_grad)
    return (mixed[None], grad[None], w_grad)


def solution(mesh):
    n_dp, n_seq = mesh.shape["dp"], mesh.shape["seq"]

    def body(*args):
        tokens, stamps, w_out = args[0], args[2], args[5]
        mesh_fits = n_seq == 4 and n_dp == 2 * n_seq and n_dp == H
        sizes_fit = w_out.shape[0] == DH and tokens.shape[1] == DH
        if mesh_fits and sizes_fit and stamps.shape == (1, n_seq * DH):
            return column_parallel(n_dp, n_seq, *args)
        return per_device(*args)

    return jax.shard_map(
        body,
        mesh=mesh,
        in_specs=(
            P("dp", "seq", None),
            P("dp", "seq", None),
            P("dp", None),
            P("dp"),
            P("dp", None),
            P("dp", None),
            P(),
            P(),
            P(),
        ),
        out_specs=(P("dp", "seq", None), P("dp", "seq", None), P("dp", None)),
        check_vma=False,
    )
```

```python
import jax
import jax.numpy as jnp
from jax import lax
from jax.experimental import pallas as pl
from jax.experimental.pallas import tpu as pltpu
from jax.sharding import PartitionSpec as P

H = 8
DH = 128


EPS = 1e-05


def layer_norm(values, gain):
    average = jnp.mean(values, axis=-1, keepdims=True)
    centred = values - average
    variance = jnp.mean(centred * centred, axis=-1, keepdims=True)
    return centred * lax.rsqrt(variance + EPS) * gain


def silu_slope(values):
    sigmoid_v = jax.nn.sigmoid(values)
    return sigmoid_v * (1.0 + values * (1.0 - sigmoid_v))


def time_bias(bias_table, stamps_q, stamps_k):
    elapsed = stamps_q[:, None] - stamps_k[None, :]
    bucket = jnp.zeros(elapsed.shape, jnp.int32)
    for degree in range(1, bias_table.shape[1]):
        bucket = bucket + (elapsed >= 2**degree - 1).astype(jnp.int32)
    levels = jnp.arange(bias_table.shape[1], dtype=jnp.int32)
    one_hot = (bucket[:, :, None] == levels[None, None, :]).astype(jnp.float32)
    return jnp.einsum(
        "qkb,hb->hqk",
        one_hot,
        bias_table,
        precision=lax.Precision.HIGHEST,
        preferred_element_type=jnp.float32,
    )


def pair_terms(
    q_heads, d_heads, stamps_q, pos_q, k_heads, v_heads, stamps_k, pos_k, length, bias_table, scale
):
    scores = (
        jnp.einsum("qhd,khd->hqk", q_heads, k_heads, preferred_element_type=jnp.float32) * scale
    )
    scores = scores + time_bias(bias_table, stamps_q, stamps_k)
    allowed = (
        (pos_k[None, :] <= pos_q[:, None]) & (pos_k[None, :] < length) & (pos_q[:, None] < length)
    )
    weight = jnp.where(allowed[None], jax.nn.silu(scores), 0.0).astype(jnp.bfloat16)
    if d_heads is None:
        return (weight, None)
    d_weight = jnp.einsum("qhd,khd->hqk", d_heads, v_heads, preferred_element_type=jnp.float32)
    d_scores = jnp.where(allowed[None], d_weight * silu_slope(scores), 0.0).astype(jnp.bfloat16)
    return (weight, d_scores)


def per_device(tokens, cotangent, stamps, lengths, w_qkvu, w_out, gain_in, gain_out, bias_table):
    rows = tokens[0]
    cot_rows = cotangent[0]
    tok_count = rows.shape[0]
    feature_width = rows.shape[1]
    seq_count = lax.axis_size("seq")
    total_rows = tok_count * seq_count
    first_row = lax.axis_index("seq") * tok_count
    length = lengths[0]
    stamp_all = stamps[0]
    pos_own = first_row + jnp.arange(tok_count, dtype=jnp.int32)
    stamp_own = lax.dynamic_slice_in_dim(stamp_all, first_row, tok_count)
    scale = DH ** (-0.5)
    block_rows = min(512, total_rows)
    block_count = total_rows // block_rows
    w_full, w_out_full = (
        lax.all_gather(w_qkvu, "dp", axis=0, tiled=True),
        lax.all_gather(w_out, "dp", axis=0, tiled=True),
    )
    wide_rows = rows.astype(jnp.float32)
    normed = layer_norm(wide_rows, gain_in).astype(jnp.bfloat16)
    projected = jnp.dot(normed, w_full, preferred_element_type=jnp.float32)
    activated = jax.nn.silu(projected)
    gate_u = activated[:, :feature_width]
    values_own = activated[:, feature_width : 2 * feature_width].astype(jnp.bfloat16)
    queries_own = activated[:, 2 * feature_width : 3 * feature_width].astype(jnp.bfloat16)
    keys_own = activated[:, 3 * feature_width :].astype(jnp.bfloat16)
    keys_all, values_all = (
        lax.all_gather(keys_own, "seq", axis=0, tiled=True),
        lax.all_gather(values_own, "seq", axis=0, tiled=True),
    )
    q_heads = queries_own.reshape(tok_count, H, DH)

    def key_block(start):
        k_heads = lax.dynamic_slice_in_dim(keys_all, start, block_rows).reshape(block_rows, H, DH)
        v_heads = lax.dynamic_slice_in_dim(values_all, start, block_rows).reshape(block_rows, H, DH)
        stamps_k = lax.dynamic_slice_in_dim(stamp_all, start, block_rows)
        pos_k = start + jnp.arange(block_rows, dtype=jnp.int32)
        return (k_heads, v_heads, stamps_k, pos_k)

    def guarded(active, action, state):
        return lax.cond(active, action, lambda same: same, state)

    def reaches(start):
        return (start <= first_row + tok_count - 1) & (start < length) & (first_row < length)

    def forward_step(block_idx, totals):
        start = block_idx * block_rows

        def forward_compute(totals):
            k_heads, v_heads, stamps_k, pos_k = key_block(start)
            weight, unused = pair_terms(
                q_heads,
                None,
                stamp_own,
                pos_own,
                k_heads,
                v_heads,
                stamps_k,
                pos_k,
                length,
                bias_table,
                scale,
            )
            return totals + jnp.einsum(
                "hqk,khd->qhd", weight, v_heads, preferred_element_type=jnp.float32
            )

        return guarded(reaches(start), forward_compute, totals)

    attended = lax.fori_loop(
        0, block_count, forward_step, jnp.zeros((tok_count, H, DH), jnp.float32)
    )
    attended = attended.reshape(tok_count, feature_width)
    normed_att, norm_back = jax.vjp(lambda values: layer_norm(values, gain_out), attended)
    mixed_rows = (normed_att * gate_u).astype(jnp.bfloat16)
    mixed = (
        wide_rows + jnp.dot(mixed_rows, w_out_full, preferred_element_type=jnp.float32)
    ).astype(jnp.bfloat16)
    grad_part = lax.psum_scatter(
        jnp.einsum("tr,tc->rc", mixed_rows, cot_rows, preferred_element_type=jnp.float32).astype(
            jnp.bfloat16
        ),
        "dp",
        scatter_dimension=0,
        tiled=True,
    )
    w_grad = lax.psum(grad_part, "seq").astype(jnp.float32)
    d_mix = jnp.einsum("tc,rc->tr", cot_rows, w_out_full, preferred_element_type=jnp.float32)
    d_gate = d_mix * normed_att
    d_att = norm_back(d_mix * gate_u)[0].astype(jnp.bfloat16)
    d_heads = d_att.reshape(tok_count, H, DH)

    def backward_step():

        def step(block_idx, state_pair):
            start = block_idx * block_rows

            def step_compute(state_pair):
                q_grad, key_terms = state_pair
                k_heads, v_heads, stamps_k, pos_k = key_block(start)
                weight, d_scores = pair_terms(
                    q_heads,
                    d_heads,
                    stamp_own,
                    pos_own,
                    k_heads,
                    v_heads,
                    stamps_k,
                    pos_k,
                    length,
                    bias_table,
                    scale,
                )
                q_grad = (
                    q_grad
                    + jnp.einsum(
                        "hqk,khd->qhd", d_scores, k_heads, preferred_element_type=jnp.float32
                    )
                    * scale
                )
                k_grad = (
                    jnp.einsum(
                        "hqk,qhd->khd", d_scores, q_heads, preferred_element_type=jnp.float32
                    )
                    * scale
                )
                v_grad = jnp.einsum(
                    "hqk,qhd->khd", weight, d_heads, preferred_element_type=jnp.float32
                )
                joined = jnp.concatenate(
                    [
                        k_grad.reshape(block_rows, feature_width),
                        v_grad.reshape(block_rows, feature_width),
                    ],
                    axis=1,
                )
                key_terms = lax.dynamic_update_slice_in_dim(key_terms, joined, start, 0)
                return (q_grad, key_terms)

            return guarded(reaches(start), step_compute, state_pair)

        return step

    q_start = jnp.zeros((tok_count, H, DH), jnp.float32)
    term_start = jnp.zeros((total_rows, 2 * feature_width), jnp.float32)
    q_grad, key_terms = lax.fori_loop(0, block_count, backward_step(), (q_start, term_start))
    key_grads = lax.psum_scatter(
        key_terms.astype(jnp.bfloat16), "seq", scatter_dimension=0, tiled=True
    ).astype(jnp.float32)
    d_act = jnp.concatenate(
        [
            d_gate,
            key_grads[:, feature_width:],
            q_grad.reshape(tok_count, feature_width),
            key_grads[:, :feature_width],
        ],
        axis=1,
    )
    d_proj = (d_act * silu_slope(projected)).astype(jnp.bfloat16)
    d_normed = jnp.einsum("tf,df->td", d_proj, w_full, preferred_element_type=jnp.float32)
    unused_rows, in_back = jax.vjp(lambda values: layer_norm(values, gain_in), wide_rows)
    input_grad = (cot_rows.astype(jnp.float32) + in_back(d_normed)[0]).astype(jnp.bfloat16)
    return (mixed[None], input_grad[None], w_grad)


MESH = pl.DeviceIdType.MESH
VM = pl.BlockSpec(memory_space=pltpu.VMEM)
F32 = jnp.float32
BF16 = jnp.bfloat16
MASKED = -1e30
PIECES = 4


def mm(a, b, dims):
    return lax.dot_general(a, b, (dims, ((), ())), preferred_element_type=F32)


def remote(src, dst, send_sem, recv_sem, target):
    return pltpu.make_async_remote_copy(
        src_ref=src,
        dst_ref=dst,
        send_sem=send_sem,
        recv_sem=recv_sem,
        device_id=target,
        device_id_type=MESH,
    )


def arrived(dst, sem):
    pltpu.make_async_copy(dst, dst, sem).wait()


def sent(block, sem, target):
    remote(block, block, sem, sem, target).wait_send()


def column_kernel(
    n_dp, n_seq, w_hbm, x_hbm, c_hbm, wo_hbm, stamps_hbm, length_ref, gin_hbm, gout_hbm, bias_hbm,
    mixed_ref, grad_ref, wg_ref,
    w_ref, x_ref, c_ref, wo_ref, stamps_ref, gin_ref, gout_ref, bias_ref, meta_ref,
    W, X, C, WO, mbuf, NB, BI, PJ, GT, ACT, ATT, WT, SL, DM, DG, DA, DP, MR, MX, KA, VA, SA, SG, TB,
    MW, WG, PS, PR, TS, TR, MA, MB, PB, SB, CS, FB, FIN, RO,
    lsem, wout, wvia, wrest, zout, shareout, farout, xrecv, woout, worecv, msem,
    saout, sarecv, sgout, sgrecv, mxout, mxrecv, gout, grecv,
    hout, hmid, hback, trecv, pout, precv, cout, crecv, oout, orecv,
):
    me = lax.axis_index("dp")
    z = lax.axis_index("seq")
    tok, width = x_ref.shape
    rows = tok * n_seq
    half = tok // 2
    n_heads = n_dp
    scale = DH ** (-0.5)
    chip, k = me // 2, me % 2
    cy, cx = chip // 2, chip % 2
    xn, yn = 2 * cy + (1 - cx), 2 * (1 - cy) + cx
    dn = 2 * (1 - cy) + (1 - cx)
    sib = 2 * chip + (1 - k)
    p, ks = z % 2, z // 2
    near, far = 1 + ks, (n_seq - 1) * ks
    zp = near + far - z
    is_near, is_far = z == near, z == far
    is_main = k == ks
    is_aux = jnp.logical_not(is_main)
    main_dp = 2 * chip + ks

    def head_of(core, j):
        return 4 * core + 2 * j + p

    def rows_of(ref_rows, index):
        return pl.ds(pl.multiple_of(index * ref_rows, ref_rows), ref_rows)

    def lanes_of(index):
        return pl.ds(pl.multiple_of(index * DH, DH), DH)

    def w_copies(core, j, make):
        return [
            make(
                w_ref.at[:, lanes_of(g * n_heads + head_of(core, j))],
                W.at[j, rows_of(tok, me), slice(g * DH, (g + 1) * DH)],
            )
            for g in range(4)
        ]

    w_targets = (
        (xn, 0, wvia.at[k]), (yn, 1, wvia.at[k]), (chip, 1 - k, wrest), (xn, 1, wrest),
        (yn, 0, wrest),
    )

    def w_start(j):
        for where, core, sem in w_targets:
            for copy in w_copies(
                core, j, lambda s, d: remote(s, d, wout, sem.at[j], (2 * where + core, z))
            ):
                copy.start()

    def w_piece(src, j):
        return W.at[j, rows_of(tok, src)]

    via, to = (1 - k) * xn + k * yn, (1 - k) * yn + k * xn

    def w_relay(i, j):
        src = 2 * via + i
        block = w_piece(src, j)
        return remote(block, block, wout, wrest.at[j], (2 * to + k, z))

    ins, outs = (x_ref, c_ref), (X, C)
    z_to = jnp.where(is_main, zp, 1 + k)

    def z_send(a):
        return remote(ins[a], outs[a].at[z], zout, xrecv.at[a, z], (me, z_to))

    def own_copy(a):
        return pltpu.make_async_copy(ins[a], outs[a].at[z], xrecv.at[a, z])

    def share(a, b):
        block = ins[a] if b is None else outs[a].at[b]
        at = z if b is None else b
        return remote(block, outs[a].at[at], shareout, xrecv.at[a, at], (sib, z))

    foreign = (2 * (1 - ks), 2 * (1 - ks) + 1)

    def to_far(a, i):
        block = outs[a].at[foreign[i]]
        return remote(block, block, farout, xrecv.at[a, foreign[i]], (me, far))

    def x_wait(a, b):
        arrived(outs[a].at[b], xrecv.at[a, b])

    def meta_send():
        return remote(meta_ref, mbuf, msem.at[0], msem.at[1], (sib, z))

    wo_core, wo_slot = chip // 2, chip % 2
    wo_part = 2 * k + wo_core
    wo_here = wo_core == k
    wo_sem = jnp.where(k == p, wo_slot, 2)
    wo_sends = [
        remote(
            wo_ref, WO.at[wo_part, wo_slot], woout, worecv.at[wo_sem],
            (2 * where + wo_core, z),
        )
        for i, where in enumerate((xn, yn, dn, chip))
    ]

    def wo_start():
        for i in range(3):
            wo_sends[i].start()

        @pl.when(wo_here)
        def _():
            pltpu.make_async_copy(wo_ref, WO.at[wo_part, wo_slot], worecv.at[wo_sem]).start()

        @pl.when(jnp.logical_not(wo_here))
        def _():
            wo_sends[3].start()

    def wo_share(parity, j):
        block = WO.at[2 * parity + k, j]
        return remote(block, block, woout, worecv.at[3], (sib, z))

    loads = [
        pltpu.make_async_copy(src, dst, lsem.at[i])
        for src, dst, i in (
            (stamps_hbm, stamps_ref, 0), (w_hbm, w_ref, 1), (x_hbm, x_ref, 1), (c_hbm, c_ref, 1),
            (wo_hbm, wo_ref, 1), (gin_hbm, gin_ref, 2), (gout_hbm, gout_ref, 3),
            (bias_hbm, bias_ref, 4),
        )
    ]
    barrier = pltpu.get_barrier_semaphore()
    peers = [(lax.rem(me + step, n_dp), z) for step in range(1, n_dp)]
    for step in range(1, n_seq):
        peers += [(me, lax.rem(z + step, n_seq)), (sib, lax.rem(z + step, n_seq))]
    for peer in peers:
        pl.semaphore_signal(barrier, inc=1, device_id=peer, device_id_type=MESH)
    for load in loads:
        load.start()
    loads[0].wait()
    meta_ref[0:1, :] = stamps_ref[...]
    meta_ref[1:2, :] = jnp.full(stamps_ref.shape, length_ref[0], jnp.int32)
    arrived(W.at[:, : (n_dp - 1) * tok], lsem.at[1])
    for load in loads[5:]:
        load.wait()
    pl.semaphore_wait(barrier, len(peers))
    @pl.when(is_main)
    def _():
        pltpu.make_async_copy(meta_ref, mbuf, msem.at[1]).start()
        meta_send().start()

    w_start(0)
    z_send(0).start()

    @pl.when(is_main)
    def _():
        own_copy(0).start()
        share(0, None).start()

    z_send(1).start()

    @pl.when(is_main)
    def _():
        own_copy(1).start()
        share(1, None).start()

    for j in range(2):
        for copy in w_copies(k, j, lambda s, d: pltpu.make_async_copy(s, d, wrest.at[j])):
            copy.start()

    def relay_weights(j):
        for i in range(2):
            arrived(w_piece(2 * via + i, j), wvia.at[i, j])
            w_relay(i, j).start()

    def near_relay(a):
        @pl.when(is_main)
        def _():
            x_wait(a, zp)
            share(a, zp).start()

        @pl.when(is_main & is_near)
        def _():
            for i in range(2):
                x_wait(a, foreign[i])
                to_far(a, i).start()
                share(a, foreign[i]).start()

    def far_relay(a):
        @pl.when(is_main & is_far)
        def _():
            for i in range(2):
                x_wait(a, foreign[i])
                share(a, foreign[i]).start()

    relay_weights(0)
    w_start(1)
    near_relay(0)

    arrived(mbuf, msem.at[1])
    lane_row = lax.broadcasted_iota(jnp.int32, (DH, DH), 0)
    lane_col = lax.broadcasted_iota(jnp.int32, (DH, DH), 1)
    length = mbuf[1:2, :DH]
    for i in range(n_seq):
        col = jnp.broadcast_to(mbuf[0:1, i * DH : (i + 1) * DH].astype(F32), (DH, DH)).T
        valid = lane_row + i * DH < length
        for b in range(i + 1):
            elapsed = col - mbuf[0:1, b * DH : (b + 1) * DH].astype(F32)
            allowed = valid & (lane_col <= lane_row) if b == i else valid
            heads = [head_of(k, j) for j in range(2)]
            terms = [jnp.full(elapsed.shape, bias_ref[h, 0], F32) for h in heads]
            for degree in range(1, bias_ref.shape[1]):
                reached = elapsed >= float(2**degree - 1)
                terms = [
                    jnp.where(reached, bias_ref[h, degree], t) for h, t in zip(heads, terms)
                ]
            for j in range(2):
                BI[j, i * DH : (i + 1) * DH, b * DH : (b + 1) * DH] = jnp.where(
                    allowed, terms[j], MASKED
                )

    near_relay(1)
    relay_weights(1)

    far_relay(0)

    @pl.when(is_main)
    def _():
        x_wait(0, z)

    @pl.when(is_aux)
    def _():
        for b in range(n_seq):
            x_wait(0, b)

    for b in range(n_seq):
        NB[b * tok : (b + 1) * tok, :] = layer_norm(X[b].astype(F32), gin_ref[...]).astype(BF16)

    def forward(j):
        arrived(W.at[j, : (n_dp - 2) * tok], wrest.at[j])
        PJ[j] = mm(NB[...], W[j], ((1,), (0,)))
        cols = slice(j * DH, (j + 1) * DH)
        GT[:, cols] = jax.nn.silu(PJ[j, :, :DH])
        for g in range(3):
            ACT[j, g] = jax.nn.silu(PJ[j, :, (1 + g) * DH : (2 + g) * DH]).astype(BF16)
        for i in range(n_seq):
            at, end = slice(i * tok, (i + 1) * tok), (i + 1) * tok
            scores = mm(ACT[j, 1, at], ACT[j, 2, :end], ((1,), (1,))) * scale + BI[j, at, :end]
            sig = jax.nn.sigmoid(scores)
            weight = (scores * sig).astype(BF16)
            WT[j, at, :end] = weight
            SL[j, at, :end] = sig * (1.0 + scores * (1.0 - sig))
            ATT[at, cols] = mm(weight, ACT[j, 0, :end], ((1,), (0,)))

    @pl.when(k == p)
    def _():
        wo_start()

    forward(0)

    forward(1)

    gain = jnp.concatenate([gout_ref[:, lanes_of(head_of(k, j))] for j in range(2)], axis=1)
    pid = 2 * p + k
    own_width = 2 * DH
    st_peers = ((sib, z), (me, zp), (sib, zp))

    def stat_sends(ref, send_sem, recv_sem):
        return [
            remote(ref.at[pid], ref.at[pid], send_sem, recv_sem, peer)
            for peer in st_peers
        ]

    def put_stats(ref, at, first, second):
        ref[pid, :, at] = jnp.where(lane_col == 0, first, second).T[:8]

    for b in range(n_seq):
        at = slice(b * tok, (b + 1) * tok)
        att = ATT[at, :]
        mean_own = jnp.mean(att, axis=1, keepdims=True)
        off = att - mean_own
        put_stats(SA, at, mean_own, jnp.sum(off * off, axis=1, keepdims=True))
    for copy in stat_sends(SA, saout, sarecv):
        copy.start()
    far_relay(1)
    @pl.when(is_main)
    def _():
        x_wait(1, z)

    @pl.when(is_aux)
    def _():
        for b in range(n_seq):
            x_wait(1, b)

    c_rows = C[...].reshape(rows, width)
    for j in range(2):
        arrived(WO.at[pid, j], worecv.at[j])
        wo_share(p, j).start()
        DM[:, j * DH : (j + 1) * DH] = mm(c_rows, WO[pid, j], ((1,), (1,)))
    for b in range(n_seq):
        at = slice(b * tok, (b + 1) * tok)
        att = ATT[at, :]
        off = att - jnp.mean(att, axis=1, keepdims=True)
        g = DM[at, :] * GT[at, :] * gain
        put_stats(
            SG, at, jnp.sum(g, axis=1, keepdims=True), jnp.sum(g * off, axis=1, keepdims=True)
        )
    for copy in stat_sends(SG, sgout, sgrecv):
        copy.start()

    arrived(SA.at[:3], sarecv)
    means = [SA[q, 0:1, :] for q in range(4)]
    mean = sum(means[1:], means[0]) / 4.0
    shifts = [m - mean for m in means]
    squares = sum(SA[q, 1:2, :] + own_width * shifts[q] * shifts[q] for q in range(4))
    rstd = lax.rsqrt(squares / width + EPS)
    TB[...] = jnp.concatenate([mean, rstd] * 4, axis=0)

    def turned(at):
        return jnp.concatenate([TB[:, at]] * (DH // 8), axis=0).T

    blocks = tuple(reversed(range(n_seq)))

    def mine(b):
        return is_near == (far != b)

    def other(b):
        return is_near == (far == b)

    def home_is_self(b):
        return is_main & (z == b)

    def mx_send(b):
        return remote(
            MR.at[b * tok : (b + 1) * tok], MX.at[pid], mxout, mxrecv, (main_dp, b)
        )

    for b in blocks:
        at = slice(b * tok, (b + 1) * tok)
        columns = turned(at)
        hat = (ATT[at, :] - columns[:, 0:1]) * columns[:, 1:2]
        ATT[at, :] = hat
        MR[at, :] = (hat * gain * GT[at, :]).astype(BF16)

    for b in blocks:

        @pl.when(home_is_self(b))
        def _():
            pltpu.make_async_copy(
                MR.at[b * tok : (b + 1) * tok], MX.at[pid], mxrecv
            ).start()

        @pl.when(jnp.logical_not(home_is_self(b)))
        def _():
            mx_send(b).start()

    pieces = PIECES
    piece = DH // pieces

    def out_rows(i):
        return slice(i * piece, (i + 1) * piece)

    def g_send(j, i):
        return remote(
            MW.at[j, i], WG.at[chip, i], gout, grecv.at[i],
            (2 * (2 * k + j) + p, z),
        )

    def g_self(j):
        return (2 * k + j == chip) & (k == p)

    for j in range(2):
        part = mm(MR[:, j * DH : (j + 1) * DH], c_rows, ((0,), (0,)))
        for i in range(pieces):
            MW[j, i] = part[out_rows(i)].astype(BF16)
    for i in range(pieces):
        for j in range(2):

            @pl.when(g_self(j))
            def _():
                pltpu.make_async_copy(MW.at[j, i], WG.at[chip, i], grecv.at[i]).start()

            @pl.when(jnp.logical_not(g_self(j)))
            def _():
                g_send(j, i).start()

    is_root = k == p
    far_root, near_root, middle, edge = (n_seq - 1) * k, 2 - k, 1 + k, (n_seq - 1) * (1 - k)
    def h_send(dst, recv, i):
        return remote(PS.at[i], dst.at[i], hout, recv.at[i], (me, middle))

    def h_relay(src, i, to):
        return remote(src.at[i], PR.at[i], hout, hback.at[i], (me, to))

    def t_send(i):
        return remote(TS.at[i], TR.at[i], hout, trecv.at[i], (me, edge))

    def plane_sum(i):
        @pl.when(is_root)
        def _():
            arrived(WG.at[:, i], grecv.at[i])
            total = WG[0, i].astype(F32)
            for c in range(1, n_dp // 2):
                total = total + WG[c, i].astype(F32)
            PS[i] = total.astype(BF16)

            @pl.when(z == far_root)
            def _():
                h_send(MA, hmid.at[0], i).start()

            @pl.when(z == near_root)
            def _():
                h_send(MB, hmid.at[1], i).start()

    def pass_in():
        @pl.when(z == middle)
        def _():
            for i in range(pieces):
                arrived(MB.at[i], hmid.at[1, i])
                h_relay(MB, i, far_root).start()

    def pass_out():
        @pl.when(z == middle)
        def _():
            for i in range(pieces):
                arrived(MA.at[i], hmid.at[0, i])
                h_relay(MA, i, near_root).start()
                wg_ref[out_rows(i)] = (MA[i].astype(F32) + MB[i].astype(F32)).astype(BF16)

    def root_total(i):
        arrived(PR.at[i], hback.at[i])
        TS[i] = (PS[i].astype(F32) + PR[i].astype(F32)).astype(BF16)
        wg_ref[out_rows(i)] = TS[i]

    def near_total():
        @pl.when(z == near_root)
        def _():
            for i in range(pieces):
                root_total(i)
                t_send(i).start()

    def outer_total():
        @pl.when(z == far_root)
        def _():
            for i in range(pieces):
                root_total(i)

        @pl.when(z == edge)
        def _():
            for i in range(pieces):
                arrived(TR.at[i], trecv.at[i])
                wg_ref[out_rows(i)] = TR[i]

    def pair_send(b):
        return remote(PB.at[b, 1 - k], SB.at[b], pout, precv.at[b], (sib, z))

    def cross_send(b):
        return remote(CS.at[b], FB.at[b], cout, crecv.at[b], (me, zp))

    def home_send(b):
        return remote(FIN.at[b], RO.at[k], oout, orecv, (main_dp, b))

    def pair_sum(b):
        return PB[b, k].astype(F32) + SB[b].astype(F32)

    def cross(b):
        arrived(SB.at[b], precv.at[b])

        @pl.when(other(b))
        def _():
            CS[b] = pair_sum(b).astype(BF16)
            cross_send(b).start()

    def finish(b):
        @pl.when(mine(b))
        def _():
            arrived(FB.at[b], crecv.at[b])
            FIN[b] = (pair_sum(b) + FB[b].astype(F32)).astype(BF16)

            @pl.when(home_is_self(b))
            def _():
                pltpu.make_async_copy(FIN.at[b], RO.at[k], orecv).start()

            @pl.when(jnp.logical_not(home_is_self(b)))
            def _():
                home_send(b).start()

    arrived(SG.at[:3], sgrecv)
    g_mean = sum(SG[q, 0:1, :] for q in range(4)) / width
    g_dot = rstd * sum(SG[q, 1:2, :] + shifts[q] * SG[q, 0:1, :] for q in range(4)) / width
    TB[...] = jnp.concatenate([rstd, g_mean, g_dot, rstd] * 2, axis=0)
    for b in range(n_seq):
        at = slice(b * tok, (b + 1) * tok)
        columns = turned(at)
        d_mix, hat = DM[at, :], ATT[at, :]
        DG[at, :] = d_mix * (hat * gain)
        g = d_mix * GT[at, :] * gain
        DA[at, :] = (
            columns[:, 0:1] * (g - columns[:, 1:2] - hat * columns[:, 2:3])
        ).astype(BF16)

    def backward(j, b):
        cols = slice(j * DH, (j + 1) * DH)
        start, end = b * tok, (b + 1) * tok

        def put(group, grad):
            at = slice(group * DH, (group + 1) * DH)
            DP[j, start:end, at] = (grad * silu_slope(PJ[j, start:end, at])).astype(BF16)

        d_att = DA[start:end, cols]
        d_weight = mm(d_att, ACT[j, 0, :end], ((1,), (1,)))
        d_scores = (d_weight * SL[j, start:end, :end]).astype(BF16)
        put(2, mm(d_scores, ACT[j, 2, :end], ((1,), (0,))) * scale)
        k_part = mm(d_scores, ACT[j, 1, start:end], ((0,), (0,)))
        v_part = mm(WT[j, start:end, :end], d_att, ((0,), (0,)))
        if end == rows:
            KA[j] = k_part
            VA[j] = v_part
        else:
            KA[j, :end] += k_part
            VA[j, :end] += v_part
        put(0, DG[start:end, cols])
        put(1, VA[j, start:end])
        put(3, KA[j, start:end] * scale)

    def d_part(b):
        at = slice(b * tok, (b + 1) * tok)
        part = mm(DP[0, at], W[0], ((1,), (1,))) + mm(DP[1, at], W[1], ((1,), (1,)))
        PB[b, 0] = part[:half].astype(BF16)
        PB[b, 1] = part[half:].astype(BF16)
        pair_send(b).start()

    last = n_seq - 1
    for b in blocks:
        for j in range(2):
            backward(j, b)
        if b == last:

            @pl.when(ks == 0)
            def _():
                d_part(last)

        else:
            d_part(b)
        if b == last - 1:

            @pl.when(ks == 0)
            def _():
                cross(last)

        elif b == 1:
            cross(2)
        if b < 2:
            for i in range(pieces // 2):
                plane_sum((1 - b) * pieces // 2 + i)
    cross(1)
    cross(0)

    @pl.when(k != p)
    def _():
        wo_start()

    @pl.when(ks != 0)
    def _():
        d_part(last)
        cross(last)

    finish(3)
    pass_in()
    finish(2)
    pass_out()
    finish(1)
    finish(0)
    near_total()
    arrived(WO.at[2 * (1 - p) + k], worecv.at[2])
    for j in range(2):
        wo_share(1 - p, j).start()

    arrived(X, worecv.at[3])
    arrived(MX, mxrecv)
    wide = x_ref[...].astype(F32)
    total = wide
    for q in range(4):
        total = total + mm(MX[q], WO[q].reshape(2 * DH, width), ((1,), (0,)))
    mixed_ref[...] = total.astype(BF16)

    average = jnp.mean(wide, axis=-1, keepdims=True)
    centred = wide - average
    inv = lax.rsqrt(jnp.mean(centred * centred, axis=-1, keepdims=True) + EPS)
    hat = centred * inv
    outer_total()
    arrived(RO, orecv)
    grad = RO[...].reshape(tok, width).astype(F32) * gin_ref[...]
    back = inv * (
        grad
        - jnp.mean(grad, axis=-1, keepdims=True)
        - hat * jnp.mean(grad * hat, axis=-1, keepdims=True)
    )
    grad_ref[...] = (c_ref[...].astype(F32) + back).astype(BF16)

    beside = (sib, z)

    def sent_when(condition, block, sem):
        @pl.when(condition)
        def _():
            sent(block, sem, beside)

    part = (n_dp - 1) * tok
    sent(W.at[:, :part], wout, beside)
    sent(X.at[:2], zout, beside)
    sent_when(is_main, W, shareout)
    sent_when(is_main & is_near, X, farout)
    sent_when(is_main, meta_ref, msem.at[0])
    sent_when(wo_here, W.at[:, :part], woout)
    sent_when(jnp.logical_not(wo_here), W, woout)
    sent(SA.at[:3], saout, beside)
    sent(SG.at[:3], sgout, beside)
    sent_when(is_main, MX.at[:3], mxout)
    sent_when(is_aux, MX, mxout)
    keeps_one = is_root & wo_here
    sent_when(keeps_one, X.at[0], gout)
    sent_when(jnp.logical_not(keeps_one), X.at[:2], gout)
    sent_when(z == far_root, PS, hout)
    sent_when((z == near_root) | (z == middle), X.at[:2], hout)
    sent(X.at[:2], pout, beside)
    sent_when(is_far, CS.at[:3], cout)
    sent_when(is_near, CS.at[:1], cout)
    sent_when(is_near & is_main, FIN.at[:2], oout)
    sent_when(is_near & is_aux, FIN.at[:3], oout)
    sent_when(is_far & is_aux, FIN.at[:1], oout)


def tail_kernel(mixed_ref, grad_ref, wg_ref, mixed_out, grad_out, wg_out, wide, sems):
    copies = [
        pltpu.make_async_copy(src, dst, sems.at[i])
        for i, (src, dst) in enumerate(
            ((mixed_ref, mixed_out), (grad_ref, grad_out), (wide, wg_out))
        )
    ]
    copies[0].start()
    copies[1].start()
    wide[...] = wg_ref[...].astype(F32)
    copies[2].start()
    for copy in copies:
        copy.wait()


def column_parallel(
    n_dp, n_seq, tokens, cotangent, stamps, lengths, w_qkvu, w_out, gain_in, gain_out, bias_table
):
    tok, width = tokens.shape[1:]
    rows = tok * n_seq
    dma = pltpu.SemaphoreType.DMA
    sds = jax.ShapeDtypeStruct
    hbm = pl.BlockSpec(memory_space=pltpu.HBM)

    def vb(*shape):
        return pltpu.VMEM(shape, BF16)

    def vf(*shape):
        return pltpu.VMEM(shape, F32)

    def in_hbm(value):
        return pltpu.with_memory_space_constraint(value, pltpu.HBM)

    half = tok // 2
    mixed, grad, w_grad = pl.pallas_call(
        lambda *refs: column_kernel(n_dp, n_seq, *refs),
        out_shape=(sds((tok, width), BF16), sds((tok, width), BF16), sds(w_out.shape, BF16)),
        in_specs=[hbm] * 5 + [pl.BlockSpec(memory_space=pltpu.SMEM)] + [hbm] * 3,
        out_specs=[VM] * 3,
        scratch_shapes=[
            pltpu.VMEM(w_qkvu.shape, BF16),
            vb(tok, width),
            vb(tok, width),
            vb(DH, width),
            pltpu.VMEM(stamps.shape, jnp.int32),
            vf(1, width),
            vf(1, width),
            pltpu.SMEM(bias_table.shape, F32),
            pltpu.VMEM((8, rows), jnp.int32),
            vb(2, width, 4 * DH),
            vb(n_seq, tok, width),
            vb(n_seq, tok, width),
            vb(4, 2, DH, width),
            pltpu.VMEM((8, rows), jnp.int32),
            vb(rows, width),
            vf(2, rows, rows),
            vf(2, rows, 4 * DH),
            vf(rows, 2 * DH),
            vb(2, 3, rows, DH),
            vf(rows, 2 * DH),
            vb(2, rows, rows),
            vf(2, rows, rows),
            vf(rows, 2 * DH),
            vf(rows, 2 * DH),
            vb(rows, 2 * DH),
            vb(2, rows, 4 * DH),
            vb(rows, 2 * DH),
            vb(4, tok, 2 * DH),
            vf(2, rows, DH),
            vf(2, rows, DH),
            vf(4, 8, rows),
            vf(4, 8, rows),
            vf(8, rows),
            vb(2, PIECES, DH // PIECES, width),
            vb(n_dp // 2, PIECES, DH // PIECES, width),
            vb(PIECES, DH // PIECES, width),
            vb(PIECES, DH // PIECES, width),
            vb(PIECES, DH // PIECES, width),
            vb(PIECES, DH // PIECES, width),
            vb(PIECES, DH // PIECES, width),
            vb(PIECES, DH // PIECES, width),
            vb(n_seq, 2, half, width),
            vb(n_seq, half, width),
            vb(n_seq, half, width),
            vb(n_seq, half, width),
            vb(n_seq, half, width),
            vb(2, half, width),
            dma((5,)),
            dma,
            dma((2, 2)),
            dma((2,)),
            dma,
            dma,
            dma,
            dma((2, n_seq)),
            dma,
            dma((4,)),
            dma((2,)),
            dma,
            dma,
            dma,
            dma,
            dma,
            dma,
            dma,
            dma((PIECES,)),
            dma,
            dma((2, PIECES)),
            dma((PIECES,)),
            dma((PIECES,)),
            dma,
            dma((n_seq,)),
            dma,
            dma((n_seq,)),
            dma,
            dma,
        ],
        compiler_params=pltpu.CompilerParams(
            has_side_effects=True, collective_id=0, vmem_limit_bytes=44 * 2**20
        ),
        name="column",
    )(
        *[in_hbm(v) for v in (w_qkvu, tokens[0], cotangent[0], w_out, stamps)],
        lengths,
        *[in_hbm(v) for v in (gain_in[None], gain_out[None], bias_table)],
    )
    mixed, grad, w_grad = pl.pallas_call(
        tail_kernel,
        out_shape=(sds(mixed.shape, BF16), sds(grad.shape, BF16), sds(w_grad.shape, F32)),
        in_specs=[VM] * 3,
        out_specs=[hbm] * 3,
        scratch_shapes=[vf(*w_grad.shape), dma((3,))],
        compiler_params=pltpu.CompilerParams(vmem_limit_bytes=8 * 2**20),
        name="tail",
    )(mixed, grad, w_grad)
    return (mixed[None], grad[None], w_grad)


def solution(mesh):
    n_dp, n_seq = mesh.shape["dp"], mesh.shape["seq"]

    def body(*args):
        tokens, stamps, w_out = args[0], args[2], args[5]
        mesh_fits = n_seq == 4 and n_dp == 2 * n_seq and n_dp == H
        sizes_fit = w_out.shape[0] == DH and tokens.shape[1] == DH
        if mesh_fits and sizes_fit and stamps.shape == (1, n_seq * DH):
            return column_parallel(n_dp, n_seq, *args)
        return per_device(*args)

    return jax.shard_map(
        body,
        mesh=mesh,
        in_specs=(
            P("dp", "seq", None),
            P("dp", "seq", None),
            P("dp", None),
            P("dp"),
            P("dp", None),
            P("dp", None),
            P(),
            P(),
            P(),
        ),
        out_specs=(P("dp", "seq", None), P("dp", "seq", None), P("dp", None)),
        check_vma=False,
    )
```

```python
import jax
import jax.numpy as jnp
from jax import lax
from jax.experimental import pallas as pl
from jax.experimental.pallas import tpu as pltpu
from jax.sharding import PartitionSpec as P

H = 8
DH = 128


EPS = 1e-05


def layer_norm(values, gain):
    average = jnp.mean(values, axis=-1, keepdims=True)
    centred = values - average
    variance = jnp.mean(centred * centred, axis=-1, keepdims=True)
    return centred * lax.rsqrt(variance + EPS) * gain


def silu_slope(values):
    sigmoid_v = jax.nn.sigmoid(values)
    return sigmoid_v * (1.0 + values * (1.0 - sigmoid_v))


def time_bias(bias_table, stamps_q, stamps_k):
    elapsed = stamps_q[:, None] - stamps_k[None, :]
    bucket = jnp.zeros(elapsed.shape, jnp.int32)
    for degree in range(1, bias_table.shape[1]):
        bucket = bucket + (elapsed >= 2**degree - 1).astype(jnp.int32)
    levels = jnp.arange(bias_table.shape[1], dtype=jnp.int32)
    one_hot = (bucket[:, :, None] == levels[None, None, :]).astype(jnp.float32)
    return jnp.einsum(
        "qkb,hb->hqk",
        one_hot,
        bias_table,
        precision=lax.Precision.HIGHEST,
        preferred_element_type=jnp.float32,
    )


def pair_terms(
    q_heads, d_heads, stamps_q, pos_q, k_heads, v_heads, stamps_k, pos_k, length, bias_table, scale
):
    scores = (
        jnp.einsum("qhd,khd->hqk", q_heads, k_heads, preferred_element_type=jnp.float32) * scale
    )
    scores = scores + time_bias(bias_table, stamps_q, stamps_k)
    allowed = (
        (pos_k[None, :] <= pos_q[:, None]) & (pos_k[None, :] < length) & (pos_q[:, None] < length)
    )
    weight = jnp.where(allowed[None], jax.nn.silu(scores), 0.0).astype(jnp.bfloat16)
    if d_heads is None:
        return (weight, None)
    d_weight = jnp.einsum("qhd,khd->hqk", d_heads, v_heads, preferred_element_type=jnp.float32)
    d_scores = jnp.where(allowed[None], d_weight * silu_slope(scores), 0.0).astype(jnp.bfloat16)
    return (weight, d_scores)


def per_device(tokens, cotangent, stamps, lengths, w_qkvu, w_out, gain_in, gain_out, bias_table):
    rows = tokens[0]
    cot_rows = cotangent[0]
    tok_count = rows.shape[0]
    feature_width = rows.shape[1]
    seq_count = lax.axis_size("seq")
    total_rows = tok_count * seq_count
    first_row = lax.axis_index("seq") * tok_count
    length = lengths[0]
    stamp_all = stamps[0]
    pos_own = first_row + jnp.arange(tok_count, dtype=jnp.int32)
    stamp_own = lax.dynamic_slice_in_dim(stamp_all, first_row, tok_count)
    scale = DH ** (-0.5)
    block_rows = min(512, total_rows)
    block_count = total_rows // block_rows
    w_full, w_out_full = (
        lax.all_gather(w_qkvu, "dp", axis=0, tiled=True),
        lax.all_gather(w_out, "dp", axis=0, tiled=True),
    )
    wide_rows = rows.astype(jnp.float32)
    normed = layer_norm(wide_rows, gain_in).astype(jnp.bfloat16)
    projected = jnp.dot(normed, w_full, preferred_element_type=jnp.float32)
    activated = jax.nn.silu(projected)
    gate_u = activated[:, :feature_width]
    values_own = activated[:, feature_width : 2 * feature_width].astype(jnp.bfloat16)
    queries_own = activated[:, 2 * feature_width : 3 * feature_width].astype(jnp.bfloat16)
    keys_own = activated[:, 3 * feature_width :].astype(jnp.bfloat16)
    keys_all, values_all = (
        lax.all_gather(keys_own, "seq", axis=0, tiled=True),
        lax.all_gather(values_own, "seq", axis=0, tiled=True),
    )
    q_heads = queries_own.reshape(tok_count, H, DH)

    def key_block(start):
        k_heads = lax.dynamic_slice_in_dim(keys_all, start, block_rows).reshape(block_rows, H, DH)
        v_heads = lax.dynamic_slice_in_dim(values_all, start, block_rows).reshape(block_rows, H, DH)
        stamps_k = lax.dynamic_slice_in_dim(stamp_all, start, block_rows)
        pos_k = start + jnp.arange(block_rows, dtype=jnp.int32)
        return (k_heads, v_heads, stamps_k, pos_k)

    def guarded(active, action, state):
        return lax.cond(active, action, lambda same: same, state)

    def reaches(start):
        return (start <= first_row + tok_count - 1) & (start < length) & (first_row < length)

    def forward_step(block_idx, totals):
        start = block_idx * block_rows

        def forward_compute(totals):
            k_heads, v_heads, stamps_k, pos_k = key_block(start)
            weight, unused = pair_terms(
                q_heads,
                None,
                stamp_own,
                pos_own,
                k_heads,
                v_heads,
                stamps_k,
                pos_k,
                length,
                bias_table,
                scale,
            )
            return totals + jnp.einsum(
                "hqk,khd->qhd", weight, v_heads, preferred_element_type=jnp.float32
            )

        return guarded(reaches(start), forward_compute, totals)

    attended = lax.fori_loop(
        0, block_count, forward_step, jnp.zeros((tok_count, H, DH), jnp.float32)
    )
    attended = attended.reshape(tok_count, feature_width)
    normed_att, norm_back = jax.vjp(lambda values: layer_norm(values, gain_out), attended)
    mixed_rows = (normed_att * gate_u).astype(jnp.bfloat16)
    mixed = (
        wide_rows + jnp.dot(mixed_rows, w_out_full, preferred_element_type=jnp.float32)
    ).astype(jnp.bfloat16)
    grad_part = lax.psum_scatter(
        jnp.einsum("tr,tc->rc", mixed_rows, cot_rows, preferred_element_type=jnp.float32).astype(
            jnp.bfloat16
        ),
        "dp",
        scatter_dimension=0,
        tiled=True,
    )
    w_grad = lax.psum(grad_part, "seq").astype(jnp.float32)
    d_mix = jnp.einsum("tc,rc->tr", cot_rows, w_out_full, preferred_element_type=jnp.float32)
    d_gate = d_mix * normed_att
    d_att = norm_back(d_mix * gate_u)[0].astype(jnp.bfloat16)
    d_heads = d_att.reshape(tok_count, H, DH)

    def backward_step():

        def step(block_idx, state_pair):
            start = block_idx * block_rows

            def step_compute(state_pair):
                q_grad, key_terms = state_pair
                k_heads, v_heads, stamps_k, pos_k = key_block(start)
                weight, d_scores = pair_terms(
                    q_heads,
                    d_heads,
                    stamp_own,
                    pos_own,
                    k_heads,
                    v_heads,
                    stamps_k,
                    pos_k,
                    length,
                    bias_table,
                    scale,
                )
                q_grad = (
                    q_grad
                    + jnp.einsum(
                        "hqk,khd->qhd", d_scores, k_heads, preferred_element_type=jnp.float32
                    )
                    * scale
                )
                k_grad = (
                    jnp.einsum(
                        "hqk,qhd->khd", d_scores, q_heads, preferred_element_type=jnp.float32
                    )
                    * scale
                )
                v_grad = jnp.einsum(
                    "hqk,qhd->khd", weight, d_heads, preferred_element_type=jnp.float32
                )
                joined = jnp.concatenate(
                    [
                        k_grad.reshape(block_rows, feature_width),
                        v_grad.reshape(block_rows, feature_width),
                    ],
                    axis=1,
                )
                key_terms = lax.dynamic_update_slice_in_dim(key_terms, joined, start, 0)
                return (q_grad, key_terms)

            return guarded(reaches(start), step_compute, state_pair)

        return step

    q_start = jnp.zeros((tok_count, H, DH), jnp.float32)
    term_start = jnp.zeros((total_rows, 2 * feature_width), jnp.float32)
    q_grad, key_terms = lax.fori_loop(0, block_count, backward_step(), (q_start, term_start))
    key_grads = lax.psum_scatter(
        key_terms.astype(jnp.bfloat16), "seq", scatter_dimension=0, tiled=True
    ).astype(jnp.float32)
    d_act = jnp.concatenate(
        [
            d_gate,
            key_grads[:, feature_width:],
            q_grad.reshape(tok_count, feature_width),
            key_grads[:, :feature_width],
        ],
        axis=1,
    )
    d_proj = (d_act * silu_slope(projected)).astype(jnp.bfloat16)
    d_normed = jnp.einsum("tf,df->td", d_proj, w_full, preferred_element_type=jnp.float32)
    unused_rows, in_back = jax.vjp(lambda values: layer_norm(values, gain_in), wide_rows)
    input_grad = (cot_rows.astype(jnp.float32) + in_back(d_normed)[0]).astype(jnp.bfloat16)
    return (mixed[None], input_grad[None], w_grad)


MESH = pl.DeviceIdType.MESH
VM = pl.BlockSpec(memory_space=pltpu.VMEM)
F32 = jnp.float32
BF16 = jnp.bfloat16
MASKED = -1e30
PIECES = 4


def mm(a, b, dims):
    return lax.dot_general(a, b, (dims, ((), ())), preferred_element_type=F32)


def remote(src, dst, send_sem, recv_sem, target):
    return pltpu.make_async_remote_copy(
        src_ref=src,
        dst_ref=dst,
        send_sem=send_sem,
        recv_sem=recv_sem,
        device_id=target,
        device_id_type=MESH,
    )


def arrived(dst, sem):
    pltpu.make_async_copy(dst, dst, sem).wait()


def sent(block, sem, target):
    remote(block, block, sem, sem, target).wait_send()


def column_kernel(
    n_dp, n_seq, w_hbm, x_hbm, c_hbm, wo_hbm, stamps_hbm, length_ref, gin_hbm, gout_hbm, bias_hbm,
    mixed_ref, grad_ref, wg_ref,
    w_ref, x_ref, c_ref, wo_ref, stamps_ref, gin_ref, gout_ref, bias_ref, meta_ref,
    W, X, C, WO, mbuf, NB, BI, PJ, GT, ACT, ATT, WT, SL, DM, DG, DA, DP, MR, MX, KA, VA, SA, SG, TB,
    MW, WG, PS, PR, TS, TR, MA, MB, PB, SB, CS, FB, FIN, RO,
    lsem, wout, wvia, wrest, zout, shareout, farout, xrecv, woout, worecv, msem,
    saout, sarecv, sgout, sgrecv, mxout, mxrecv, gout, grecv,
    hout, hmid, hback, trecv, pout, precv, cout, crecv, oout, orecv,
):
    me = lax.axis_index("dp")
    z = lax.axis_index("seq")
    tok, width = x_ref.shape
    rows = tok * n_seq
    half = tok // 2
    n_heads = n_dp
    scale = DH ** (-0.5)
    chip, k = me // 2, me % 2
    cy, cx = chip // 2, chip % 2
    xn, yn = 2 * cy + (1 - cx), 2 * (1 - cy) + cx
    dn = 2 * (1 - cy) + (1 - cx)
    sib = 2 * chip + (1 - k)
    p, ks = z % 2, z // 2
    near, far = 1 + ks, (n_seq - 1) * ks
    zp = near + far - z
    is_near, is_far = z == near, z == far
    is_main = k == ks
    is_aux = jnp.logical_not(is_main)
    main_dp = 2 * chip + ks

    def head_of(core, j):
        return 4 * core + 2 * j + p

    def rows_of(ref_rows, index):
        return pl.ds(pl.multiple_of(index * ref_rows, ref_rows), ref_rows)

    def lanes_of(index):
        return pl.ds(pl.multiple_of(index * DH, DH), DH)

    def w_copies(core, j, make):
        return [
            make(
                w_ref.at[:, lanes_of(g * n_heads + head_of(core, j))],
                W.at[j, rows_of(tok, me), slice(g * DH, (g + 1) * DH)],
            )
            for g in range(4)
        ]

    w_targets = (
        (xn, 0, wvia.at[k]), (yn, 1, wvia.at[k]), (chip, 1 - k, wrest), (xn, 1, wrest),
        (yn, 0, wrest),
    )

    def w_start(j):
        for where, core, sem in w_targets:
            for copy in w_copies(
                core, j, lambda s, d: remote(s, d, wout, sem.at[j], (2 * where + core, z))
            ):
                copy.start()

    def w_piece(src, j):
        return W.at[j, rows_of(tok, src)]

    via, to = (1 - k) * xn + k * yn, (1 - k) * yn + k * xn

    def w_relay(i, j):
        src = 2 * via + i
        block = w_piece(src, j)
        return remote(block, block, wout, wrest.at[j], (2 * to + k, z))

    ins, outs = (x_ref, c_ref), (X, C)
    z_to = jnp.where(is_main, zp, 1 + k)

    def z_send(a):
        return remote(ins[a], outs[a].at[z], zout, xrecv.at[a, z], (me, z_to))

    def own_copy(a):
        return pltpu.make_async_copy(ins[a], outs[a].at[z], xrecv.at[a, z])

    def share(a, b):
        block = ins[a] if b is None else outs[a].at[b]
        at = z if b is None else b
        return remote(block, outs[a].at[at], shareout, xrecv.at[a, at], (sib, z))

    foreign = (2 * (1 - ks), 2 * (1 - ks) + 1)

    def to_far(a, i):
        block = outs[a].at[foreign[i]]
        return remote(block, block, farout, xrecv.at[a, foreign[i]], (me, far))

    def x_wait(a, b):
        arrived(outs[a].at[b], xrecv.at[a, b])

    def meta_send():
        return remote(meta_ref, mbuf, msem.at[0], msem.at[1], (sib, z))

    wo_core, wo_slot = chip // 2, chip % 2
    wo_part = 2 * k + wo_core
    wo_here = wo_core == k
    wo_sem = jnp.where(k == p, wo_slot, 2)
    wo_sends = [
        remote(
            wo_ref, WO.at[wo_part, wo_slot], woout, worecv.at[wo_sem],
            (2 * where + wo_core, z),
        )
        for i, where in enumerate((xn, yn, dn, chip))
    ]

    def wo_start():
        for i in range(3):
            wo_sends[i].start()

        @pl.when(wo_here)
        def _():
            pltpu.make_async_copy(wo_ref, WO.at[wo_part, wo_slot], worecv.at[wo_sem]).start()

        @pl.when(jnp.logical_not(wo_here))
        def _():
            wo_sends[3].start()

    def wo_share(parity, j):
        block = WO.at[2 * parity + k, j]
        return remote(block, block, woout, worecv.at[3], (sib, z))

    loads = [
        pltpu.make_async_copy(src, dst, lsem.at[i])
        for src, dst, i in (
            (stamps_hbm, stamps_ref, 0), (w_hbm, w_ref, 1), (x_hbm, x_ref, 1), (c_hbm, c_ref, 1),
            (wo_hbm, wo_ref, 1), (gin_hbm, gin_ref, 2), (gout_hbm, gout_ref, 3),
            (bias_hbm, bias_ref, 4),
        )
    ]
    barrier = pltpu.get_barrier_semaphore()
    for step in range(1, n_dp):
        pl.semaphore_signal(
            barrier, inc=1, device_id=(lax.rem(me + step, n_dp), z), device_id_type=MESH
        )
    for step in range(1, n_seq):
        there = lax.rem(z + step, n_seq)

        @pl.when(jnp.abs(there - z) < n_seq - 1)
        def _():
            for peer in (me, sib):
                pl.semaphore_signal(
                    barrier, inc=1, device_id=(peer, there), device_id_type=MESH
                )

    for load in loads:
        load.start()
    loads[0].wait()
    meta_ref[0:1, :] = stamps_ref[...]
    meta_ref[1:2, :] = jnp.full(stamps_ref.shape, length_ref[0], jnp.int32)
    arrived(W.at[:, : (n_dp - 1) * tok], lsem.at[1])
    for load in loads[5:]:
        load.wait()
    inner = jnp.where((z > 0) & (z < n_seq - 1), 1, 0)
    pl.semaphore_wait(barrier, n_dp - 1 + 2 * (n_seq - 2) + 2 * inner)
    @pl.when(is_main)
    def _():
        pltpu.make_async_copy(meta_ref, mbuf, msem.at[1]).start()
        meta_send().start()

    w_start(0)
    z_send(0).start()

    @pl.when(is_main)
    def _():
        own_copy(0).start()
        share(0, None).start()

    z_send(1).start()

    @pl.when(is_main)
    def _():
        own_copy(1).start()
        share(1, None).start()

    for j in range(2):
        for copy in w_copies(k, j, lambda s, d: pltpu.make_async_copy(s, d, wrest.at[j])):
            copy.start()

    def relay_weights(j):
        for i in range(2):
            arrived(w_piece(2 * via + i, j), wvia.at[i, j])
            w_relay(i, j).start()

    def near_relay(a):
        @pl.when(is_main)
        def _():
            x_wait(a, zp)
            share(a, zp).start()

        @pl.when(is_main & is_near)
        def _():
            for i in range(2):
                x_wait(a, foreign[i])
                to_far(a, i).start()
                share(a, foreign[i]).start()

    def far_relay(a):
        @pl.when(is_main & is_far)
        def _():
            for i in range(2):
                x_wait(a, foreign[i])
                share(a, foreign[i]).start()

    relay_weights(0)
    w_start(1)
    near_relay(0)

    arrived(mbuf, msem.at[1])
    lane_row = lax.broadcasted_iota(jnp.int32, (DH, DH), 0)
    lane_col = lax.broadcasted_iota(jnp.int32, (DH, DH), 1)
    length = mbuf[1:2, :DH]
    for i in range(n_seq):
        col = jnp.broadcast_to(mbuf[0:1, i * DH : (i + 1) * DH].astype(F32), (DH, DH)).T
        valid = lane_row + i * DH < length
        for b in range(i + 1):
            elapsed = col - mbuf[0:1, b * DH : (b + 1) * DH].astype(F32)
            allowed = valid & (lane_col <= lane_row) if b == i else valid
            heads = [head_of(k, j) for j in range(2)]
            terms = [jnp.full(elapsed.shape, bias_ref[h, 0], F32) for h in heads]
            for degree in range(1, bias_ref.shape[1]):
                reached = elapsed >= float(2**degree - 1)
                terms = [
                    jnp.where(reached, bias_ref[h, degree], t) for h, t in zip(heads, terms)
                ]
            for j in range(2):
                BI[j, i * DH : (i + 1) * DH, b * DH : (b + 1) * DH] = jnp.where(
                    allowed, terms[j], MASKED
                )

    near_relay(1)
    relay_weights(1)

    far_relay(0)

    @pl.when(is_main)
    def _():
        x_wait(0, z)

    @pl.when(is_aux)
    def _():
        for b in range(n_seq):
            x_wait(0, b)

    for b in range(n_seq):
        NB[b * tok : (b + 1) * tok, :] = layer_norm(X[b].astype(F32), gin_ref[...]).astype(BF16)

    def forward(j):
        arrived(W.at[j, : (n_dp - 2) * tok], wrest.at[j])
        PJ[j] = mm(NB[...], W[j], ((1,), (0,)))
        cols = slice(j * DH, (j + 1) * DH)
        GT[:, cols] = jax.nn.silu(PJ[j, :, :DH])
        for g in range(3):
            ACT[j, g] = jax.nn.silu(PJ[j, :, (1 + g) * DH : (2 + g) * DH]).astype(BF16)
        for i in range(n_seq):
            at, end = slice(i * tok, (i + 1) * tok), (i + 1) * tok
            scores = mm(ACT[j, 1, at], ACT[j, 2, :end], ((1,), (1,))) * scale + BI[j, at, :end]
            sig = jax.nn.sigmoid(scores)
            weight = (scores * sig).astype(BF16)
            WT[j, at, :end] = weight
            SL[j, at, :end] = sig * (1.0 + scores * (1.0 - sig))
            ATT[at, cols] = mm(weight, ACT[j, 0, :end], ((1,), (0,)))

    @pl.when(k == p)
    def _():
        wo_start()

    forward(0)

    forward(1)

    gain = jnp.concatenate([gout_ref[:, lanes_of(head_of(k, j))] for j in range(2)], axis=1)
    pid = 2 * p + k
    own_width = 2 * DH
    st_peers = ((sib, z), (me, zp), (sib, zp))

    def stat_sends(ref, send_sem, recv_sem):
        return [
            remote(ref.at[pid], ref.at[pid], send_sem, recv_sem, peer)
            for peer in st_peers
        ]

    def put_stats(ref, at, first, second):
        ref[pid, :, at] = jnp.where(lane_col == 0, first, second).T[:8]

    for b in range(n_seq):
        at = slice(b * tok, (b + 1) * tok)
        att = ATT[at, :]
        mean_own = jnp.mean(att, axis=1, keepdims=True)
        off = att - mean_own
        put_stats(SA, at, mean_own, jnp.sum(off * off, axis=1, keepdims=True))
    for copy in stat_sends(SA, saout, sarecv):
        copy.start()
    far_relay(1)
    @pl.when(is_main)
    def _():
        x_wait(1, z)

    @pl.when(is_aux)
    def _():
        for b in range(n_seq):
            x_wait(1, b)

    c_rows = C[...].reshape(rows, width)
    for j in range(2):
        arrived(WO.at[pid, j], worecv.at[j])
        wo_share(p, j).start()
        DM[:, j * DH : (j + 1) * DH] = mm(c_rows, WO[pid, j], ((1,), (1,)))
    for b in range(n_seq):
        at = slice(b * tok, (b + 1) * tok)
        att = ATT[at, :]
        off = att - jnp.mean(att, axis=1, keepdims=True)
        g = DM[at, :] * GT[at, :] * gain
        put_stats(
            SG, at, jnp.sum(g, axis=1, keepdims=True), jnp.sum(g * off, axis=1, keepdims=True)
        )
    for copy in stat_sends(SG, sgout, sgrecv):
        copy.start()

    arrived(SA.at[:3], sarecv)
    means = [SA[q, 0:1, :] for q in range(4)]
    mean = sum(means[1:], means[0]) / 4.0
    shifts = [m - mean for m in means]
    squares = sum(SA[q, 1:2, :] + own_width * shifts[q] * shifts[q] for q in range(4))
    rstd = lax.rsqrt(squares / width + EPS)
    TB[...] = jnp.concatenate([mean, rstd] * 4, axis=0)

    def turned(at):
        return jnp.concatenate([TB[:, at]] * (DH // 8), axis=0).T

    blocks = tuple(reversed(range(n_seq)))

    def mine(b):
        return is_near == (far != b)

    def other(b):
        return is_near == (far == b)

    def home_is_self(b):
        return is_main & (z == b)

    def mx_send(b):
        return remote(
            MR.at[b * tok : (b + 1) * tok], MX.at[pid], mxout, mxrecv, (main_dp, b)
        )

    for b in blocks:
        at = slice(b * tok, (b + 1) * tok)
        columns = turned(at)
        hat = (ATT[at, :] - columns[:, 0:1]) * columns[:, 1:2]
        ATT[at, :] = hat
        MR[at, :] = (hat * gain * GT[at, :]).astype(BF16)

    pieces = PIECES
    piece = DH // pieces

    def out_rows(i):
        return slice(i * piece, (i + 1) * piece)

    def g_send(j, i):
        return remote(
            MW.at[j, i], WG.at[chip, i], gout, grecv.at[i],
            (2 * (2 * k + j) + p, z),
        )

    def g_self(j):
        return (2 * k + j == chip) & (k == p)

    for j in range(2):
        part = mm(MR[:, j * DH : (j + 1) * DH], c_rows, ((0,), (0,)))
        for i in range(pieces):
            MW[j, i] = part[out_rows(i)].astype(BF16)
    for i in range(pieces):
        for j in range(2):

            @pl.when(g_self(j))
            def _():
                pltpu.make_async_copy(MW.at[j, i], WG.at[chip, i], grecv.at[i]).start()

            @pl.when(jnp.logical_not(g_self(j)))
            def _():
                g_send(j, i).start()

    is_root = k == p
    far_root, near_root, middle, edge = (n_seq - 1) * k, 2 - k, 1 + k, (n_seq - 1) * (1 - k)
    def h_send(dst, recv, i):
        return remote(PS.at[i], dst.at[i], hout, recv.at[i], (me, middle))

    def h_relay(src, i, to):
        return remote(src.at[i], PR.at[i], hout, hback.at[i], (me, to))

    def t_send(i):
        return remote(TS.at[i], TR.at[i], hout, trecv.at[i], (me, edge))

    def plane_sum(i):
        @pl.when(is_root)
        def _():
            arrived(WG.at[:, i], grecv.at[i])
            total = WG[0, i].astype(F32)
            for c in range(1, n_dp // 2):
                total = total + WG[c, i].astype(F32)
            PS[i] = total.astype(BF16)

            @pl.when(z == far_root)
            def _():
                h_send(MA, hmid.at[0], i).start()

            @pl.when(z == near_root)
            def _():
                h_send(MB, hmid.at[1], i).start()

    def pass_in():
        @pl.when(z == middle)
        def _():
            for i in range(pieces):
                arrived(MB.at[i], hmid.at[1, i])
                h_relay(MB, i, far_root).start()

    def pass_out():
        @pl.when(z == middle)
        def _():
            for i in range(pieces):
                arrived(MA.at[i], hmid.at[0, i])
                h_relay(MA, i, near_root).start()
                wg_ref[out_rows(i)] = (MA[i].astype(F32) + MB[i].astype(F32)).astype(BF16)

    def root_total(i):
        arrived(PR.at[i], hback.at[i])
        TS[i] = (PS[i].astype(F32) + PR[i].astype(F32)).astype(BF16)
        wg_ref[out_rows(i)] = TS[i]

    def near_total():
        @pl.when(z == near_root)
        def _():
            for i in range(pieces):
                root_total(i)
                t_send(i).start()

    def outer_total():
        @pl.when(z == far_root)
        def _():
            for i in range(pieces):
                root_total(i)

        @pl.when(z == edge)
        def _():
            for i in range(pieces):
                arrived(TR.at[i], trecv.at[i])
                wg_ref[out_rows(i)] = TR[i]

    def pair_send(b):
        return remote(PB.at[b, 1 - k], SB.at[b], pout, precv.at[b], (sib, z))

    def cross_send(b):
        return remote(CS.at[b], FB.at[b], cout, crecv.at[b], (me, zp))

    def home_send(b):
        return remote(FIN.at[b], RO.at[k], oout, orecv, (main_dp, b))

    def pair_sum(b):
        return PB[b, k].astype(F32) + SB[b].astype(F32)

    def cross(b):
        arrived(SB.at[b], precv.at[b])

        @pl.when(other(b))
        def _():
            CS[b] = pair_sum(b).astype(BF16)
            cross_send(b).start()

    def finish(b):
        @pl.when(mine(b))
        def _():
            arrived(FB.at[b], crecv.at[b])
            FIN[b] = (pair_sum(b) + FB[b].astype(F32)).astype(BF16)

            @pl.when(home_is_self(b))
            def _():
                pltpu.make_async_copy(FIN.at[b], RO.at[k], orecv).start()

            @pl.when(jnp.logical_not(home_is_self(b)))
            def _():
                home_send(b).start()

    arrived(SG.at[:3], sgrecv)
    for b in blocks:

        @pl.when(home_is_self(b))
        def _():
            pltpu.make_async_copy(
                MR.at[b * tok : (b + 1) * tok], MX.at[pid], mxrecv
            ).start()

        @pl.when(jnp.logical_not(home_is_self(b)))
        def _():
            mx_send(b).start()

    g_mean = sum(SG[q, 0:1, :] for q in range(4)) / width
    g_dot = rstd * sum(SG[q, 1:2, :] + shifts[q] * SG[q, 0:1, :] for q in range(4)) / width
    TB[...] = jnp.concatenate([rstd, g_mean, g_dot, rstd] * 2, axis=0)
    for b in range(n_seq):
        at = slice(b * tok, (b + 1) * tok)
        columns = turned(at)
        d_mix, hat = DM[at, :], ATT[at, :]
        DG[at, :] = d_mix * (hat * gain)
        g = d_mix * GT[at, :] * gain
        DA[at, :] = (
            columns[:, 0:1] * (g - columns[:, 1:2] - hat * columns[:, 2:3])
        ).astype(BF16)

    def backward(j, b):
        cols = slice(j * DH, (j + 1) * DH)
        start, end = b * tok, (b + 1) * tok

        def put(group, grad):
            at = slice(group * DH, (group + 1) * DH)
            DP[j, start:end, at] = (grad * silu_slope(PJ[j, start:end, at])).astype(BF16)

        d_att = DA[start:end, cols]
        d_weight = mm(d_att, ACT[j, 0, :end], ((1,), (1,)))
        d_scores = (d_weight * SL[j, start:end, :end]).astype(BF16)
        put(2, mm(d_scores, ACT[j, 2, :end], ((1,), (0,))) * scale)
        k_part = mm(d_scores, ACT[j, 1, start:end], ((0,), (0,)))
        v_part = mm(WT[j, start:end, :end], d_att, ((0,), (0,)))
        if end == rows:
            KA[j] = k_part
            VA[j] = v_part
        else:
            KA[j, :end] += k_part
            VA[j, :end] += v_part
        put(0, DG[start:end, cols])
        put(1, VA[j, start:end])
        put(3, KA[j, start:end] * scale)

    def d_part(b):
        at = slice(b * tok, (b + 1) * tok)
        part = mm(DP[0, at], W[0], ((1,), (1,))) + mm(DP[1, at], W[1], ((1,), (1,)))
        PB[b, 0] = part[:half].astype(BF16)
        PB[b, 1] = part[half:].astype(BF16)
        pair_send(b).start()

    last = n_seq - 1
    for b in blocks:
        for j in range(2):
            backward(j, b)
        if b == last:

            @pl.when(ks == 0)
            def _():
                d_part(last)

        else:
            d_part(b)
        if b == last - 1:

            @pl.when(ks == 0)
            def _():
                cross(last)

        elif b == 1:
            cross(2)
        if b < 2:
            for i in range(pieces // 2):
                plane_sum((1 - b) * pieces // 2 + i)
    cross(1)
    cross(0)

    @pl.when(k != p)
    def _():
        wo_start()

    @pl.when(ks != 0)
    def _():
        d_part(last)
        cross(last)

    finish(3)
    pass_in()
    finish(2)
    pass_out()
    finish(1)
    finish(0)
    near_total()
    arrived(WO.at[2 * (1 - p) + k], worecv.at[2])
    for j in range(2):
        wo_share(1 - p, j).start()

    arrived(X, worecv.at[3])
    arrived(MX, mxrecv)
    wide = x_ref[...].astype(F32)
    total = wide
    for q in range(4):
        total = total + mm(MX[q], WO[q].reshape(2 * DH, width), ((1,), (0,)))
    mixed_ref[...] = total.astype(BF16)

    average = jnp.mean(wide, axis=-1, keepdims=True)
    centred = wide - average
    inv = lax.rsqrt(jnp.mean(centred * centred, axis=-1, keepdims=True) + EPS)
    hat = centred * inv
    outer_total()
    arrived(RO, orecv)
    grad = RO[...].reshape(tok, width).astype(F32) * gin_ref[...]
    back = inv * (
        grad
        - jnp.mean(grad, axis=-1, keepdims=True)
        - hat * jnp.mean(grad * hat, axis=-1, keepdims=True)
    )
    grad_ref[...] = (c_ref[...].astype(F32) + back).astype(BF16)

    beside = (sib, z)

    def sent_when(condition, block, sem):
        @pl.when(condition)
        def _():
            sent(block, sem, beside)

    part = (n_dp - 1) * tok
    sent(W.at[:, :part], wout, beside)
    sent(X.at[:2], zout, beside)
    sent_when(is_main, W, shareout)
    sent_when(is_main & is_near, X, farout)
    sent_when(is_main, meta_ref, msem.at[0])
    sent_when(wo_here, W.at[:, :part], woout)
    sent_when(jnp.logical_not(wo_here), W, woout)
    sent(SA.at[:3], saout, beside)
    sent(SG.at[:3], sgout, beside)
    sent_when(is_main, MX.at[:3], mxout)
    sent_when(is_aux, MX, mxout)
    keeps_one = is_root & wo_here
    sent_when(keeps_one, X.at[0], gout)
    sent_when(jnp.logical_not(keeps_one), X.at[:2], gout)
    sent_when(z == far_root, PS, hout)
    sent_when((z == near_root) | (z == middle), X.at[:2], hout)
    sent(X.at[:2], pout, beside)
    sent_when(is_far, CS.at[:3], cout)
    sent_when(is_near, CS.at[:1], cout)
    sent_when(is_near & is_main, FIN.at[:2], oout)
    sent_when(is_near & is_aux, FIN.at[:3], oout)
    sent_when(is_far & is_aux, FIN.at[:1], oout)


def tail_kernel(mixed_ref, grad_ref, wg_ref, mixed_out, grad_out, wg_out, wide, sems):
    copies = [
        pltpu.make_async_copy(src, dst, sems.at[i])
        for i, (src, dst) in enumerate(
            ((mixed_ref, mixed_out), (grad_ref, grad_out), (wide, wg_out))
        )
    ]
    copies[0].start()
    copies[1].start()
    wide[...] = wg_ref[...].astype(F32)
    copies[2].start()
    for copy in copies:
        copy.wait()


def column_parallel(
    n_dp, n_seq, tokens, cotangent, stamps, lengths, w_qkvu, w_out, gain_in, gain_out, bias_table
):
    tok, width = tokens.shape[1:]
    rows = tok * n_seq
    dma = pltpu.SemaphoreType.DMA
    sds = jax.ShapeDtypeStruct
    hbm = pl.BlockSpec(memory_space=pltpu.HBM)

    def vb(*shape):
        return pltpu.VMEM(shape, BF16)

    def vf(*shape):
        return pltpu.VMEM(shape, F32)

    def in_hbm(value):
        return pltpu.with_memory_space_constraint(value, pltpu.HBM)

    half = tok // 2
    mixed, grad, w_grad = pl.pallas_call(
        lambda *refs: column_kernel(n_dp, n_seq, *refs),
        out_shape=(sds((tok, width), BF16), sds((tok, width), BF16), sds(w_out.shape, BF16)),
        in_specs=[hbm] * 5 + [pl.BlockSpec(memory_space=pltpu.SMEM)] + [hbm] * 3,
        out_specs=[VM] * 3,
        scratch_shapes=[
            pltpu.VMEM(w_qkvu.shape, BF16),
            vb(tok, width),
            vb(tok, width),
            vb(DH, width),
            pltpu.VMEM(stamps.shape, jnp.int32),
            vf(1, width),
            vf(1, width),
            pltpu.SMEM(bias_table.shape, F32),
            pltpu.VMEM((8, rows), jnp.int32),
            vb(2, width, 4 * DH),
            vb(n_seq, tok, width),
            vb(n_seq, tok, width),
            vb(4, 2, DH, width),
            pltpu.VMEM((8, rows), jnp.int32),
            vb(rows, width),
            vf(2, rows, rows),
            vf(2, rows, 4 * DH),
            vf(rows, 2 * DH),
            vb(2, 3, rows, DH),
            vf(rows, 2 * DH),
            vb(2, rows, rows),
            vf(2, rows, rows),
            vf(rows, 2 * DH),
            vf(rows, 2 * DH),
            vb(rows, 2 * DH),
            vb(2, rows, 4 * DH),
            vb(rows, 2 * DH),
            vb(4, tok, 2 * DH),
            vf(2, rows, DH),
            vf(2, rows, DH),
            vf(4, 8, rows),
            vf(4, 8, rows),
            vf(8, rows),
            vb(2, PIECES, DH // PIECES, width),
            vb(n_dp // 2, PIECES, DH // PIECES, width),
            vb(PIECES, DH // PIECES, width),
            vb(PIECES, DH // PIECES, width),
            vb(PIECES, DH // PIECES, width),
            vb(PIECES, DH // PIECES, width),
            vb(PIECES, DH // PIECES, width),
            vb(PIECES, DH // PIECES, width),
            vb(n_seq, 2, half, width),
            vb(n_seq, half, width),
            vb(n_seq, half, width),
            vb(n_seq, half, width),
            vb(n_seq, half, width),
            vb(2, half, width),
            dma((5,)),
            dma,
            dma((2, 2)),
            dma((2,)),
            dma,
            dma,
            dma,
            dma((2, n_seq)),
            dma,
            dma((4,)),
            dma((2,)),
            dma,
            dma,
            dma,
            dma,
            dma,
            dma,
            dma,
            dma((PIECES,)),
            dma,
            dma((2, PIECES)),
            dma((PIECES,)),
            dma((PIECES,)),
            dma,
            dma((n_seq,)),
            dma,
            dma((n_seq,)),
            dma,
            dma,
        ],
        compiler_params=pltpu.CompilerParams(
            has_side_effects=True, collective_id=0, vmem_limit_bytes=44 * 2**20
        ),
        name="column",
    )(
        *[in_hbm(v) for v in (w_qkvu, tokens[0], cotangent[0], w_out, stamps)],
        lengths,
        *[in_hbm(v) for v in (gain_in[None], gain_out[None], bias_table)],
    )
    mixed, grad, w_grad = pl.pallas_call(
        tail_kernel,
        out_shape=(sds(mixed.shape, BF16), sds(grad.shape, BF16), sds(w_grad.shape, F32)),
        in_specs=[VM] * 3,
        out_specs=[hbm] * 3,
        scratch_shapes=[vf(*w_grad.shape), dma((3,))],
        compiler_params=pltpu.CompilerParams(vmem_limit_bytes=8 * 2**20),
        name="tail",
    )(mixed, grad, w_grad)
    return (mixed[None], grad[None], w_grad)


def solution(mesh):
    n_dp, n_seq = mesh.shape["dp"], mesh.shape["seq"]

    def body(*args):
        tokens, stamps, w_out = args[0], args[2], args[5]
        mesh_fits = n_seq == 4 and n_dp == 2 * n_seq and n_dp == H
        sizes_fit = w_out.shape[0] == DH and tokens.shape[1] == DH
        if mesh_fits and sizes_fit and stamps.shape == (1, n_seq * DH):
            return column_parallel(n_dp, n_seq, *args)
        return per_device(*args)

    return jax.shard_map(
        body,
        mesh=mesh,
        in_specs=(
            P("dp", "seq", None),
            P("dp", "seq", None),
            P("dp", None),
            P("dp"),
            P("dp", None),
            P("dp", None),
            P(),
            P(),
            P(),
        ),
        out_specs=(P("dp", "seq", None), P("dp", "seq", None), P("dp", None)),
        check_vma=False,
    )
```

```python
import jax
import jax.numpy as jnp
from jax import lax
from jax.experimental import pallas as pl
from jax.experimental.pallas import tpu as pltpu
from jax.sharding import PartitionSpec as P

H = 8
DH = 128


EPS = 1e-05


def layer_norm(values, gain):
    average = jnp.mean(values, axis=-1, keepdims=True)
    centred = values - average
    variance = jnp.mean(centred * centred, axis=-1, keepdims=True)
    return centred * lax.rsqrt(variance + EPS) * gain


def silu_slope(values):
    sigmoid_v = jax.nn.sigmoid(values)
    return sigmoid_v * (1.0 + values * (1.0 - sigmoid_v))


def time_bias(bias_table, stamps_q, stamps_k):
    elapsed = stamps_q[:, None] - stamps_k[None, :]
    bucket = jnp.zeros(elapsed.shape, jnp.int32)
    for degree in range(1, bias_table.shape[1]):
        bucket = bucket + (elapsed >= 2**degree - 1).astype(jnp.int32)
    levels = jnp.arange(bias_table.shape[1], dtype=jnp.int32)
    one_hot = (bucket[:, :, None] == levels[None, None, :]).astype(jnp.float32)
    return jnp.einsum(
        "qkb,hb->hqk",
        one_hot,
        bias_table,
        precision=lax.Precision.HIGHEST,
        preferred_element_type=jnp.float32,
    )


def pair_terms(
    q_heads, d_heads, stamps_q, pos_q, k_heads, v_heads, stamps_k, pos_k, length, bias_table, scale
):
    scores = (
        jnp.einsum("qhd,khd->hqk", q_heads, k_heads, preferred_element_type=jnp.float32) * scale
    )
    scores = scores + time_bias(bias_table, stamps_q, stamps_k)
    allowed = (
        (pos_k[None, :] <= pos_q[:, None]) & (pos_k[None, :] < length) & (pos_q[:, None] < length)
    )
    weight = jnp.where(allowed[None], jax.nn.silu(scores), 0.0).astype(jnp.bfloat16)
    if d_heads is None:
        return (weight, None)
    d_weight = jnp.einsum("qhd,khd->hqk", d_heads, v_heads, preferred_element_type=jnp.float32)
    d_scores = jnp.where(allowed[None], d_weight * silu_slope(scores), 0.0).astype(jnp.bfloat16)
    return (weight, d_scores)


def per_device(tokens, cotangent, stamps, lengths, w_qkvu, w_out, gain_in, gain_out, bias_table):
    rows = tokens[0]
    cot_rows = cotangent[0]
    tok_count = rows.shape[0]
    feature_width = rows.shape[1]
    seq_count = lax.axis_size("seq")
    total_rows = tok_count * seq_count
    first_row = lax.axis_index("seq") * tok_count
    length = lengths[0]
    stamp_all = stamps[0]
    pos_own = first_row + jnp.arange(tok_count, dtype=jnp.int32)
    stamp_own = lax.dynamic_slice_in_dim(stamp_all, first_row, tok_count)
    scale = DH ** (-0.5)
    block_rows = min(512, total_rows)
    block_count = total_rows // block_rows
    w_full, w_out_full = (
        lax.all_gather(w_qkvu, "dp", axis=0, tiled=True),
        lax.all_gather(w_out, "dp", axis=0, tiled=True),
    )
    wide_rows = rows.astype(jnp.float32)
    normed = layer_norm(wide_rows, gain_in).astype(jnp.bfloat16)
    projected = jnp.dot(normed, w_full, preferred_element_type=jnp.float32)
    activated = jax.nn.silu(projected)
    gate_u = activated[:, :feature_width]
    values_own = activated[:, feature_width : 2 * feature_width].astype(jnp.bfloat16)
    queries_own = activated[:, 2 * feature_width : 3 * feature_width].astype(jnp.bfloat16)
    keys_own = activated[:, 3 * feature_width :].astype(jnp.bfloat16)
    keys_all, values_all = (
        lax.all_gather(keys_own, "seq", axis=0, tiled=True),
        lax.all_gather(values_own, "seq", axis=0, tiled=True),
    )
    q_heads = queries_own.reshape(tok_count, H, DH)

    def key_block(start):
        k_heads = lax.dynamic_slice_in_dim(keys_all, start, block_rows).reshape(block_rows, H, DH)
        v_heads = lax.dynamic_slice_in_dim(values_all, start, block_rows).reshape(block_rows, H, DH)
        stamps_k = lax.dynamic_slice_in_dim(stamp_all, start, block_rows)
        pos_k = start + jnp.arange(block_rows, dtype=jnp.int32)
        return (k_heads, v_heads, stamps_k, pos_k)

    def guarded(active, action, state):
        return lax.cond(active, action, lambda same: same, state)

    def reaches(start):
        return (start <= first_row + tok_count - 1) & (start < length) & (first_row < length)

    def forward_step(block_idx, totals):
        start = block_idx * block_rows

        def forward_compute(totals):
            k_heads, v_heads, stamps_k, pos_k = key_block(start)
            weight, unused = pair_terms(
                q_heads,
                None,
                stamp_own,
                pos_own,
                k_heads,
                v_heads,
                stamps_k,
                pos_k,
                length,
                bias_table,
                scale,
            )
            return totals + jnp.einsum(
                "hqk,khd->qhd", weight, v_heads, preferred_element_type=jnp.float32
            )

        return guarded(reaches(start), forward_compute, totals)

    attended = lax.fori_loop(
        0, block_count, forward_step, jnp.zeros((tok_count, H, DH), jnp.float32)
    )
    attended = attended.reshape(tok_count, feature_width)
    normed_att, norm_back = jax.vjp(lambda values: layer_norm(values, gain_out), attended)
    mixed_rows = (normed_att * gate_u).astype(jnp.bfloat16)
    mixed = (
        wide_rows + jnp.dot(mixed_rows, w_out_full, preferred_element_type=jnp.float32)
    ).astype(jnp.bfloat16)
    grad_part = lax.psum_scatter(
        jnp.einsum("tr,tc->rc", mixed_rows, cot_rows, preferred_element_type=jnp.float32).astype(
            jnp.bfloat16
        ),
        "dp",
        scatter_dimension=0,
        tiled=True,
    )
    w_grad = lax.psum(grad_part, "seq").astype(jnp.float32)
    d_mix = jnp.einsum("tc,rc->tr", cot_rows, w_out_full, preferred_element_type=jnp.float32)
    d_gate = d_mix * normed_att
    d_att = norm_back(d_mix * gate_u)[0].astype(jnp.bfloat16)
    d_heads = d_att.reshape(tok_count, H, DH)

    def backward_step():

        def step(block_idx, state_pair):
            start = block_idx * block_rows

            def step_compute(state_pair):
                q_grad, key_terms = state_pair
                k_heads, v_heads, stamps_k, pos_k = key_block(start)
                weight, d_scores = pair_terms(
                    q_heads,
                    d_heads,
                    stamp_own,
                    pos_own,
                    k_heads,
                    v_heads,
                    stamps_k,
                    pos_k,
                    length,
                    bias_table,
                    scale,
                )
                q_grad = (
                    q_grad
                    + jnp.einsum(
                        "hqk,khd->qhd", d_scores, k_heads, preferred_element_type=jnp.float32
                    )
                    * scale
                )
                k_grad = (
                    jnp.einsum(
                        "hqk,qhd->khd", d_scores, q_heads, preferred_element_type=jnp.float32
                    )
                    * scale
                )
                v_grad = jnp.einsum(
                    "hqk,qhd->khd", weight, d_heads, preferred_element_type=jnp.float32
                )
                joined = jnp.concatenate(
                    [
                        k_grad.reshape(block_rows, feature_width),
                        v_grad.reshape(block_rows, feature_width),
                    ],
                    axis=1,
                )
                key_terms = lax.dynamic_update_slice_in_dim(key_terms, joined, start, 0)
                return (q_grad, key_terms)

            return guarded(reaches(start), step_compute, state_pair)

        return step

    q_start = jnp.zeros((tok_count, H, DH), jnp.float32)
    term_start = jnp.zeros((total_rows, 2 * feature_width), jnp.float32)
    q_grad, key_terms = lax.fori_loop(0, block_count, backward_step(), (q_start, term_start))
    key_grads = lax.psum_scatter(
        key_terms.astype(jnp.bfloat16), "seq", scatter_dimension=0, tiled=True
    ).astype(jnp.float32)
    d_act = jnp.concatenate(
        [
            d_gate,
            key_grads[:, feature_width:],
            q_grad.reshape(tok_count, feature_width),
            key_grads[:, :feature_width],
        ],
        axis=1,
    )
    d_proj = (d_act * silu_slope(projected)).astype(jnp.bfloat16)
    d_normed = jnp.einsum("tf,df->td", d_proj, w_full, preferred_element_type=jnp.float32)
    unused_rows, in_back = jax.vjp(lambda values: layer_norm(values, gain_in), wide_rows)
    input_grad = (cot_rows.astype(jnp.float32) + in_back(d_normed)[0]).astype(jnp.bfloat16)
    return (mixed[None], input_grad[None], w_grad)


MESH = pl.DeviceIdType.MESH
VM = pl.BlockSpec(memory_space=pltpu.VMEM)
F32 = jnp.float32
BF16 = jnp.bfloat16
MASKED = -1e30
PIECES = 4


def mm(a, b, dims):
    return lax.dot_general(a, b, (dims, ((), ())), preferred_element_type=F32)


def remote(src, dst, send_sem, recv_sem, target):
    return pltpu.make_async_remote_copy(
        src_ref=src,
        dst_ref=dst,
        send_sem=send_sem,
        recv_sem=recv_sem,
        device_id=target,
        device_id_type=MESH,
    )


def arrived(dst, sem):
    pltpu.make_async_copy(dst, dst, sem).wait()


def sent(block, sem, target):
    remote(block, block, sem, sem, target).wait_send()


def column_kernel(
    n_dp, n_seq, w_hbm, x_hbm, c_hbm, wo_hbm, stamps_hbm, length_ref, gin_hbm, gout_hbm, bias_hbm,
    mixed_ref, grad_ref, wg_ref,
    w_ref, x_ref, c_ref, wo_ref, stamps_ref, gin_ref, gout_ref, bias_ref, meta_ref,
    W, X, C, WO, mbuf, NB, BI, PJ, GT, ACT, ATT, WT, SL, DM, DG, DA, DP, MR, MX, KA, VA, SA, SG, TB,
    MW, WG, PS, PR, TS, TR, MA, MB, PB, SB, CS, FB, FIN, RO,
    lsem, wout, wvia, wrest, zout, shareout, farout, xrecv, woout, worecv, msem,
    saout, sarecv, sgout, sgrecv, mxout, mxrecv, gout, grecv,
    hout, hmid, hback, trecv, pout, precv, cout, crecv, oout, orecv,
):
    me = lax.axis_index("dp")
    z = lax.axis_index("seq")
    tok, width = x_ref.shape
    rows = tok * n_seq
    half = tok // 2
    n_heads = n_dp
    scale = DH ** (-0.5)
    chip, k = me // 2, me % 2
    cy, cx = chip // 2, chip % 2
    xn, yn = 2 * cy + (1 - cx), 2 * (1 - cy) + cx
    dn = 2 * (1 - cy) + (1 - cx)
    sib = 2 * chip + (1 - k)
    p, ks = z % 2, z // 2
    near, far = 1 + ks, (n_seq - 1) * ks
    zp = near + far - z
    is_near, is_far = z == near, z == far
    is_main = k == ks
    is_aux = jnp.logical_not(is_main)
    main_dp = 2 * chip + ks

    def head_of(core, j):
        return 4 * core + 2 * j + p

    def rows_of(ref_rows, index):
        return pl.ds(pl.multiple_of(index * ref_rows, ref_rows), ref_rows)

    def lanes_of(index):
        return pl.ds(pl.multiple_of(index * DH, DH), DH)

    def w_copies(core, j, make):
        return [
            make(
                w_ref.at[:, lanes_of(g * n_heads + head_of(core, j))],
                W.at[j, rows_of(tok, me), slice(g * DH, (g + 1) * DH)],
            )
            for g in range(4)
        ]

    w_targets = (
        (xn, 0, wvia.at[k]), (yn, 1, wvia.at[k]), (chip, 1 - k, wrest), (xn, 1, wrest),
        (yn, 0, wrest),
    )

    def w_start(j):
        for where, core, sem in w_targets:
            for copy in w_copies(
                core, j, lambda s, d: remote(s, d, wout, sem.at[j], (2 * where + core, z))
            ):
                copy.start()

    def w_piece(src, j):
        return W.at[j, rows_of(tok, src)]

    via, to = (1 - k) * xn + k * yn, (1 - k) * yn + k * xn

    def w_relay(i, j):
        src = 2 * via + i
        block = w_piece(src, j)
        return remote(block, block, wout, wrest.at[j], (2 * to + k, z))

    ins, outs = (x_ref, c_ref), (X, C)
    z_to = jnp.where(is_main, zp, 1 + k)

    def z_send(a):
        return remote(ins[a], outs[a].at[z], zout, xrecv.at[a, z], (me, z_to))

    def own_copy(a):
        return pltpu.make_async_copy(ins[a], outs[a].at[z], xrecv.at[a, z])

    def share(a, b):
        block = ins[a] if b is None else outs[a].at[b]
        at = z if b is None else b
        return remote(block, outs[a].at[at], shareout, xrecv.at[a, at], (sib, z))

    foreign = (2 * (1 - ks), 2 * (1 - ks) + 1)

    def to_far(a, i):
        block = outs[a].at[foreign[i]]
        return remote(block, block, farout, xrecv.at[a, foreign[i]], (me, far))

    def x_wait(a, b):
        arrived(outs[a].at[b], xrecv.at[a, b])

    def meta_send():
        return remote(meta_ref, mbuf, msem.at[0], msem.at[1], (sib, z))

    wo_core, wo_slot = chip // 2, chip % 2
    wo_part = 2 * k + wo_core
    wo_here = wo_core == k
    wo_sem = jnp.where(k == p, wo_slot, 2)
    wo_sends = [
        remote(
            wo_ref, WO.at[wo_part, wo_slot], woout, worecv.at[wo_sem],
            (2 * where + wo_core, z),
        )
        for i, where in enumerate((xn, yn, dn, chip))
    ]

    def wo_start():
        for i in range(3):
            wo_sends[i].start()

        @pl.when(wo_here)
        def _():
            pltpu.make_async_copy(wo_ref, WO.at[wo_part, wo_slot], worecv.at[wo_sem]).start()

        @pl.when(jnp.logical_not(wo_here))
        def _():
            wo_sends[3].start()

    def wo_share(parity, j):
        block = WO.at[2 * parity + k, j]
        return remote(block, block, woout, worecv.at[3], (sib, z))

    loads = [
        pltpu.make_async_copy(src, dst, lsem.at[i])
        for src, dst, i in (
            (stamps_hbm, stamps_ref, 0), (w_hbm, w_ref, 1), (x_hbm, x_ref, 1), (c_hbm, c_ref, 1),
            (wo_hbm, wo_ref, 1), (gin_hbm, gin_ref, 2), (gout_hbm, gout_ref, 3),
            (bias_hbm, bias_ref, 4),
        )
    ]
    barrier = pltpu.get_barrier_semaphore()
    for step in range(1, n_dp):
        pl.semaphore_signal(
            barrier, inc=1, device_id=(lax.rem(me + step, n_dp), z), device_id_type=MESH
        )
    for step in range(1, n_seq):
        there = lax.rem(z + step, n_seq)

        @pl.when(jnp.abs(there - z) < n_seq - 1)
        def _():
            for peer in (me, sib):
                pl.semaphore_signal(
                    barrier, inc=1, device_id=(peer, there), device_id_type=MESH
                )

    for load in loads:
        load.start()
    loads[0].wait()
    meta_ref[0:1, :] = stamps_ref[...]
    meta_ref[1:2, :] = jnp.full(stamps_ref.shape, length_ref[0], jnp.int32)
    arrived(W.at[:, : (n_dp - 1) * tok], lsem.at[1])
    for load in loads[5:]:
        load.wait()
    inner = jnp.where((z > 0) & (z < n_seq - 1), 1, 0)
    pl.semaphore_wait(barrier, n_dp - 1 + 2 * (n_seq - 2) + 2 * inner)
    @pl.when(is_main)
    def _():
        pltpu.make_async_copy(meta_ref, mbuf, msem.at[1]).start()
        meta_send().start()

    w_start(0)
    z_send(0).start()

    @pl.when(is_main)
    def _():
        own_copy(0).start()
        share(0, None).start()

    z_send(1).start()

    @pl.when(is_main)
    def _():
        own_copy(1).start()
        share(1, None).start()

    for j in range(2):
        for copy in w_copies(k, j, lambda s, d: pltpu.make_async_copy(s, d, wrest.at[j])):
            copy.start()

    def relay_weights(j):
        for i in range(2):
            arrived(w_piece(2 * via + i, j), wvia.at[i, j])
            w_relay(i, j).start()

    def near_relay(a):
        @pl.when(is_main)
        def _():
            x_wait(a, zp)
            share(a, zp).start()

        @pl.when(is_main & is_near)
        def _():
            for i in range(2):
                x_wait(a, foreign[i])
                to_far(a, i).start()
                share(a, foreign[i]).start()

    def far_relay(a):
        @pl.when(is_main & is_far)
        def _():
            for i in range(2):
                x_wait(a, foreign[i])
                share(a, foreign[i]).start()

    relay_weights(0)
    w_start(1)
    near_relay(0)

    arrived(mbuf, msem.at[1])
    lane_row = lax.broadcasted_iota(jnp.int32, (DH, DH), 0)
    lane_col = lax.broadcasted_iota(jnp.int32, (DH, DH), 1)
    length = mbuf[1:2, :DH]
    for i in range(n_seq):
        col = jnp.broadcast_to(mbuf[0:1, i * DH : (i + 1) * DH].astype(F32), (DH, DH)).T
        valid = lane_row + i * DH < length
        for b in range(i + 1):
            elapsed = col - mbuf[0:1, b * DH : (b + 1) * DH].astype(F32)
            allowed = valid & (lane_col <= lane_row) if b == i else valid
            heads = [head_of(k, j) for j in range(2)]
            terms = [jnp.full(elapsed.shape, bias_ref[h, 0], F32) for h in heads]
            for degree in range(1, bias_ref.shape[1]):
                reached = elapsed >= float(2**degree - 1)
                terms = [
                    jnp.where(reached, bias_ref[h, degree], t) for h, t in zip(heads, terms)
                ]
            for j in range(2):
                BI[j, i * DH : (i + 1) * DH, b * DH : (b + 1) * DH] = jnp.where(
                    allowed, terms[j], MASKED
                )

    near_relay(1)
    relay_weights(1)

    far_relay(0)

    @pl.when(is_main)
    def _():
        x_wait(0, z)

    @pl.when(is_aux)
    def _():
        for b in range(n_seq):
            x_wait(0, b)

    for b in range(n_seq):
        NB[b * tok : (b + 1) * tok, :] = layer_norm(X[b].astype(F32), gin_ref[...]).astype(BF16)

    def forward(j):
        arrived(W.at[j, : (n_dp - 2) * tok], wrest.at[j])
        PJ[j] = mm(NB[...], W[j], ((1,), (0,)))
        cols = slice(j * DH, (j + 1) * DH)
        GT[:, cols] = jax.nn.silu(PJ[j, :, :DH])
        for g in range(3):
            ACT[j, g] = jax.nn.silu(PJ[j, :, (1 + g) * DH : (2 + g) * DH]).astype(BF16)
        for i in range(n_seq):
            at, end = slice(i * tok, (i + 1) * tok), (i + 1) * tok
            scores = mm(ACT[j, 1, at], ACT[j, 2, :end], ((1,), (1,))) * scale + BI[j, at, :end]
            sig = jax.nn.sigmoid(scores)
            weight = (scores * sig).astype(BF16)
            WT[j, at, :end] = weight
            SL[j, at, :end] = sig * (1.0 + scores * (1.0 - sig))
            ATT[at, cols] = mm(weight, ACT[j, 0, :end], ((1,), (0,)))

    @pl.when(k == p)
    def _():
        wo_start()

    forward(0)

    forward(1)

    gain = jnp.concatenate([gout_ref[:, lanes_of(head_of(k, j))] for j in range(2)], axis=1)
    pid = 2 * p + k
    own_width = 2 * DH
    st_peers = ((sib, z), (me, zp), (sib, zp))

    def stat_sends(ref, send_sem, recv_sem):
        return [
            remote(ref.at[pid], ref.at[pid], send_sem, recv_sem, peer)
            for peer in st_peers
        ]

    def put_stats(ref, b, first, second):
        pair = jnp.where(lane_col == 0, first, second).T
        ref[pid, b : b + 1, :] = pair[0:1]
        ref[pid, n_seq + b : n_seq + b + 1, :] = pair[1:2]

    for b in range(n_seq):
        at = slice(b * tok, (b + 1) * tok)
        att = ATT[at, :]
        mean_own = jnp.mean(att, axis=1, keepdims=True)
        off = att - mean_own
        put_stats(SA, b, mean_own, jnp.sum(off * off, axis=1, keepdims=True))
    for copy in stat_sends(SA, saout, sarecv):
        copy.start()
    far_relay(1)
    @pl.when(is_main)
    def _():
        x_wait(1, z)

    @pl.when(is_aux)
    def _():
        for b in range(n_seq):
            x_wait(1, b)

    c_rows = C[...].reshape(rows, width)
    for j in range(2):
        arrived(WO.at[pid, j], worecv.at[j])
        wo_share(p, j).start()
        DM[:, j * DH : (j + 1) * DH] = mm(c_rows, WO[pid, j], ((1,), (1,)))
    for b in range(n_seq):
        at = slice(b * tok, (b + 1) * tok)
        att = ATT[at, :]
        off = att - jnp.mean(att, axis=1, keepdims=True)
        g = DM[at, :] * GT[at, :] * gain
        put_stats(
            SG, b, jnp.sum(g, axis=1, keepdims=True), jnp.sum(g * off, axis=1, keepdims=True)
        )
    for copy in stat_sends(SG, sgout, sgrecv):
        copy.start()

    arrived(SA.at[:3], sarecv)
    first, second = slice(0, n_seq), slice(n_seq, 2 * n_seq)
    means = [SA[q, first, :] for q in range(4)]
    mean = sum(means[1:], means[0]) / 4.0
    shifts = [m - mean for m in means]
    squares = sum(SA[q, second, :] + own_width * shifts[q] * shifts[q] for q in range(4))
    rstd = lax.rsqrt(squares / width + EPS)
    TB[0], TB[1] = mean, rstd

    def turned(i, b):
        wide_row = jnp.broadcast_to(TB[i, b : b + 1, :], (DH, DH)).T
        return jnp.concatenate([wide_row] * 2, axis=1)

    blocks = tuple(reversed(range(n_seq)))

    def mine(b):
        return is_near == (far != b)

    def other(b):
        return is_near == (far == b)

    def home_is_self(b):
        return is_main & (z == b)

    def mx_send(b):
        return remote(
            MR.at[b * tok : (b + 1) * tok], MX.at[pid], mxout, mxrecv, (main_dp, b)
        )

    for b in blocks:
        at = slice(b * tok, (b + 1) * tok)
        hat = (ATT[at, :] - turned(0, b)) * turned(1, b)
        ATT[at, :] = hat
        MR[at, :] = (hat * gain * GT[at, :]).astype(BF16)

    pieces = PIECES
    piece = DH // pieces

    def out_rows(i):
        return slice(i * piece, (i + 1) * piece)

    def g_send(j, i):
        return remote(
            MW.at[j, i], WG.at[chip, i], gout, grecv.at[i],
            (2 * (2 * k + j) + p, z),
        )

    def g_self(j):
        return (2 * k + j == chip) & (k == p)

    for j in range(2):
        part = mm(MR[:, j * DH : (j + 1) * DH], c_rows, ((0,), (0,)))
        for i in range(pieces):
            MW[j, i] = part[out_rows(i)].astype(BF16)
    for i in range(pieces):
        for j in range(2):

            @pl.when(g_self(j))
            def _():
                pltpu.make_async_copy(MW.at[j, i], WG.at[chip, i], grecv.at[i]).start()

            @pl.when(jnp.logical_not(g_self(j)))
            def _():
                g_send(j, i).start()

    is_root = k == p
    far_root, near_root, middle, edge = (n_seq - 1) * k, 2 - k, 1 + k, (n_seq - 1) * (1 - k)
    def h_send(dst, recv, i):
        return remote(PS.at[i], dst.at[i], hout, recv.at[i], (me, middle))

    def h_relay(src, i, to):
        return remote(src.at[i], PR.at[i], hout, hback.at[i], (me, to))

    def t_send(i):
        return remote(TS.at[i], TR.at[i], hout, trecv.at[i], (me, edge))

    def plane_sum(i):
        @pl.when(is_root)
        def _():
            arrived(WG.at[:, i], grecv.at[i])
            total = WG[0, i].astype(F32)
            for c in range(1, n_dp // 2):
                total = total + WG[c, i].astype(F32)
            PS[i] = total.astype(BF16)

            @pl.when(z == far_root)
            def _():
                h_send(MA, hmid.at[0], i).start()

            @pl.when(z == near_root)
            def _():
                h_send(MB, hmid.at[1], i).start()

    def pass_in():
        @pl.when(z == middle)
        def _():
            for i in range(pieces):
                arrived(MB.at[i], hmid.at[1, i])
                h_relay(MB, i, far_root).start()

    def pass_out():
        @pl.when(z == middle)
        def _():
            for i in range(pieces):
                arrived(MA.at[i], hmid.at[0, i])
                h_relay(MA, i, near_root).start()
                wg_ref[out_rows(i)] = (MA[i].astype(F32) + MB[i].astype(F32)).astype(BF16)

    def root_total(i):
        arrived(PR.at[i], hback.at[i])
        TS[i] = (PS[i].astype(F32) + PR[i].astype(F32)).astype(BF16)
        wg_ref[out_rows(i)] = TS[i]

    def near_total():
        @pl.when(z == near_root)
        def _():
            for i in range(pieces):
                root_total(i)
                t_send(i).start()

    def outer_total():
        @pl.when(z == far_root)
        def _():
            for i in range(pieces):
                root_total(i)

        @pl.when(z == edge)
        def _():
            for i in range(pieces):
                arrived(TR.at[i], trecv.at[i])
                wg_ref[out_rows(i)] = TR[i]

    def pair_send(b):
        return remote(PB.at[b, 1 - k], SB.at[b], pout, precv.at[b], (sib, z))

    def cross_send(b):
        return remote(CS.at[b], FB.at[b], cout, crecv.at[b], (me, zp))

    def home_send(b):
        return remote(FIN.at[b], RO.at[k], oout, orecv, (main_dp, b))

    def pair_sum(b):
        return PB[b, k].astype(F32) + SB[b].astype(F32)

    def cross(b):
        arrived(SB.at[b], precv.at[b])

        @pl.when(other(b))
        def _():
            CS[b] = pair_sum(b).astype(BF16)
            cross_send(b).start()

    def finish(b):
        @pl.when(mine(b))
        def _():
            arrived(FB.at[b], crecv.at[b])
            FIN[b] = (pair_sum(b) + FB[b].astype(F32)).astype(BF16)

            @pl.when(home_is_self(b))
            def _():
                pltpu.make_async_copy(FIN.at[b], RO.at[k], orecv).start()

            @pl.when(jnp.logical_not(home_is_self(b)))
            def _():
                home_send(b).start()

    arrived(SG.at[:3], sgrecv)
    for b in blocks:

        @pl.when(home_is_self(b))
        def _():
            pltpu.make_async_copy(
                MR.at[b * tok : (b + 1) * tok], MX.at[pid], mxrecv
            ).start()

        @pl.when(jnp.logical_not(home_is_self(b)))
        def _():
            mx_send(b).start()

    g_mean = sum(SG[q, first, :] for q in range(4)) / width
    g_dot = rstd * sum(SG[q, second, :] + shifts[q] * SG[q, first, :] for q in range(4)) / width
    TB[1], TB[2], TB[3] = rstd, g_mean, g_dot
    for b in range(n_seq):
        at = slice(b * tok, (b + 1) * tok)
        d_mix, hat = DM[at, :], ATT[at, :]
        DG[at, :] = d_mix * (hat * gain)
        g = d_mix * GT[at, :] * gain
        DA[at, :] = (
            turned(1, b) * (g - turned(2, b) - hat * turned(3, b))
        ).astype(BF16)

    def backward(j, b):
        cols = slice(j * DH, (j + 1) * DH)
        start, end = b * tok, (b + 1) * tok

        def put(group, grad):
            at = slice(group * DH, (group + 1) * DH)
            DP[j, start:end, at] = (grad * silu_slope(PJ[j, start:end, at])).astype(BF16)

        d_att = DA[start:end, cols]
        d_weight = mm(d_att, ACT[j, 0, :end], ((1,), (1,)))
        d_scores = (d_weight * SL[j, start:end, :end]).astype(BF16)
        put(2, mm(d_scores, ACT[j, 2, :end], ((1,), (0,))) * scale)
        k_part = mm(d_scores, ACT[j, 1, start:end], ((0,), (0,)))
        v_part = mm(WT[j, start:end, :end], d_att, ((0,), (0,)))
        if end == rows:
            KA[j] = k_part
            VA[j] = v_part
        else:
            KA[j, :end] += k_part
            VA[j, :end] += v_part
        put(0, DG[start:end, cols])
        put(1, VA[j, start:end])
        put(3, KA[j, start:end] * scale)

    def d_part(b):
        at = slice(b * tok, (b + 1) * tok)
        part = mm(DP[0, at], W[0], ((1,), (1,))) + mm(DP[1, at], W[1], ((1,), (1,)))
        PB[b, 0] = part[:half].astype(BF16)
        PB[b, 1] = part[half:].astype(BF16)
        pair_send(b).start()

    last = n_seq - 1
    for b in blocks:
        for j in range(2):
            backward(j, b)
        if b == last - 1:

            @pl.when(ks == 0)
            def _():
                cross(last)

        elif b == 1:

            @pl.when(ks == 0)
            def _():
                cross(2)

        if b == last:

            @pl.when(ks == 0)
            def _():
                d_part(last)

        else:
            d_part(b)
        if b < 2:
            for i in range(pieces // 2):
                plane_sum((1 - b) * pieces // 2 + i)
    cross(1)
    cross(0)

    @pl.when(k != p)
    def _():
        wo_start()

    @pl.when(ks != 0)
    def _():
        cross(2)
        d_part(last)
        cross(last)

    finish(3)
    pass_in()
    @pl.when(ks == 0)
    def _():
        finish(2)

    pass_out()
    finish(1)
    finish(0)

    @pl.when(ks != 0)
    def _():
        finish(2)

    near_total()
    arrived(WO.at[2 * (1 - p) + k], worecv.at[2])
    for j in range(2):
        wo_share(1 - p, j).start()

    arrived(X, worecv.at[3])
    arrived(MX, mxrecv)
    wide = x_ref[...].astype(F32)
    total = wide
    for q in range(4):
        total = total + mm(MX[q], WO[q].reshape(2 * DH, width), ((1,), (0,)))
    mixed_ref[...] = total.astype(BF16)

    average = jnp.mean(wide, axis=-1, keepdims=True)
    centred = wide - average
    inv = lax.rsqrt(jnp.mean(centred * centred, axis=-1, keepdims=True) + EPS)
    hat = centred * inv
    outer_total()
    arrived(RO, orecv)
    grad = RO[...].reshape(tok, width).astype(F32) * gin_ref[...]
    back = inv * (
        grad
        - jnp.mean(grad, axis=-1, keepdims=True)
        - hat * jnp.mean(grad * hat, axis=-1, keepdims=True)
    )
    grad_ref[...] = (c_ref[...].astype(F32) + back).astype(BF16)

    beside = (sib, z)

    def sent_when(condition, block, sem):
        @pl.when(condition)
        def _():
            sent(block, sem, beside)

    part = (n_dp - 1) * tok
    sent(W.at[:, :part], wout, beside)
    sent(X.at[:2], zout, beside)
    sent_when(is_main, W, shareout)
    sent_when(is_main & is_near, X, farout)
    sent_when(is_main, meta_ref, msem.at[0])
    sent_when(wo_here, W.at[:, :part], woout)
    sent_when(jnp.logical_not(wo_here), W, woout)
    sent(SA.at[:3], saout, beside)
    sent(SG.at[:3], sgout, beside)
    sent_when(is_main, MX.at[:3], mxout)
    sent_when(is_aux, MX, mxout)
    keeps_one = is_root & wo_here
    sent_when(keeps_one, X.at[0], gout)
    sent_when(jnp.logical_not(keeps_one), X.at[:2], gout)
    sent_when(z == far_root, PS, hout)
    sent_when((z == near_root) | (z == middle), X.at[:2], hout)
    sent(X.at[:2], pout, beside)
    sent_when(is_far, CS.at[:3], cout)
    sent_when(is_near, CS.at[:1], cout)
    sent_when(is_near & is_main, FIN.at[:2], oout)
    sent_when(is_near & is_aux, FIN.at[:3], oout)
    sent_when(is_far & is_aux, FIN.at[:1], oout)


def tail_kernel(mixed_ref, grad_ref, wg_ref, mixed_out, grad_out, wg_out, wide, sems):
    copies = [
        pltpu.make_async_copy(src, dst, sems.at[i])
        for i, (src, dst) in enumerate(
            ((mixed_ref, mixed_out), (grad_ref, grad_out), (wide, wg_out))
        )
    ]
    copies[0].start()
    copies[1].start()
    wide[...] = wg_ref[...].astype(F32)
    copies[2].start()
    for copy in copies:
        copy.wait()


def column_parallel(
    n_dp, n_seq, tokens, cotangent, stamps, lengths, w_qkvu, w_out, gain_in, gain_out, bias_table
):
    tok, width = tokens.shape[1:]
    rows = tok * n_seq
    dma = pltpu.SemaphoreType.DMA
    sds = jax.ShapeDtypeStruct
    hbm = pl.BlockSpec(memory_space=pltpu.HBM)

    def vb(*shape):
        return pltpu.VMEM(shape, BF16)

    def vf(*shape):
        return pltpu.VMEM(shape, F32)

    def in_hbm(value):
        return pltpu.with_memory_space_constraint(value, pltpu.HBM)

    half = tok // 2
    mixed, grad, w_grad = pl.pallas_call(
        lambda *refs: column_kernel(n_dp, n_seq, *refs),
        out_shape=(sds((tok, width), BF16), sds((tok, width), BF16), sds(w_out.shape, BF16)),
        in_specs=[hbm] * 5 + [pl.BlockSpec(memory_space=pltpu.SMEM)] + [hbm] * 3,
        out_specs=[VM] * 3,
        scratch_shapes=[
            pltpu.VMEM(w_qkvu.shape, BF16),
            vb(tok, width),
            vb(tok, width),
            vb(DH, width),
            pltpu.VMEM(stamps.shape, jnp.int32),
            vf(1, width),
            vf(1, width),
            pltpu.SMEM(bias_table.shape, F32),
            pltpu.VMEM((8, rows), jnp.int32),
            vb(2, width, 4 * DH),
            vb(n_seq, tok, width),
            vb(n_seq, tok, width),
            vb(4, 2, DH, width),
            pltpu.VMEM((8, rows), jnp.int32),
            vb(rows, width),
            vf(2, rows, rows),
            vf(2, rows, 4 * DH),
            vf(rows, 2 * DH),
            vb(2, 3, rows, DH),
            vf(rows, 2 * DH),
            vb(2, rows, rows),
            vf(2, rows, rows),
            vf(rows, 2 * DH),
            vf(rows, 2 * DH),
            vb(rows, 2 * DH),
            vb(2, rows, 4 * DH),
            vb(rows, 2 * DH),
            vb(4, tok, 2 * DH),
            vf(2, rows, DH),
            vf(2, rows, DH),
            vf(4, 8, DH),
            vf(4, 8, DH),
            vf(4, n_seq, DH),
            vb(2, PIECES, DH // PIECES, width),
            vb(n_dp // 2, PIECES, DH // PIECES, width),
            vb(PIECES, DH // PIECES, width),
            vb(PIECES, DH // PIECES, width),
            vb(PIECES, DH // PIECES, width),
            vb(PIECES, DH // PIECES, width),
            vb(PIECES, DH // PIECES, width),
            vb(PIECES, DH // PIECES, width),
            vb(n_seq, 2, half, width),
            vb(n_seq, half, width),
            vb(n_seq, half, width),
            vb(n_seq, half, width),
            vb(n_seq, half, width),
            vb(2, half, width),
            dma((5,)),
            dma,
            dma((2, 2)),
            dma((2,)),
            dma,
            dma,
            dma,
            dma((2, n_seq)),
            dma,
            dma((4,)),
            dma((2,)),
            dma,
            dma,
            dma,
            dma,
            dma,
            dma,
            dma,
            dma((PIECES,)),
            dma,
            dma((2, PIECES)),
            dma((PIECES,)),
            dma((PIECES,)),
            dma,
            dma((n_seq,)),
            dma,
            dma((n_seq,)),
            dma,
            dma,
        ],
        compiler_params=pltpu.CompilerParams(
            has_side_effects=True, collective_id=0, vmem_limit_bytes=44 * 2**20
        ),
        name="column",
    )(
        *[in_hbm(v) for v in (w_qkvu, tokens[0], cotangent[0], w_out, stamps)],
        lengths,
        *[in_hbm(v) for v in (gain_in[None], gain_out[None], bias_table)],
    )
    mixed, grad, w_grad = pl.pallas_call(
        tail_kernel,
        out_shape=(sds(mixed.shape, BF16), sds(grad.shape, BF16), sds(w_grad.shape, F32)),
        in_specs=[VM] * 3,
        out_specs=[hbm] * 3,
        scratch_shapes=[vf(*w_grad.shape), dma((3,))],
        compiler_params=pltpu.CompilerParams(vmem_limit_bytes=8 * 2**20),
        name="tail",
    )(mixed, grad, w_grad)
    return (mixed[None], grad[None], w_grad)


def solution(mesh):
    n_dp, n_seq = mesh.shape["dp"], mesh.shape["seq"]

    def body(*args):
        tokens, stamps, w_out = args[0], args[2], args[5]
        mesh_fits = n_seq == 4 and n_dp == 2 * n_seq and n_dp == H
        sizes_fit = w_out.shape[0] == DH and tokens.shape[1] == DH
        if mesh_fits and sizes_fit and stamps.shape == (1, n_seq * DH):
            return column_parallel(n_dp, n_seq, *args)
        return per_device(*args)

    return jax.shard_map(
        body,
        mesh=mesh,
        in_specs=(
            P("dp", "seq", None),
            P("dp", "seq", None),
            P("dp", None),
            P("dp"),
            P("dp", None),
            P("dp", None),
            P(),
            P(),
            P(),
        ),
        out_specs=(P("dp", "seq", None), P("dp", "seq", None), P("dp", None)),
        check_vma=False,
    )
```

```python
import jax
import jax.numpy as jnp
from jax import lax
from jax.experimental import pallas as pl
from jax.experimental.pallas import tpu as pltpu
from jax.sharding import PartitionSpec as P

H = 8
DH = 128


EPS = 1e-05


def layer_norm(values, gain):
    average = jnp.mean(values, axis=-1, keepdims=True)
    centred = values - average
    variance = jnp.mean(centred * centred, axis=-1, keepdims=True)
    return centred * lax.rsqrt(variance + EPS) * gain


def silu_slope(values):
    sigmoid_v = jax.nn.sigmoid(values)
    return sigmoid_v * (1.0 + values * (1.0 - sigmoid_v))


def time_bias(bias_table, stamps_q, stamps_k):
    elapsed = stamps_q[:, None] - stamps_k[None, :]
    bucket = jnp.zeros(elapsed.shape, jnp.int32)
    for degree in range(1, bias_table.shape[1]):
        bucket = bucket + (elapsed >= 2**degree - 1).astype(jnp.int32)
    levels = jnp.arange(bias_table.shape[1], dtype=jnp.int32)
    one_hot = (bucket[:, :, None] == levels[None, None, :]).astype(jnp.float32)
    return jnp.einsum(
        "qkb,hb->hqk",
        one_hot,
        bias_table,
        precision=lax.Precision.HIGHEST,
        preferred_element_type=jnp.float32,
    )


def pair_terms(
    q_heads, d_heads, stamps_q, pos_q, k_heads, v_heads, stamps_k, pos_k, length, bias_table, scale
):
    scores = (
        jnp.einsum("qhd,khd->hqk", q_heads, k_heads, preferred_element_type=jnp.float32) * scale
    )
    scores = scores + time_bias(bias_table, stamps_q, stamps_k)
    allowed = (
        (pos_k[None, :] <= pos_q[:, None]) & (pos_k[None, :] < length) & (pos_q[:, None] < length)
    )
    weight = jnp.where(allowed[None], jax.nn.silu(scores), 0.0).astype(jnp.bfloat16)
    if d_heads is None:
        return (weight, None)
    d_weight = jnp.einsum("qhd,khd->hqk", d_heads, v_heads, preferred_element_type=jnp.float32)
    d_scores = jnp.where(allowed[None], d_weight * silu_slope(scores), 0.0).astype(jnp.bfloat16)
    return (weight, d_scores)


def per_device(tokens, cotangent, stamps, lengths, w_qkvu, w_out, gain_in, gain_out, bias_table):
    rows = tokens[0]
    cot_rows = cotangent[0]
    tok_count = rows.shape[0]
    feature_width = rows.shape[1]
    seq_count = lax.axis_size("seq")
    total_rows = tok_count * seq_count
    first_row = lax.axis_index("seq") * tok_count
    length = lengths[0]
    stamp_all = stamps[0]
    pos_own = first_row + jnp.arange(tok_count, dtype=jnp.int32)
    stamp_own = lax.dynamic_slice_in_dim(stamp_all, first_row, tok_count)
    scale = DH ** (-0.5)
    block_rows = min(512, total_rows)
    block_count = total_rows // block_rows
    w_full, w_out_full = (
        lax.all_gather(w_qkvu, "dp", axis=0, tiled=True),
        lax.all_gather(w_out, "dp", axis=0, tiled=True),
    )
    wide_rows = rows.astype(jnp.float32)
    normed = layer_norm(wide_rows, gain_in).astype(jnp.bfloat16)
    projected = jnp.dot(normed, w_full, preferred_element_type=jnp.float32)
    activated = jax.nn.silu(projected)
    gate_u = activated[:, :feature_width]
    values_own = activated[:, feature_width : 2 * feature_width].astype(jnp.bfloat16)
    queries_own = activated[:, 2 * feature_width : 3 * feature_width].astype(jnp.bfloat16)
    keys_own = activated[:, 3 * feature_width :].astype(jnp.bfloat16)
    keys_all, values_all = (
        lax.all_gather(keys_own, "seq", axis=0, tiled=True),
        lax.all_gather(values_own, "seq", axis=0, tiled=True),
    )
    q_heads = queries_own.reshape(tok_count, H, DH)

    def key_block(start):
        k_heads = lax.dynamic_slice_in_dim(keys_all, start, block_rows).reshape(block_rows, H, DH)
        v_heads = lax.dynamic_slice_in_dim(values_all, start, block_rows).reshape(block_rows, H, DH)
        stamps_k = lax.dynamic_slice_in_dim(stamp_all, start, block_rows)
        pos_k = start + jnp.arange(block_rows, dtype=jnp.int32)
        return (k_heads, v_heads, stamps_k, pos_k)

    def guarded(active, action, state):
        return lax.cond(active, action, lambda same: same, state)

    def reaches(start):
        return (start <= first_row + tok_count - 1) & (start < length) & (first_row < length)

    def forward_step(block_idx, totals):
        start = block_idx * block_rows

        def forward_compute(totals):
            k_heads, v_heads, stamps_k, pos_k = key_block(start)
            weight, unused = pair_terms(
                q_heads,
                None,
                stamp_own,
                pos_own,
                k_heads,
                v_heads,
                stamps_k,
                pos_k,
                length,
                bias_table,
                scale,
            )
            return totals + jnp.einsum(
                "hqk,khd->qhd", weight, v_heads, preferred_element_type=jnp.float32
            )

        return guarded(reaches(start), forward_compute, totals)

    attended = lax.fori_loop(
        0, block_count, forward_step, jnp.zeros((tok_count, H, DH), jnp.float32)
    )
    attended = attended.reshape(tok_count, feature_width)
    normed_att, norm_back = jax.vjp(lambda values: layer_norm(values, gain_out), attended)
    mixed_rows = (normed_att * gate_u).astype(jnp.bfloat16)
    mixed = (
        wide_rows + jnp.dot(mixed_rows, w_out_full, preferred_element_type=jnp.float32)
    ).astype(jnp.bfloat16)
    grad_part = lax.psum_scatter(
        jnp.einsum("tr,tc->rc", mixed_rows, cot_rows, preferred_element_type=jnp.float32).astype(
            jnp.bfloat16
        ),
        "dp",
        scatter_dimension=0,
        tiled=True,
    )
    w_grad = lax.psum(grad_part, "seq").astype(jnp.float32)
    d_mix = jnp.einsum("tc,rc->tr", cot_rows, w_out_full, preferred_element_type=jnp.float32)
    d_gate = d_mix * normed_att
    d_att = norm_back(d_mix * gate_u)[0].astype(jnp.bfloat16)
    d_heads = d_att.reshape(tok_count, H, DH)

    def backward_step():

        def step(block_idx, state_pair):
            start = block_idx * block_rows

            def step_compute(state_pair):
                q_grad, key_terms = state_pair
                k_heads, v_heads, stamps_k, pos_k = key_block(start)
                weight, d_scores = pair_terms(
                    q_heads,
                    d_heads,
                    stamp_own,
                    pos_own,
                    k_heads,
                    v_heads,
                    stamps_k,
                    pos_k,
                    length,
                    bias_table,
                    scale,
                )
                q_grad = (
                    q_grad
                    + jnp.einsum(
                        "hqk,khd->qhd", d_scores, k_heads, preferred_element_type=jnp.float32
                    )
                    * scale
                )
                k_grad = (
                    jnp.einsum(
                        "hqk,qhd->khd", d_scores, q_heads, preferred_element_type=jnp.float32
                    )
                    * scale
                )
                v_grad = jnp.einsum(
                    "hqk,qhd->khd", weight, d_heads, preferred_element_type=jnp.float32
                )
                joined = jnp.concatenate(
                    [
                        k_grad.reshape(block_rows, feature_width),
                        v_grad.reshape(block_rows, feature_width),
                    ],
                    axis=1,
                )
                key_terms = lax.dynamic_update_slice_in_dim(key_terms, joined, start, 0)
                return (q_grad, key_terms)

            return guarded(reaches(start), step_compute, state_pair)

        return step

    q_start = jnp.zeros((tok_count, H, DH), jnp.float32)
    term_start = jnp.zeros((total_rows, 2 * feature_width), jnp.float32)
    q_grad, key_terms = lax.fori_loop(0, block_count, backward_step(), (q_start, term_start))
    key_grads = lax.psum_scatter(
        key_terms.astype(jnp.bfloat16), "seq", scatter_dimension=0, tiled=True
    ).astype(jnp.float32)
    d_act = jnp.concatenate(
        [
            d_gate,
            key_grads[:, feature_width:],
            q_grad.reshape(tok_count, feature_width),
            key_grads[:, :feature_width],
        ],
        axis=1,
    )
    d_proj = (d_act * silu_slope(projected)).astype(jnp.bfloat16)
    d_normed = jnp.einsum("tf,df->td", d_proj, w_full, preferred_element_type=jnp.float32)
    unused_rows, in_back = jax.vjp(lambda values: layer_norm(values, gain_in), wide_rows)
    input_grad = (cot_rows.astype(jnp.float32) + in_back(d_normed)[0]).astype(jnp.bfloat16)
    return (mixed[None], input_grad[None], w_grad)


MESH = pl.DeviceIdType.MESH
VM = pl.BlockSpec(memory_space=pltpu.VMEM)
F32 = jnp.float32
BF16 = jnp.bfloat16
MASKED = -1e30
PIECES = 4


def mm(a, b, dims):
    return lax.dot_general(a, b, (dims, ((), ())), preferred_element_type=F32)


def remote(src, dst, send_sem, recv_sem, target):
    return pltpu.make_async_remote_copy(
        src_ref=src,
        dst_ref=dst,
        send_sem=send_sem,
        recv_sem=recv_sem,
        device_id=target,
        device_id_type=MESH,
    )


def arrived(dst, sem):
    pltpu.make_async_copy(dst, dst, sem).wait()


def sent(block, sem, target):
    remote(block, block, sem, sem, target).wait_send()


def column_kernel(
    n_dp, n_seq, w_hbm, x_hbm, c_hbm, wo_hbm, stamps_hbm, length_ref, gin_hbm, gout_hbm, bias_hbm,
    mixed_ref, grad_ref, wg_ref,
    w_ref, x_ref, c_ref, wo_ref, stamps_ref, gin_ref, gout_ref, bias_ref, meta_ref,
    W, X, C, WO, mbuf, NB, BI, PJ, GT, ACT, ATT, WT, SL, DM, DG, DA, DP, MR, MX, KA, VA, SA, SG, TB,
    MW, WG, PS, PR, TS, TR, MA, MB, PB, SB, CS, FB, FIN, RO,
    lsem, wout, wvia, wrest, zout, shareout, farout, xrecv, woout, worecv, msem,
    saout, sarecv, sgout, sgrecv, mxout, mxrecv, gout, grecv,
    hout, hmid, hback, trecv, pout, precv, cout, crecv, oout, orecv,
):
    me = lax.axis_index("dp")
    z = lax.axis_index("seq")
    tok, width = x_ref.shape
    rows = tok * n_seq
    half = tok // 2
    n_heads = n_dp
    scale = DH ** (-0.5)
    chip, k = me // 2, me % 2
    cy, cx = chip // 2, chip % 2
    xn, yn = 2 * cy + (1 - cx), 2 * (1 - cy) + cx
    dn = 2 * (1 - cy) + (1 - cx)
    sib = 2 * chip + (1 - k)
    p, ks = z % 2, z // 2
    near, far = 1 + ks, (n_seq - 1) * ks
    zp = near + far - z
    is_near, is_far = z == near, z == far
    is_main = k == ks
    is_aux = jnp.logical_not(is_main)
    main_dp = 2 * chip + ks

    def head_of(core, j):
        return 4 * core + 2 * j + p

    def rows_of(ref_rows, index):
        return pl.ds(pl.multiple_of(index * ref_rows, ref_rows), ref_rows)

    def lanes_of(index):
        return pl.ds(pl.multiple_of(index * DH, DH), DH)

    def w_copies(core, j, make):
        return [
            make(
                w_ref.at[:, lanes_of(g * n_heads + head_of(core, j))],
                W.at[j, rows_of(tok, me), slice(g * DH, (g + 1) * DH)],
            )
            for g in range(4)
        ]

    w_targets = (
        (xn, 0, wvia.at[k]), (yn, 1, wvia.at[k]), (chip, 1 - k, wrest), (xn, 1, wrest),
        (yn, 0, wrest),
    )

    def w_start(j):
        for where, core, sem in w_targets:
            for copy in w_copies(
                core, j, lambda s, d: remote(s, d, wout, sem.at[j], (2 * where + core, z))
            ):
                copy.start()

    def w_piece(src, j):
        return W.at[j, rows_of(tok, src)]

    via, to = (1 - k) * xn + k * yn, (1 - k) * yn + k * xn

    def w_relay(i, j):
        src = 2 * via + i
        block = w_piece(src, j)
        return remote(block, block, wout, wrest.at[j], (2 * to + k, z))

    ins, outs = (x_ref, c_ref), (X, C)
    z_to = jnp.where(is_main, zp, 1 + k)

    def z_send(a):
        return remote(ins[a], outs[a].at[z], zout, xrecv.at[a, z], (me, z_to))

    def own_copy(a):
        return pltpu.make_async_copy(ins[a], outs[a].at[z], xrecv.at[a, z])

    def share(a, b):
        block = ins[a] if b is None else outs[a].at[b]
        at = z if b is None else b
        return remote(block, outs[a].at[at], shareout, xrecv.at[a, at], (sib, z))

    foreign = (2 * (1 - ks), 2 * (1 - ks) + 1)

    def to_far(a, i):
        block = outs[a].at[foreign[i]]
        return remote(block, block, farout, xrecv.at[a, foreign[i]], (me, far))

    def x_wait(a, b):
        arrived(outs[a].at[b], xrecv.at[a, b])

    def meta_send():
        return remote(meta_ref, mbuf, msem.at[0], msem.at[1], (sib, z))

    wo_core, wo_slot = chip // 2, chip % 2
    wo_part = 2 * k + wo_core
    wo_here = wo_core == k
    wo_sem = jnp.where(k == p, wo_slot, 2)
    wo_sends = [
        remote(
            wo_ref, WO.at[wo_part, wo_slot], woout, worecv.at[wo_sem],
            (2 * where + wo_core, z),
        )
        for i, where in enumerate((xn, yn, dn, chip))
    ]

    def wo_start():
        for i in range(3):
            wo_sends[i].start()

        @pl.when(wo_here)
        def _():
            pltpu.make_async_copy(wo_ref, WO.at[wo_part, wo_slot], worecv.at[wo_sem]).start()

        @pl.when(jnp.logical_not(wo_here))
        def _():
            wo_sends[3].start()

    def wo_share(parity, j):
        block = WO.at[2 * parity + k, j]
        return remote(block, block, woout, worecv.at[3], (sib, z))

    loads = [
        pltpu.make_async_copy(src, dst, lsem.at[i])
        for src, dst, i in (
            (stamps_hbm, stamps_ref, 0), (w_hbm, w_ref, 1), (x_hbm, x_ref, 1), (c_hbm, c_ref, 1),
            (wo_hbm, wo_ref, 1), (gin_hbm, gin_ref, 2), (gout_hbm, gout_ref, 3),
            (bias_hbm, bias_ref, 4),
        )
    ]
    barrier = pltpu.get_barrier_semaphore()
    for step in range(1, n_dp):
        pl.semaphore_signal(
            barrier, inc=1, device_id=(lax.rem(me + step, n_dp), z), device_id_type=MESH
        )
    for step in range(1, n_seq):
        there = lax.rem(z + step, n_seq)

        @pl.when(jnp.abs(there - z) < n_seq - 1)
        def _():
            for peer in (me, sib):
                pl.semaphore_signal(
                    barrier, inc=1, device_id=(peer, there), device_id_type=MESH
                )

    for load in loads:
        load.start()
    loads[0].wait()
    meta_ref[0:1, :] = stamps_ref[...]
    meta_ref[1:2, :] = jnp.full(stamps_ref.shape, length_ref[0], jnp.int32)
    arrived(W.at[:, : (n_dp - 1) * tok], lsem.at[1])
    for load in loads[5:]:
        load.wait()
    inner = jnp.where((z > 0) & (z < n_seq - 1), 1, 0)
    pl.semaphore_wait(barrier, n_dp - 1 + 2 * (n_seq - 2) + 2 * inner)
    @pl.when(is_main)
    def _():
        pltpu.make_async_copy(meta_ref, mbuf, msem.at[1]).start()
        meta_send().start()

    w_start(0)
    z_send(0).start()

    @pl.when(is_main)
    def _():
        own_copy(0).start()
        share(0, None).start()

    z_send(1).start()

    @pl.when(is_main)
    def _():
        own_copy(1).start()
        share(1, None).start()

    for j in range(2):
        for copy in w_copies(k, j, lambda s, d: pltpu.make_async_copy(s, d, wrest.at[j])):
            copy.start()

    def relay_weights(j):
        for i in range(2):
            arrived(w_piece(2 * via + i, j), wvia.at[i, j])
            w_relay(i, j).start()

    def near_relay(a):
        @pl.when(is_main)
        def _():
            x_wait(a, zp)
            share(a, zp).start()

        @pl.when(is_main & is_near)
        def _():
            for i in range(2):
                x_wait(a, foreign[i])
                to_far(a, i).start()
                share(a, foreign[i]).start()

    def far_relay(a):
        @pl.when(is_main & is_far)
        def _():
            for i in range(2):
                x_wait(a, foreign[i])
                share(a, foreign[i]).start()

    relay_weights(0)
    w_start(1)
    near_relay(0)

    arrived(mbuf, msem.at[1])
    lane_row = lax.broadcasted_iota(jnp.int32, (DH, DH), 0)
    lane_col = lax.broadcasted_iota(jnp.int32, (DH, DH), 1)
    length = mbuf[1:2, :DH]
    for i in range(n_seq):
        col = jnp.broadcast_to(mbuf[0:1, i * DH : (i + 1) * DH].astype(F32), (DH, DH)).T
        valid = lane_row + i * DH < length
        for b in range(i + 1):
            elapsed = col - mbuf[0:1, b * DH : (b + 1) * DH].astype(F32)
            allowed = valid & (lane_col <= lane_row) if b == i else valid
            heads = [head_of(k, j) for j in range(2)]
            terms = [jnp.full(elapsed.shape, bias_ref[h, 0], F32) for h in heads]
            for degree in range(1, bias_ref.shape[1]):
                reached = elapsed >= float(2**degree - 1)
                terms = [
                    jnp.where(reached, bias_ref[h, degree], t) for h, t in zip(heads, terms)
                ]
            for j in range(2):
                BI[j, i * DH : (i + 1) * DH, b * DH : (b + 1) * DH] = jnp.where(
                    allowed, terms[j], MASKED
                )

    near_relay(1)
    relay_weights(1)

    far_relay(0)

    @pl.when(is_main)
    def _():
        x_wait(0, z)

    @pl.when(is_aux)
    def _():
        for b in range(n_seq):
            x_wait(0, b)

    for b in range(n_seq):
        NB[b * tok : (b + 1) * tok, :] = layer_norm(X[b].astype(F32), gin_ref[...]).astype(BF16)

    def forward(j):
        arrived(W.at[j, : (n_dp - 2) * tok], wrest.at[j])
        PJ[j] = mm(NB[...], W[j], ((1,), (0,)))
        cols = slice(j * DH, (j + 1) * DH)
        GT[:, cols] = jax.nn.silu(PJ[j, :, :DH])
        for g in range(3):
            ACT[j, g] = jax.nn.silu(PJ[j, :, (1 + g) * DH : (2 + g) * DH]).astype(BF16)
        for i in range(n_seq):
            at, end = slice(i * tok, (i + 1) * tok), (i + 1) * tok
            scores = mm(ACT[j, 1, at], ACT[j, 2, :end], ((1,), (1,))) * scale + BI[j, at, :end]
            sig = jax.nn.sigmoid(scores)
            weight = (scores * sig).astype(BF16)
            WT[j, at, :end] = weight
            SL[j, at, :end] = sig * (1.0 + scores * (1.0 - sig))
            ATT[at, cols] = mm(weight, ACT[j, 0, :end], ((1,), (0,)))

    @pl.when(k == p)
    def _():
        wo_start()

    forward(0)

    forward(1)

    gain = jnp.concatenate([gout_ref[:, lanes_of(head_of(k, j))] for j in range(2)], axis=1)
    pid = 2 * p + k
    own_width = 2 * DH
    st_peers = ((sib, z), (me, zp), (sib, zp))

    def stat_sends(ref, send_sem, recv_sem):
        return [
            remote(ref.at[pid], ref.at[pid], send_sem, recv_sem, peer)
            for peer in st_peers
        ]

    def put_stats(ref, b, first, second):
        pair = jnp.where(lane_col == 0, first, second).T
        ref[pid, b : b + 1, :] = pair[0:1]
        ref[pid, n_seq + b : n_seq + b + 1, :] = pair[1:2]

    for b in range(n_seq):
        at = slice(b * tok, (b + 1) * tok)
        att = ATT[at, :]
        mean_own = jnp.mean(att, axis=1, keepdims=True)
        off = att - mean_own
        put_stats(SA, b, mean_own, jnp.sum(off * off, axis=1, keepdims=True))
    for copy in stat_sends(SA, saout, sarecv):
        copy.start()
    far_relay(1)
    @pl.when(is_main)
    def _():
        x_wait(1, z)

    @pl.when(is_aux)
    def _():
        for b in range(n_seq):
            x_wait(1, b)

    c_rows = C[...].reshape(rows, width)
    for j in range(2):
        arrived(WO.at[pid, j], worecv.at[j])
        wo_share(p, j).start()
        DM[:, j * DH : (j + 1) * DH] = mm(c_rows, WO[pid, j], ((1,), (1,)))
    for b in range(n_seq):
        at = slice(b * tok, (b + 1) * tok)
        att = ATT[at, :]
        off = att - jnp.mean(att, axis=1, keepdims=True)
        g = DM[at, :] * GT[at, :] * gain
        put_stats(
            SG, b, jnp.sum(g, axis=1, keepdims=True), jnp.sum(g * off, axis=1, keepdims=True)
        )
    for copy in stat_sends(SG, sgout, sgrecv):
        copy.start()

    arrived(SA.at[:3], sarecv)
    first, second = slice(0, n_seq), slice(n_seq, 2 * n_seq)
    means = [SA[q, first, :] for q in range(4)]
    mean = sum(means[1:], means[0]) / 4.0
    shifts = [m - mean for m in means]
    squares = sum(SA[q, second, :] + own_width * shifts[q] * shifts[q] for q in range(4))
    rstd = lax.rsqrt(squares / width + EPS)
    TB[0], TB[1] = mean, rstd

    def turned(i, b):
        wide_row = jnp.broadcast_to(TB[i, b : b + 1, :], (DH, DH)).T
        return jnp.concatenate([wide_row] * 2, axis=1)

    blocks = tuple(reversed(range(n_seq)))

    def mine(b):
        return is_near == (far != b)

    def other(b):
        return is_near == (far == b)

    def home_is_self(b):
        return is_main & (z == b)

    def mx_send(b):
        return remote(
            MR.at[b * tok : (b + 1) * tok], MX.at[pid], mxout, mxrecv, (main_dp, b)
        )

    for b in blocks:
        at = slice(b * tok, (b + 1) * tok)
        hat = (ATT[at, :] - turned(0, b)) * turned(1, b)
        ATT[at, :] = hat
        MR[at, :] = (hat * gain * GT[at, :]).astype(BF16)

    pieces = PIECES
    piece = DH // pieces

    def out_rows(i):
        return slice(i * piece, (i + 1) * piece)

    def g_send(j, i):
        return remote(
            MW.at[j, i], WG.at[chip, i], gout, grecv.at[i],
            (2 * (2 * k + j) + p, z),
        )

    def g_self(j):
        return (2 * k + j == chip) & (k == p)

    for j in range(2):
        part = mm(MR[:, j * DH : (j + 1) * DH], c_rows, ((0,), (0,)))
        for i in range(pieces):
            MW[j, i] = part[out_rows(i)].astype(BF16)
    for i in range(pieces):
        for j in range(2):

            @pl.when(g_self(j))
            def _():
                pltpu.make_async_copy(MW.at[j, i], WG.at[chip, i], grecv.at[i]).start()

            @pl.when(jnp.logical_not(g_self(j)))
            def _():
                g_send(j, i).start()

    is_root = k == p
    far_root, near_root, middle, edge = (n_seq - 1) * k, 2 - k, 1 + k, (n_seq - 1) * (1 - k)
    def h_send(dst, recv, i):
        return remote(PS.at[i], dst.at[i], hout, recv.at[i], (me, middle))

    def h_relay(src, i, to):
        return remote(src.at[i], PR.at[i], hout, hback.at[i], (me, to))

    def t_send(i):
        return remote(TS.at[i], TR.at[i], hout, trecv.at[i], (me, edge))

    def plane_sum(i):
        @pl.when(is_root)
        def _():
            arrived(WG.at[:, i], grecv.at[i])
            total = WG[0, i].astype(F32)
            for c in range(1, n_dp // 2):
                total = total + WG[c, i].astype(F32)
            PS[i] = total.astype(BF16)

            @pl.when(z == far_root)
            def _():
                h_send(MA, hmid.at[0], i).start()

            @pl.when(z == near_root)
            def _():
                h_send(MB, hmid.at[1], i).start()

    def pass_in():
        @pl.when(z == middle)
        def _():
            for i in range(pieces):
                arrived(MB.at[i], hmid.at[1, i])
                h_relay(MB, i, far_root).start()

    def pass_out():
        @pl.when(z == middle)
        def _():
            for i in range(pieces):
                arrived(MA.at[i], hmid.at[0, i])
                h_relay(MA, i, near_root).start()
                wg_ref[out_rows(i)] = (MA[i].astype(F32) + MB[i].astype(F32)).astype(BF16)

    def root_total(i):
        arrived(PR.at[i], hback.at[i])
        TS[i] = (PS[i].astype(F32) + PR[i].astype(F32)).astype(BF16)
        wg_ref[out_rows(i)] = TS[i]

    def near_total():
        @pl.when(z == near_root)
        def _():
            for i in range(pieces):
                root_total(i)
                t_send(i).start()

    def outer_total():
        @pl.when(z == far_root)
        def _():
            for i in range(pieces):
                root_total(i)

        @pl.when(z == edge)
        def _():
            for i in range(pieces):
                arrived(TR.at[i], trecv.at[i])
                wg_ref[out_rows(i)] = TR[i]

    def pair_send(b):
        return remote(PB.at[b, 1 - k], SB.at[b], pout, precv.at[b], (sib, z))

    def cross_send(b):
        return remote(CS.at[b], FB.at[b], cout, crecv.at[b], (me, zp))

    def home_send(b):
        return remote(FIN.at[b], RO.at[k], oout, orecv, (main_dp, b))

    def pair_sum(b):
        return PB[b, k].astype(F32) + SB[b].astype(F32)

    def cross(b):
        arrived(SB.at[b], precv.at[b])

        @pl.when(other(b))
        def _():
            CS[b] = pair_sum(b).astype(BF16)
            cross_send(b).start()

    def finish(b):
        @pl.when(mine(b))
        def _():
            arrived(FB.at[b], crecv.at[b])
            FIN[b] = (pair_sum(b) + FB[b].astype(F32)).astype(BF16)

            @pl.when(home_is_self(b))
            def _():
                pltpu.make_async_copy(FIN.at[b], RO.at[k], orecv).start()

            @pl.when(jnp.logical_not(home_is_self(b)))
            def _():
                home_send(b).start()

    arrived(SG.at[:3], sgrecv)
    for b in blocks:

        @pl.when(home_is_self(b))
        def _():
            pltpu.make_async_copy(
                MR.at[b * tok : (b + 1) * tok], MX.at[pid], mxrecv
            ).start()

        @pl.when(jnp.logical_not(home_is_self(b)))
        def _():
            mx_send(b).start()

    g_mean = sum(SG[q, first, :] for q in range(4)) / width
    g_dot = rstd * sum(SG[q, second, :] + shifts[q] * SG[q, first, :] for q in range(4)) / width
    TB[1], TB[2], TB[3] = rstd, g_mean, g_dot
    for b in range(n_seq):
        at = slice(b * tok, (b + 1) * tok)
        d_mix, hat = DM[at, :], ATT[at, :]
        DG[at, :] = d_mix * (hat * gain)
        g = d_mix * GT[at, :] * gain
        DA[at, :] = (
            turned(1, b) * (g - turned(2, b) - hat * turned(3, b))
        ).astype(BF16)

    def backward(j, b):
        cols = slice(j * DH, (j + 1) * DH)
        start, end = b * tok, (b + 1) * tok

        def put(group, grad):
            at = slice(group * DH, (group + 1) * DH)
            DP[j, start:end, at] = (grad * silu_slope(PJ[j, start:end, at])).astype(BF16)

        d_att = DA[start:end, cols]
        d_weight = mm(d_att, ACT[j, 0, :end], ((1,), (1,)))
        d_scores = (d_weight * SL[j, start:end, :end]).astype(BF16)
        put(2, mm(d_scores, ACT[j, 2, :end], ((1,), (0,))) * scale)
        k_part = mm(d_scores, ACT[j, 1, start:end], ((0,), (0,)))
        v_part = mm(WT[j, start:end, :end], d_att, ((0,), (0,)))
        if end == rows:
            KA[j] = k_part
            VA[j] = v_part
        else:
            KA[j, :end] += k_part
            VA[j, :end] += v_part
        put(0, DG[start:end, cols])
        put(1, VA[j, start:end])
        put(3, KA[j, start:end] * scale)

    def d_part(b):
        at = slice(b * tok, (b + 1) * tok)
        part = mm(DP[0, at], W[0], ((1,), (1,))) + mm(DP[1, at], W[1], ((1,), (1,)))
        PB[b, 0] = part[:half].astype(BF16)
        PB[b, 1] = part[half:].astype(BF16)
        pair_send(b).start()

    last = n_seq - 1
    for b in blocks:
        for j in range(2):
            backward(j, b)
        if b == last - 1:

            @pl.when(ks == 0)
            def _():
                cross(last)

        elif b == 1:

            @pl.when(ks == 0)
            def _():
                cross(2)

        if b == last:

            @pl.when(ks == 0)
            def _():
                d_part(last)

        else:
            d_part(b)
        if b < 2:
            for i in range(pieces // 2):
                plane_sum((1 - b) * pieces // 2 + i)
    cross(1)
    cross(0)

    @pl.when(k != p)
    def _():
        wo_start()

    @pl.when(ks != 0)
    def _():
        cross(2)
        d_part(last)
        cross(last)

    finish(3)
    pass_in()
    @pl.when(ks == 0)
    def _():
        finish(2)

    pass_out()
    finish(1)
    finish(0)

    @pl.when(ks != 0)
    def _():
        finish(2)

    near_total()
    arrived(WO.at[2 * (1 - p) + k], worecv.at[2])
    for j in range(2):
        wo_share(1 - p, j).start()

    arrived(X, worecv.at[3])
    arrived(MX, mxrecv)
    wide = x_ref[...].astype(F32)
    total = wide
    for q in range(4):
        total = total + mm(MX[q], WO[q].reshape(2 * DH, width), ((1,), (0,)))
    mixed_ref[...] = total.astype(BF16)

    average = jnp.mean(wide, axis=-1, keepdims=True)
    centred = wide - average
    inv = lax.rsqrt(jnp.mean(centred * centred, axis=-1, keepdims=True) + EPS)
    hat = centred * inv
    arrived(RO, orecv)
    grad = RO[...].reshape(tok, width).astype(F32) * gin_ref[...]
    back = inv * (
        grad
        - jnp.mean(grad, axis=-1, keepdims=True)
        - hat * jnp.mean(grad * hat, axis=-1, keepdims=True)
    )
    grad_ref[...] = (c_ref[...].astype(F32) + back).astype(BF16)
    outer_total()

    beside = (sib, z)

    def sent_when(condition, block, sem):
        @pl.when(condition)
        def _():
            sent(block, sem, beside)

    part = (n_dp - 1) * tok
    sent(W.at[:, :part], wout, beside)
    sent(X.at[:2], zout, beside)
    sent_when(is_main, W, shareout)
    sent_when(is_main & is_near, X, farout)
    sent_when(is_main, meta_ref, msem.at[0])
    sent_when(wo_here, W.at[:, :part], woout)
    sent_when(jnp.logical_not(wo_here), W, woout)
    sent(SA.at[:3], saout, beside)
    sent(SG.at[:3], sgout, beside)
    sent_when(is_main, MX.at[:3], mxout)
    sent_when(is_aux, MX, mxout)
    keeps_one = is_root & wo_here
    sent_when(keeps_one, X.at[0], gout)
    sent_when(jnp.logical_not(keeps_one), X.at[:2], gout)
    sent_when(z == far_root, PS, hout)
    sent_when((z == near_root) | (z == middle), X.at[:2], hout)
    sent(X.at[:2], pout, beside)
    sent_when(is_far, CS.at[:3], cout)
    sent_when(is_near, CS.at[:1], cout)
    sent_when(is_near & is_main, FIN.at[:2], oout)
    sent_when(is_near & is_aux, FIN.at[:3], oout)
    sent_when(is_far & is_aux, FIN.at[:1], oout)


def tail_kernel(mixed_ref, grad_ref, wg_ref, mixed_out, grad_out, wg_out, wide, sems):
    copies = [
        pltpu.make_async_copy(src, dst, sems.at[i])
        for i, (src, dst) in enumerate(
            ((mixed_ref, mixed_out), (grad_ref, grad_out), (wide, wg_out))
        )
    ]
    copies[0].start()
    copies[1].start()
    wide[...] = wg_ref[...].astype(F32)
    copies[2].start()
    for copy in copies:
        copy.wait()


def column_parallel(
    n_dp, n_seq, tokens, cotangent, stamps, lengths, w_qkvu, w_out, gain_in, gain_out, bias_table
):
    tok, width = tokens.shape[1:]
    rows = tok * n_seq
    dma = pltpu.SemaphoreType.DMA
    sds = jax.ShapeDtypeStruct
    hbm = pl.BlockSpec(memory_space=pltpu.HBM)

    def vb(*shape):
        return pltpu.VMEM(shape, BF16)

    def vf(*shape):
        return pltpu.VMEM(shape, F32)

    def in_hbm(value):
        return pltpu.with_memory_space_constraint(value, pltpu.HBM)

    half = tok // 2
    mixed, grad, w_grad = pl.pallas_call(
        lambda *refs: column_kernel(n_dp, n_seq, *refs),
        out_shape=(sds((tok, width), BF16), sds((tok, width), BF16), sds(w_out.shape, BF16)),
        in_specs=[hbm] * 5 + [pl.BlockSpec(memory_space=pltpu.SMEM)] + [hbm] * 3,
        out_specs=[VM] * 3,
        scratch_shapes=[
            pltpu.VMEM(w_qkvu.shape, BF16),
            vb(tok, width),
            vb(tok, width),
            vb(DH, width),
            pltpu.VMEM(stamps.shape, jnp.int32),
            vf(1, width),
            vf(1, width),
            pltpu.SMEM(bias_table.shape, F32),
            pltpu.VMEM((8, rows), jnp.int32),
            vb(2, width, 4 * DH),
            vb(n_seq, tok, width),
            vb(n_seq, tok, width),
            vb(4, 2, DH, width),
            pltpu.VMEM((8, rows), jnp.int32),
            vb(rows, width),
            vf(2, rows, rows),
            vf(2, rows, 4 * DH),
            vf(rows, 2 * DH),
            vb(2, 3, rows, DH),
            vf(rows, 2 * DH),
            vb(2, rows, rows),
            vf(2, rows, rows),
            vf(rows, 2 * DH),
            vf(rows, 2 * DH),
            vb(rows, 2 * DH),
            vb(2, rows, 4 * DH),
            vb(rows, 2 * DH),
            vb(4, tok, 2 * DH),
            vf(2, rows, DH),
            vf(2, rows, DH),
            vf(4, 8, DH),
            vf(4, 8, DH),
            vf(4, n_seq, DH),
            vb(2, PIECES, DH // PIECES, width),
            vb(n_dp // 2, PIECES, DH // PIECES, width),
            vb(PIECES, DH // PIECES, width),
            vb(PIECES, DH // PIECES, width),
            vb(PIECES, DH // PIECES, width),
            vb(PIECES, DH // PIECES, width),
            vb(PIECES, DH // PIECES, width),
            vb(PIECES, DH // PIECES, width),
            vb(n_seq, 2, half, width),
            vb(n_seq, half, width),
            vb(n_seq, half, width),
            vb(n_seq, half, width),
            vb(n_seq, half, width),
            vb(2, half, width),
            dma((5,)),
            dma,
            dma((2, 2)),
            dma((2,)),
            dma,
            dma,
            dma,
            dma((2, n_seq)),
            dma,
            dma((4,)),
            dma((2,)),
            dma,
            dma,
            dma,
            dma,
            dma,
            dma,
            dma,
            dma((PIECES,)),
            dma,
            dma((2, PIECES)),
            dma((PIECES,)),
            dma((PIECES,)),
            dma,
            dma((n_seq,)),
            dma,
            dma((n_seq,)),
            dma,
            dma,
        ],
        compiler_params=pltpu.CompilerParams(
            has_side_effects=True, collective_id=0, vmem_limit_bytes=44 * 2**20
        ),
        name="column",
    )(
        *[in_hbm(v) for v in (w_qkvu, tokens[0], cotangent[0], w_out, stamps)],
        lengths,
        *[in_hbm(v) for v in (gain_in[None], gain_out[None], bias_table)],
    )
    mixed, grad, w_grad = pl.pallas_call(
        tail_kernel,
        out_shape=(sds(mixed.shape, BF16), sds(grad.shape, BF16), sds(w_grad.shape, F32)),
        in_specs=[VM] * 3,
        out_specs=[hbm] * 3,
        scratch_shapes=[vf(*w_grad.shape), dma((3,))],
        compiler_params=pltpu.CompilerParams(vmem_limit_bytes=8 * 2**20),
        name="tail",
    )(mixed, grad, w_grad)
    return (mixed[None], grad[None], w_grad)


def solution(mesh):
    n_dp, n_seq = mesh.shape["dp"], mesh.shape["seq"]

    def body(*args):
        tokens, stamps, w_out = args[0], args[2], args[5]
        mesh_fits = n_seq == 4 and n_dp == 2 * n_seq and n_dp == H
        sizes_fit = w_out.shape[0] == DH and tokens.shape[1] == DH
        if mesh_fits and sizes_fit and stamps.shape == (1, n_seq * DH):
            return column_parallel(n_dp, n_seq, *args)
        return per_device(*args)

    return jax.shard_map(
        body,
        mesh=mesh,
        in_specs=(
            P("dp", "seq", None),
            P("dp", "seq", None),
            P("dp", None),
            P("dp"),
            P("dp", None),
            P("dp", None),
            P(),
            P(),
            P(),
        ),
        out_specs=(P("dp", "seq", None), P("dp", "seq", None), P("dp", None)),
        check_vma=False,
    )
```
